32 devices in a mesh: expert: 8 (over y, x, core), shard: 4 (over z).
Axes of the slice: x: 2, y: 2, z: 4, core: 2. Of those that a mesh axis runs over, the one named last changes fastest.
Arguments:
- states: bfloat16 [18912, 512], P(('expert', 'shard')), may hold values from -6 to 6
- qkv_weight: bfloat16 [2, 512, 1536], P(None, 'shard'), may hold values from -0.25 to 0.25
- out_weight: bfloat16 [2, 512, 512], P(None, 'shard'), may hold values from -0.75 to 0.75
- norm_gain: bfloat16 [2, 512, 2], P(None, 'shard'), may hold values from 0.5 to 1.5
- norm_bias: bfloat16 [2, 512, 2], P(None, 'shard'), may hold values from -1.5 to 1.5
- router_weight: bfloat16 [2, 512, 32], P(None, 'shard'), may hold values from -0.25 to 0.25
- expert_in: bfloat16 [2, 32, 512, 2048], P(None, 'expert', 'shard'), may hold values from -0.25 to 0.25
- expert_out: bfloat16 [2, 32, 2048, 512], P(None, 'expert', 'shard'), may hold values from -2 to 2
- chosen: int32 [2, 18912, 2], P(None, ('expert', 'shard')), may hold values from 0 to 31, all different within a row; in each aligned block of 591 rows (0 to 590, 591 to 1181, ..., all dimensions but the last counted through in order) at most 74 rows name the same one
- image_count: int32 [32], P(('expert', 'shard')), may hold values from 2 to 3
- teacher: bfloat16 [18912, 512], P(('expert', 'shard')), may hold values from -6 to 6
Outputs:
- final_states: bfloat16 [18912, 512], P(('expert', 'shard'))
- input_grad: float32 [18912, 512], P(('expert', 'shard'))
- qkv_grad: float32 [2, 512, 1536], P(None, 'shard')
- out_grad: float32 [2, 512, 512], P(None, 'shard')
- gain_grad: float32 [2, 512, 2], P(None, 'shard')
- bias_grad: float32 [2, 512, 2], P(None, 'shard')
- router_grad: float32 [2, 512, 32], P(None, 'shard')
- expert_in_grad: float32 [2, 32, 512, 2048], P(None, 'expert', 'shard')
- expert_out_grad: float32 [2, 32, 2048, 512], P(None, 'expert', 'shard')
The draws below stay inside these ranges and needn't reach their ends.
Inputs may be any that keep to these rules, and one draw needn't show every extreme that they name: `chosen`: in each block the 591 rows of one device name every expert at most 74 times, and in each block some device names some expert exactly 74 times; the two experts of a token differ. Device i, counted in the order of the expert axis then the shard axis, holds image_count[i] live images in its first image slots; its other slots are padding: their rows of final_states are computed like any other row, but the loss and every gradient ignore them.
All inputs are finite; a program needn't handle non-finite values.
Results may differ from the reference program's by a relative error of at most 0.012.
Values may be sent and summed in bfloat16 or wider, within the bound.
A program may use at most 256 MiB of HBM per device.

```python
import math
import jax
import jax.numpy as jnp
import numpy as np
from jax import lax

D = 512
HEADS = 8
HEAD_DIM = 64
HIDDEN_SIZE = 2048
EXPERTS = 32
TOP = 2
SEQ = 197
LAYERS = 2
SLOTS = 3
TOK_DEV = 591
TOKENS = 18912
CAP = 74
N_EXPERT = 8
N_SHARD = 4


def set_ends(drawn, key, low, high):
    longest = drawn.shape.index(max(drawn.shape))
    spots = []
    for shift in (0, 1):
        where = [jax.random.randint(jax.random.fold_in(key, axis), (), 0, length) for axis, length in enumerate(drawn.shape)]
        where[longest] = (where[longest] + shift) % drawn.shape[longest]
        spots.append(tuple(where))
    return drawn.at[spots[0]].set(low).at[spots[1]].set(high)


def levels(key, shape, shards, least, top_value):
    level, own = 1.0, jax.random.fold_in(key, 6)
    for axis_at, shards_of in shards:
        steps = jnp.exp(jax.random.uniform(jax.random.fold_in(own, axis_at), (shards_of,), jnp.float32, least / len(shards), top_value / len(shards)))
        level = level * jnp.repeat(steps, shape[axis_at] // shards_of).reshape([-1 if axis == axis_at else 1 for axis in range(len(shape))])
    return level


def assign_block(stream_key, own, number, rows, number_of, top, reach, lean):
    order = jax.random.permutation(stream_key, number_of)
    crowded, usual = portions_of(number_of, rows * top, reach, lean, True), portions_of(number_of, rows * top, reach, lean, False)
    places = jnp.arange(number_of)

    def named(sizes, turn):
        used = int((sizes > 0).sum())
        fixed = max(1, used // 4)
        passed = fixed + (places - fixed + turn * (used - fixed)) % max(1, number_of - fixed)
        return jnp.zeros((number_of,), jnp.int32).at[order[jnp.where(places < fixed, places, passed)]].set(jnp.asarray(sizes, jnp.int32))

    sizes = jnp.where(number % 4 == 0, named(crowded, number // 4), named(usual, number - number // 4 - 1))
    mixed = jax.random.permutation(jax.random.fold_in(own, 3), number_of)
    giver, taker = mixed[0:number_of // 2 * 2:2], mixed[1:number_of // 2 * 2:2]
    slack = jnp.minimum(sizes[giver] - 1, reach - sizes[taker]) // 2
    slack = jnp.where((giver == order[0]) | (taker == order[0]) | (sizes[taker] == 0), 0, jnp.maximum(slack, 0))
    passed = jax.random.randint(jax.random.fold_in(own, 4), (number_of // 2,), 0, 1 << 20) % (slack + 1)
    sizes = sizes.at[giver].add(-passed).at[taker].add(passed)
    members = jnp.searchsorted(jnp.cumsum(sizes), jnp.arange(rows * top), side="right").astype(jnp.int32)
    listing = members.reshape(top, rows).T
    listing = listing[jax.random.permutation(jax.random.fold_in(own, 1), rows)]
    turn = jax.random.randint(jax.random.fold_in(own, 2), (rows, 1), 0, top)
    return jnp.take_along_axis(listing, (jnp.arange(top)[None, :] + turn) % top, axis=1)


def portions_of(amount, total, reach, slope, full):
    portions = [(1 << 20) // math.isqrt(rank ** slope) + 1 for rank in range(1, amount + 1)]
    largest = reach if full else min(reach, max(-(-total // amount), total * portions[0] // sum(portions)))
    least = 1 if total - largest >= amount - 1 else 0
    given, surplus = [largest] + [least] * (amount - 1), total - largest - least * (amount - 1)
    while surplus > 0:
        candidates = [i for i in range(1, amount) if given[i] < largest] or [i for i in range(1, amount) if given[i] < reach]
        whole, left = sum([portions[i] for i in candidates]), surplus
        for i in candidates:
            addition = min(reach - given[i], max(1, left * portions[i] // whole), surplus)
            given[i] = given[i] + addition
            surplus = surplus - addition
    return np.array(given)


def bell_draw(own_key, extent, scale, reach, split=(), held_as=jnp.bfloat16):
    array = scale * jax.random.normal(own_key, extent, jnp.float32)
    if split:
        array = array * levels(own_key, extent, split, -0.22, 0.18)
    return jnp.clip(array, -reach, reach).astype(held_as)


def setup_inputs(seed: int = 0) -> dict:
    keys = jax.random.split(jax.random.key(seed), 12)
    states = bell_draw(keys[0], (TOKENS, D), 1.0, 6.0, ((0, 32),))
    qkv_weight = bell_draw(keys[1], (LAYERS, D, 3 * D), D ** -0.5, 0.25, ((1, 4),))
    out_weight = bell_draw(keys[2], (LAYERS, D, D), (D // 8) ** -0.5, 0.75, ((1, 4),))
    norm_gain = jnp.clip(1.0 + 0.1 * jax.random.normal(keys[3], (LAYERS, D, 2), jnp.float32), 0.5, 1.5).astype(jnp.bfloat16)
    norm_bias = bell_draw(keys[4], (LAYERS, D, 2), 0.3, 1.5, ((1, 4),))
    router_weight = bell_draw(keys[5], (LAYERS, D, EXPERTS), D ** -0.5, 0.25, ((1, 4),))
    expert_in = bell_draw(keys[6], (LAYERS, EXPERTS, D, HIDDEN_SIZE), D ** -0.5, 0.25, ((1, 8), (2, 4)))
    expert_out = bell_draw(keys[7], (LAYERS, EXPERTS, HIDDEN_SIZE, D), (max(HIDDEN_SIZE // 256, 1)) ** -0.5, 2.0, ((1, 8), (2, 4)))
    chosen_keys = jax.random.split(jax.random.fold_in(keys[8], 1), LAYERS * TOKENS // TOK_DEV)
    chosen_turns = jax.random.permutation(jax.random.fold_in(keys[8], 3), LAYERS * TOKENS // TOK_DEV)
    chosen = jax.vmap(lambda own, number: assign_block(jax.random.fold_in(keys[8], 2), own, number, TOK_DEV, EXPERTS, TOP, CAP, 2))(chosen_keys, chosen_turns).reshape((LAYERS, TOKENS, TOP))
    image_count = set_ends(jax.random.randint(keys[9], (N_EXPERT * N_SHARD,), SLOTS - 1, SLOTS + 1), jax.random.fold_in(keys[9], 1), SLOTS - 1, SLOTS).astype(jnp.int32)
    teacher = bell_draw(keys[10], (TOKENS, D), 1.0, 6.0, ((0, 32),))
    return dict(states=states, qkv_weight=qkv_weight, out_weight=out_weight, norm_gain=norm_gain, norm_bias=norm_bias, router_weight=router_weight, expert_in=expert_in, expert_out=expert_out, chosen=chosen, image_count=image_count, teacher=teacher)


norm_eps = 1e-06
highest = lax.Precision.HIGHEST

@jax.custom_vjp
def low(v):
    return lax.optimization_barrier(v.astype(jnp.bfloat16)).astype(jnp.float32)

@jax.custom_vjp
def low_back(v):
    return v

def low_keep(v):
    return (low(v), None)

def low_pass(kept, grad):
    return (grad,)

def back_keep(v):
    return (v, None)

def back_low(kept, grad):
    return (low(grad),)
low.defvjp(low_keep, low_pass)
low_back.defvjp(back_keep, back_low)

def layer_norm(values, gain_row, shift_row):
    centred = values - lax.optimization_barrier(jnp.mean(values, axis=-1, keepdims=True))
    spread = lax.optimization_barrier(jnp.mean(centred * centred, axis=-1, keepdims=True))
    return centred * lax.rsqrt(spread + norm_eps) * gain_row + shift_row

def route_slots(picks_dev, capacity):
    flat_ids = picks_dev.reshape(-1).astype(jnp.int32)
    onehot = (flat_ids[:, None] == jnp.arange(EXPERTS, dtype=jnp.int32)[None, :]).astype(jnp.int32)
    before = (jnp.cumsum(onehot, axis=0) - onehot).astype(jnp.int32)
    ranking = lax.optimization_barrier(jnp.sum(before * onehot, axis=1)).astype(jnp.int32)
    slot_index = (flat_ids * capacity + ranking).astype(jnp.int32)
    routes_dev = flat_ids.shape[0]
    source = jnp.full((EXPERTS * capacity,), routes_dev, jnp.int32)
    source = source.at[slot_index].set(jnp.arange(routes_dev, dtype=jnp.int32))
    return (slot_index, source)

def plan_routes(picks_layer):
    devices = N_EXPERT * N_SHARD
    per_device = picks_layer.reshape(devices, TOK_DEV, TOP)
    slot_index, source = jax.vmap(lambda picks_dev: route_slots(picks_dev, CAP))(per_device)
    filled = source < TOP * TOK_DEV
    offsets = (jnp.arange(devices, dtype=jnp.int32) * TOK_DEV)[:, None]
    row_index = (offsets + jnp.minimum(source, TOP * TOK_DEV - 1) // TOP).astype(jnp.int32)
    row_index = row_index.reshape(devices, EXPERTS, CAP).transpose(1, 0, 2).reshape(EXPERTS, devices * CAP)
    filled = filled.reshape(devices, EXPERTS, CAP).transpose(1, 0, 2).reshape(EXPERTS, devices * CAP)
    device_base = jnp.arange(devices, dtype=jnp.int32)[:, None] * CAP
    positions = slot_index // CAP * (devices * CAP) + device_base + slot_index % CAP
    return (row_index, filled, positions.reshape(-1).astype(jnp.int32))

def attend_block(image_rows, qkv_layer, out_layer, gain_row, shift_row):
    normed = low(layer_norm(image_rows, gain_row, shift_row))
    projected = low_back(low(jnp.dot(normed, qkv_layer, precision=highest)))
    split_parts = projected.reshape(SLOTS, SEQ, 3, HEADS, HEAD_DIM)
    queries = split_parts[:, :, 0]
    keys_part = split_parts[:, :, 1]
    values_part = split_parts[:, :, 2]
    scores = low_back(jnp.einsum('ashd,athd->ahst', queries, keys_part, precision=highest) * HEAD_DIM ** (-0.5))
    weights = low(jax.nn.softmax(scores, axis=-1))
    attended = jnp.einsum('ahst,athd->ashd', weights, values_part, precision=highest)
    attended = low_back(low(attended.reshape(SLOTS * SEQ, HEADS * HEAD_DIM)))
    return image_rows + low_back(jnp.dot(attended, out_layer, precision=highest))

def expert_apply(operands):
    rows_in, weight_in, weight_out = operands
    hidden_pre = low_back(jnp.dot(rows_in, weight_in, precision=highest))
    activated = low(jax.nn.gelu(hidden_pre))
    return low_back(low(jnp.dot(activated, weight_out, precision=highest)))

def mixture(states_in, gain_row, shift_row, router_layer, in_layer, out_layer, picks_layer, row_index, filled, positions):
    model_width = states_in.shape[1]
    normed = low(layer_norm(states_in, gain_row, shift_row))
    logits = low_back(jnp.dot(normed, router_layer, precision=highest))
    chances = jax.nn.softmax(logits, axis=-1)
    gate_values = jnp.take_along_axis(chances, picks_layer, axis=1)
    dispatched = low_back(jnp.where(filled[:, :, None], normed[row_index], 0.0))
    produced = lax.map(jax.checkpoint(expert_apply), (dispatched, in_layer, out_layer))
    routed = produced.reshape(-1, model_width)[positions].reshape(-1, TOP, model_width)
    return states_in + lax.optimization_barrier(jnp.sum(gate_values[:, :, None] * routed, axis=1))

def reference(states, qkv_weight, out_weight, norm_gain, norm_bias, router_weight, expert_in, expert_out, chosen, image_count, teacher):
    devices = N_EXPERT * N_SHARD
    model_width = HEADS * HEAD_DIM
    slot_image = jnp.arange(TOK_DEV, dtype=jnp.int32) // SEQ
    living = (slot_image[None, :] < image_count[:, None]).reshape(devices * TOK_DEV)
    counted = jnp.sum(image_count.astype(jnp.float32)) * SEQ
    route_plans = [plan_routes(chosen[layer_index]) for layer_index in range(LAYERS)]
    target = teacher.astype(jnp.float32)

    def forward_pass(current, qkv_all, out_all, gain_all, shift_all, router_all, in_all, out_experts):
        for layer_index in range(LAYERS):

            def attend_one(image_rows, layer_index=layer_index):
                return attend_block(image_rows, qkv_all[layer_index], out_all[layer_index], gain_all[layer_index, :, 0], shift_all[layer_index, :, 0])
            grouped = current.reshape(devices, TOK_DEV, model_width)
            current = lax.map(jax.checkpoint(attend_one), grouped).reshape(devices * TOK_DEV, model_width)
            row_index, filled, positions = route_plans[layer_index]
            current = mixture(current, gain_all[layer_index, :, 1], shift_all[layer_index, :, 1], router_all[layer_index], in_all[layer_index], out_experts[layer_index], chosen[layer_index], row_index, filled, positions)
        missed = current - target
        loss_value = jnp.sum(jnp.where(living[:, None], missed * missed, 0.0)) / counted
        return (loss_value, current)
    float_inputs = tuple((array_in.astype(jnp.float32) for array_in in (states, qkv_weight, out_weight, norm_gain, norm_bias, router_weight, expert_in, expert_out)))
    loss_value, pullback, final = jax.vjp(forward_pass, *float_inputs, has_aux=True)
    gradients = pullback(jnp.ones((), jnp.float32))
    return (final.astype(jnp.bfloat16), gradients[0] * counted, gradients[1], gradients[2], gradients[3], gradients[4], gradients[5], gradients[6], gradients[7])
```

```python
import jax
import jax.numpy as jnp
from jax import lax
from jax.experimental import pallas as pl
from jax.experimental.pallas import tpu as pltpu
from jax.sharding import PartitionSpec as P

HEADS = 8
HEAD_DIM = 64
EXPERTS = 32
TOP = 2
SEQ = 197
SLOTS = 3
CAP = 74
norm_eps = 1e-06

LANES = 128
SEQ_PAD = 208
ROWS = 640
CAP_PAD = 80
CHUNK = 64
F32 = jnp.float32
BF16 = jnp.bfloat16


def dot(a, b):
    return jnp.dot(a, b, preferred_element_type=F32)


def dot_nt(a, b):
    return lax.dot_general(a, b, (((1,), (1,)), ((), ())), preferred_element_type=F32)


def dot_tn(a, b):
    return lax.dot_general(a, b, (((0,), (0,)), ((), ())), preferred_element_type=F32)


def rows_of(step, size):
    return pl.ds(pl.multiple_of(step * size, size), size)


def each_chunk(body, size=CHUNK, total=ROWS):
    def step(i, carry):
        body(rows_of(i, size))
        return carry

    lax.fori_loop(0, total // size, step, 0)


def centre(values):
    centred = values - jnp.mean(values, axis=-1, keepdims=True)
    spread = jnp.mean(centred * centred, axis=-1, keepdims=True)
    return centred, lax.rsqrt(spread + norm_eps)


def norm_rows(x_ref, gain, shift, out_ref):
    def body(rows):
        centred, inverse = centre(x_ref[rows, :])
        out_ref[rows, :] = (centred * inverse * gain + shift).astype(BF16)

    each_chunk(body)


def norm_pullback(x_ref, gain, grad_ref, total_ref, out_ref, sums_ref):
    sums_ref[...] = jnp.zeros_like(sums_ref)

    def body(rows):
        centred, inverse = centre(x_ref[rows, :])
        unit = centred * inverse
        grad = grad_ref[rows, :]
        scaled = grad * gain
        first = jnp.mean(scaled, axis=-1, keepdims=True)
        second = jnp.mean(scaled * unit, axis=-1, keepdims=True)
        out_ref[rows, :] = total_ref[rows, :] + inverse * (scaled - first - unit * second)
        sums_ref[0:1, :] += jnp.sum(grad * unit, axis=0, keepdims=True)
        sums_ref[1:2, :] += jnp.sum(grad, axis=0, keepdims=True)

    each_chunk(body)


def weight_parts(w_ref, model):
    side = jnp.transpose(w_ref[:, 4 * model :].astype(F32))
    return [side[EXPERTS + i : EXPERTS + i + 1, :] for i in range(4)]


def attention_rows(x_ref, w_ref, gain, shift, x1_ref, proj_ref, log_ref, att_ref, normed_ref):
    model = x_ref.shape[1]
    norm_rows(x_ref, gain, shift, normed_ref)
    for part in range(3):
        columns = slice(part * model, (part + 1) * model)
        proj_ref[:, columns] = dot(normed_ref[...], w_ref[:, columns]).astype(BF16)
    att_ref[...] = jnp.zeros_like(att_ref)
    log_ref[...] = jnp.zeros_like(log_ref)
    low = lax.broadcasted_iota(jnp.int32, (SEQ_PAD, LANES), 1) < HEAD_DIM
    inside = lax.broadcasted_iota(jnp.int32, (SEQ_PAD, SEQ_PAD), 1) < SEQ
    lane = lax.broadcasted_iota(jnp.int32, (SEQ_PAD, LANES), 1)

    def image(i, carry):
        rows = rows_of(i, SEQ_PAD)
        logs = jnp.zeros((SEQ_PAD, LANES), F32)
        for pair in range(HEADS // 2):
            at = pair * LANES
            queries = proj_ref[rows, at : at + LANES]
            keys = proj_ref[rows, model + at : model + at + LANES]
            values = proj_ref[rows, 2 * model + at : 2 * model + at + LANES]
            results = []
            for side in range(2):
                mine = low if side == 0 else jnp.logical_not(low)
                masked = jnp.where(mine, queries, jnp.zeros_like(queries))
                scores = dot_nt(masked, keys) * HEAD_DIM ** (-0.5)
                scores = jnp.where(inside, scores, -1e30)
                highest = jnp.max(scores, axis=-1, keepdims=True)
                exponent = jnp.exp(scores - highest)
                summed = jnp.sum(exponent, axis=-1, keepdims=True)
                weights = (exponent / summed).astype(BF16)
                logs = jnp.where(lane == 2 * pair + side, highest + jnp.log(summed), logs)
                results.append(dot(weights, values))
            att_ref[rows, at : at + LANES] = jnp.where(low, results[0], results[1]).astype(BF16)
        log_ref[rows, :] = logs
        return carry

    lax.fori_loop(0, SLOTS, image, 0)
    x1_ref[...] = x_ref[...] + dot(att_ref[...], w_ref[:, 3 * model : 4 * model])


def route_rows(picks_ref, slots_ref, turned_ref):
    lane = lax.broadcasted_iota(jnp.int32, (ROWS, LANES), 1)
    picks = picks_ref[...]
    firsts, seconds = picks[:, 0:1], picks[:, 1:2]
    match_first, match_second = lane == firsts, lane == seconds
    either = jnp.where(match_first | match_second, 1.0, 0.0).astype(BF16)
    down = lax.broadcasted_iota(jnp.int32, (ROWS, ROWS), 0)
    across = lax.broadcasted_iota(jnp.int32, (ROWS, ROWS), 1)
    before = dot(jnp.where(across < down, 1.0, 0.0).astype(BF16), either)
    rank_first = jnp.sum(jnp.where(match_first, before, 0.0), axis=-1, keepdims=True)
    rank_second = jnp.sum(jnp.where(match_second, before, 0.0), axis=-1, keepdims=True)
    slot_first = jnp.where(firsts < 0, -1.0, firsts.astype(F32) * CAP_PAD + rank_first)
    slot_second = jnp.where(seconds < 0, -1.0, seconds.astype(F32) * CAP_PAD + rank_second)
    both = jnp.where(lane == 0, slot_first, jnp.where(lane == 1, slot_second, -1.0))
    slots_ref[...] = both.astype(jnp.int32)
    turned_ref[...] = jnp.transpose(both)[0:8, :].astype(jnp.int32)


def gate_rows(normed_ref, w_ref, picks_ref, chances_ref, gates_ref):
    model = normed_ref.shape[1]
    lane = lax.broadcasted_iota(jnp.int32, (ROWS, LANES), 1)
    logits = dot(normed_ref[...], w_ref[:, 4 * model :])
    logits = jnp.where(lane < EXPERTS, logits, -1e30)
    exponent = jnp.exp(logits - jnp.max(logits, axis=-1, keepdims=True))
    chances = exponent / jnp.sum(exponent, axis=-1, keepdims=True)
    chances_ref[...] = chances
    picks = picks_ref[...]
    gate_first = jnp.sum(jnp.where(lane == picks[:, 0:1], chances, 0.0), axis=-1, keepdims=True)
    gate_second = jnp.sum(jnp.where(lane == picks[:, 1:2], chances, 0.0), axis=-1, keepdims=True)
    gates_ref[...] = jnp.where(lane == 0, gate_first, jnp.where(lane == 1, gate_second, 0.0))


BLOCK = 4 * CAP_PAD


def dispatch_rows(turned_ref, rows_ref, out_ref):
    def block(i, carry):
        slot = lax.broadcasted_iota(jnp.int32, (BLOCK, ROWS), 0) + i * BLOCK
        chosen = (slot == turned_ref[0:1, :]) | (slot == turned_ref[1:2, :])
        out_ref[rows_of(i, BLOCK), :] = dot(
            jnp.where(chosen, 1.0, 0.0).astype(BF16), rows_ref[...]
        ).astype(BF16)
        return carry

    lax.fori_loop(0, EXPERTS * CAP_PAD // BLOCK, block, 0)


def dispatch_pairs(turned_ref, pairs_ref, out_ref):
    def block(i, carry):
        slot = lax.broadcasted_iota(jnp.int32, (BLOCK, ROWS), 0) + i * BLOCK
        first = jnp.where(slot == turned_ref[0:1, :], 1.0, 0.0).astype(BF16)
        second = jnp.where(slot == turned_ref[1:2, :], 1.0, 0.0).astype(BF16)
        out_ref[rows_of(i, BLOCK), :] = dot(
            jnp.concatenate([first, second], axis=1), pairs_ref[...]
        ).astype(BF16)
        return carry

    lax.fori_loop(0, EXPERTS * CAP_PAD // BLOCK, block, 0)


PART = 512


def collect_pairs(slots_ref, returned_ref, total_ref):
    total_ref[...] = jnp.zeros_like(total_ref)

    def part(i, carry):
        slot = lax.broadcasted_iota(jnp.int32, (ROWS, PART), 1) + i * PART
        rows = returned_ref[rows_of(i, PART), :]
        for side in range(2):
            chosen = jnp.where(slot == slots_ref[:, side : side + 1], 1.0, 0.0).astype(BF16)
            total_ref[side * ROWS : (side + 1) * ROWS, :] += dot(chosen, rows)
        return carry

    lax.fori_loop(0, EXPERTS * CAP_PAD // PART, part, 0)


def collect_sums(slots_ref, returned_ref, total_ref):
    total_ref[...] = jnp.zeros_like(total_ref)

    def part(i, carry):
        slot = lax.broadcasted_iota(jnp.int32, (ROWS, PART), 1) + i * PART
        chosen = (slot == slots_ref[:, 0:1]) | (slot == slots_ref[:, 1:2])
        total_ref[...] += dot(
            jnp.where(chosen, 1.0, 0.0).astype(BF16), returned_ref[rows_of(i, PART), :]
        )
        return carry

    lax.fori_loop(0, EXPERTS * CAP_PAD // PART, part, 0)


def combine(x1_ref, gates_ref, slots_ref, returned_ref, x_ref, routed_ref, total_ref):
    collect_pairs(slots_ref, returned_ref, total_ref)

    def body(rows):
        later = pl.ds(pl.multiple_of(rows.start + ROWS, CHUNK), CHUNK)
        first, second = total_ref[rows, :], total_ref[later, :]
        gates = gates_ref[rows, :]
        x_ref[rows, :] = x1_ref[rows, :] + gates[:, 0:1] * first + gates[:, 1:2] * second
        routed_ref[rows, :] = first.astype(BF16)
        routed_ref[later, :] = second.astype(BF16)

    each_chunk(body)


def split_grads(grad_ref, gates_ref, routed_ref, turned_ref, pairs_ref, grad_gates_ref, out_ref):
    lane = lax.broadcasted_iota(jnp.int32, (CHUNK, LANES), 1)

    def body(rows):
        later = pl.ds(pl.multiple_of(rows.start + ROWS, CHUNK), CHUNK)
        grad = grad_ref[rows, :]
        gates = gates_ref[rows, :]
        pairs_ref[rows, :] = (gates[:, 0:1] * grad).astype(BF16)
        pairs_ref[later, :] = (gates[:, 1:2] * grad).astype(BF16)
        first = jnp.sum(grad * routed_ref[rows, :].astype(F32), axis=-1, keepdims=True)
        second = jnp.sum(grad * routed_ref[later, :].astype(F32), axis=-1, keepdims=True)
        grad_gates_ref[rows, :] = jnp.where(lane == 0, first, jnp.where(lane == 1, second, 0.0))

    each_chunk(body)
    dispatch_pairs(turned_ref, pairs_ref, out_ref)


def attention_pullback(grad_ref, w_ref, proj_ref, log_ref, att_ref, normed_ref, small_ref, gproj_ref, gatt_ref, back_ref, gnormed_ref):
    model = grad_ref.shape[1]

    def body(rows):
        back_ref[rows, :] = grad_ref[rows, :].astype(BF16)

    each_chunk(body)
    small_ref[:, 3 * model : 4 * model] = dot_tn(att_ref[...], back_ref[...])
    gatt_ref[...] = dot_nt(back_ref[...], w_ref[:, 3 * model : 4 * model]).astype(BF16)
    gproj_ref[SLOTS * SEQ_PAD :, :] = jnp.zeros((ROWS - SLOTS * SEQ_PAD, 3 * model), BF16)
    low = lax.broadcasted_iota(jnp.int32, (SEQ_PAD, LANES), 1) < HEAD_DIM
    inside = lax.broadcasted_iota(jnp.int32, (SEQ_PAD, SEQ_PAD), 1) < SEQ
    scaling = HEAD_DIM ** (-0.5)

    def image(i, carry):
        rows = rows_of(i, SEQ_PAD)
        for pair in range(HEADS // 2):
            at = pair * LANES
            queries = proj_ref[rows, at : at + LANES]
            keys = proj_ref[rows, model + at : model + at + LANES]
            values = proj_ref[rows, 2 * model + at : 2 * model + at + LANES]
            grad_heads = gatt_ref[rows, at : at + LANES]
            parts = []
            for side in range(2):
                mine = low if side == 0 else jnp.logical_not(low)
                zero = jnp.zeros_like(queries)
                head = 2 * pair + side
                scores = dot_nt(jnp.where(mine, queries, zero), keys) * scaling
                chances = jnp.where(inside, jnp.exp(scores - log_ref[rows, head : head + 1]), 0.0)
                grad_weights = dot_nt(jnp.where(mine, grad_heads, zero), values)
                centre_term = jnp.sum(grad_weights * chances, axis=-1, keepdims=True)
                grad_scores = (chances * (grad_weights - centre_term)).astype(BF16)
                parts.append(
                    (
                        dot(grad_scores, keys) * scaling,
                        dot_tn(grad_scores, queries) * scaling,
                        dot_tn(chances.astype(BF16), grad_heads),
                    )
                )
            for which in range(3):
                to = which * model + at
                gproj_ref[rows, to : to + LANES] = jnp.where(low, parts[0][which], parts[1][which]).astype(BF16)
        return carry

    lax.fori_loop(0, SLOTS, image, 0)
    for part in range(3):
        columns = slice(part * model, (part + 1) * model)
        small_ref[:, columns] = dot_tn(normed_ref[...], gproj_ref[:, columns])
    gnormed_ref[...] = dot_nt(gproj_ref[...], w_ref[:, : 3 * model])


def router_pullback(grad_gates_ref, picks_ref, chances_ref, w_ref, normed_ref, gnormed_ref, router_ref):
    model = normed_ref.shape[1]
    lane = lax.broadcasted_iota(jnp.int32, (ROWS, LANES), 1)
    picks, grads, chances = picks_ref[...], grad_gates_ref[...], chances_ref[...]
    spread = jnp.where(lane == picks[:, 0:1], grads[:, 0:1], 0.0) + jnp.where(lane == picks[:, 1:2], grads[:, 1:2], 0.0)
    logits = chances * (spread - jnp.sum(spread * chances, axis=-1, keepdims=True))
    logits = logits.astype(BF16)
    router_ref[...] = dot_tn(normed_ref[...], logits)
    gnormed_ref[...] += dot_nt(logits, w_ref[:, 4 * model :])


def front(x_ref, w_ref, picks_ref, outs, scratch):
    x1_ref, proj_ref, log_ref, att_ref, slots_ref, turned_ref, chances_ref, gates_ref, leaving_ref = outs
    (normed_ref,) = scratch
    gain1, gain2, shift1, shift2 = weight_parts(w_ref, x_ref.shape[1])
    attention_rows(x_ref, w_ref, gain1, shift1, x1_ref, proj_ref, log_ref, att_ref, normed_ref)
    route_rows(picks_ref, slots_ref, turned_ref)
    norm_rows(x1_ref, gain2, shift2, normed_ref)
    gate_rows(normed_ref, w_ref, picks_ref, chances_ref, gates_ref)
    dispatch_rows(turned_ref, normed_ref, leaving_ref)


def first_kernel(x_ref, w_ref, picks_ref, *rest):
    front(x_ref, w_ref, picks_ref, rest[:9], rest[9:])


def middle_kernel(x1_ref, gates_ref, slots_ref, returned_ref, w_ref, picks_ref, x_ref, routed_ref, *rest):
    combine(x1_ref, gates_ref, slots_ref, returned_ref, x_ref, routed_ref, rest[10])
    front(x_ref, w_ref, picks_ref, rest[:9], rest[9:10])


def last_kernel(x1_ref, gates_ref, slots_ref, turned_ref, returned_ref, teacher_ref, scale_ref, final_ref, grad_ref, grad_gates_ref, leaving_ref, x_ref, routed_ref, total_ref, pairs_ref):
    combine(x1_ref, gates_ref, slots_ref, returned_ref, x_ref, routed_ref, total_ref)

    def body(rows):
        values = x_ref[rows, :]
        final_ref[rows, :] = values.astype(BF16)
        grad_ref[rows, :] = (values - teacher_ref[rows, :].astype(F32)) * scale_ref[rows, :]

    each_chunk(body)
    split_grads(grad_ref, gates_ref, routed_ref, turned_ref, pairs_ref, grad_gates_ref, leaving_ref)


def back(grad_in_ref, returned_ref, slots_ref, picks_ref, grad_gates_ref, chances_ref, x1_ref, x_ref, proj_ref, log_ref, att_ref, w_ref, grad_ref, small_ref, scratch):
    normed_ref, gnormed_ref, gproj_ref, gatt_ref, back_ref, mid_ref, sums_a, sums_b, router_ref = scratch
    model = x_ref.shape[1]
    gain1, gain2, shift1, shift2 = weight_parts(w_ref, model)
    collect_sums(slots_ref, returned_ref, gnormed_ref)
    norm_rows(x1_ref, gain2, shift2, normed_ref)
    router_pullback(grad_gates_ref, picks_ref, chances_ref, w_ref, normed_ref, gnormed_ref, router_ref)
    norm_pullback(x1_ref, gain2, gnormed_ref, grad_in_ref, mid_ref, sums_b)
    norm_rows(x_ref, gain1, shift1, normed_ref)
    attention_pullback(mid_ref, w_ref, proj_ref, log_ref, att_ref, normed_ref, small_ref, gproj_ref, gatt_ref, back_ref, gnormed_ref)
    norm_pullback(x_ref, gain1, gnormed_ref, mid_ref, grad_ref, sums_a)
    rows = lax.broadcasted_iota(jnp.int32, (LANES, model), 0)
    side = jnp.zeros((LANES, model), F32)
    for i, value in enumerate((sums_a[0:1, :], sums_b[0:1, :], sums_a[1:2, :], sums_b[1:2, :])):
        side = jnp.where(rows == EXPERTS + i, value, side)
    lane = lax.broadcasted_iota(jnp.int32, (model, LANES), 1)
    small_ref[:, 4 * model :] = jnp.where(lane < EXPERTS, router_ref[...], jnp.transpose(side))


def back_kernel(*refs):
    ins, (grad_ref, small_ref), scratch = refs[:12], refs[12:14], refs[14:]
    back(*ins, grad_ref, small_ref, scratch)


def back_middle_kernel(*refs):
    ins, (gates_ref, routed_ref, turned_ref) = refs[:12], refs[12:15]
    grad_ref, small_ref, grad_gates_ref, leaving_ref = refs[15:19]
    scratch, pairs_ref = refs[19:-1], refs[-1]
    back(*ins, grad_ref, small_ref, scratch)
    split_grads(grad_ref, gates_ref, routed_ref, turned_ref, pairs_ref, grad_gates_ref, leaving_ref)


def shape(dims, kind):
    return jax.ShapeDtypeStruct(dims, kind)


def front_outs(model):
    return [
        shape((ROWS, model), F32),
        shape((ROWS, 3 * model), BF16),
        shape((ROWS, LANES), F32),
        shape((ROWS, model), BF16),
        shape((ROWS, LANES), jnp.int32),
        shape((8, ROWS), jnp.int32),
        shape((ROWS, LANES), F32),
        shape((ROWS, LANES), F32),
        shape((EXPERTS * CAP_PAD, model), BF16),
    ]


def back_scratch(model):
    return [
        pltpu.VMEM((ROWS, model), BF16),
        pltpu.VMEM((ROWS, model), F32),
        pltpu.VMEM((ROWS, 3 * model), BF16),
        pltpu.VMEM((ROWS, model), BF16),
        pltpu.VMEM((ROWS, model), BF16),
        pltpu.VMEM((ROWS, model), F32),
        pltpu.VMEM((2, model), F32),
        pltpu.VMEM((2, model), F32),
        pltpu.VMEM((model, LANES), F32),
    ]


def call(kernel, outs, scratch, name, limit=56):
    return pl.pallas_call(
        kernel,
        out_shape=outs,
        scratch_shapes=scratch,
        compiler_params=pltpu.CompilerParams(vmem_limit_bytes=limit << 20),
        name=name,
    )


def run_first(x, w, picks):
    model = x.shape[1]
    return call(first_kernel, front_outs(model), [pltpu.VMEM((ROWS, model), BF16)], "first")(x, w, picks)


def run_middle(x1, gates, slots, returned, w, picks):
    model = x1.shape[1]
    outs = [shape((ROWS, model), F32), shape((TOP * ROWS, model), BF16)] + front_outs(model)
    scratch = [pltpu.VMEM((ROWS, model), BF16), pltpu.VMEM((TOP * ROWS, model), F32)]
    return call(middle_kernel, outs, scratch, "middle")(x1, gates, slots, returned, w, picks)


def run_last(x1, gates, slots, turned, returned, teacher, scale):
    model = x1.shape[1]
    outs = [
        shape((ROWS, model), BF16),
        shape((ROWS, model), F32),
        shape((ROWS, LANES), F32),
        shape((EXPERTS * CAP_PAD, model), BF16),
    ]
    scratch = [
        pltpu.VMEM((ROWS, model), F32),
        pltpu.VMEM((TOP * ROWS, model), BF16),
        pltpu.VMEM((TOP * ROWS, model), F32),
        pltpu.VMEM((TOP * ROWS, model), BF16),
    ]
    return call(last_kernel, outs, scratch, "last")(x1, gates, slots, turned, returned, teacher, scale)


def small_shape(model):
    return shape((model, 4 * model + LANES), F32)


def run_back(*ins):
    model = ins[0].shape[1]
    return call(back_kernel, [shape((ROWS, model), F32), small_shape(model)], back_scratch(model), "back")(*ins)


def run_back_middle(*ins):
    model = ins[0].shape[1]
    outs = [shape((ROWS, model), F32), small_shape(model), shape((ROWS, LANES), F32), shape((EXPERTS * CAP_PAD, model), BF16)]
    scratch = back_scratch(model) + [pltpu.VMEM((TOP * ROWS, model), BF16)]
    return call(back_middle_kernel, outs, scratch, "back_middle")(*ins)


TILE = 640
WIDE = 512
ROOT = 0.7978845608028654
CUBE = 0.044715


def expert_kernel(x_ref, in_ref, out_ref, made_ref, act_ref, slope_ref):
    total = jnp.zeros((x_ref.shape[0], out_ref.shape[1]), F32)
    for start in range(0, in_ref.shape[1], WIDE):
        columns = slice(start, start + WIDE)
        pre = dot(x_ref[...], in_ref[:, columns])
        square = pre * pre
        bend = jnp.tanh(pre * (ROOT + ROOT * CUBE * square))
        half = 0.5 + 0.5 * bend
        act = (pre * half).astype(BF16)
        slope = half + (0.5 * pre) * (1.0 - bend * bend) * (ROOT + 3.0 * ROOT * CUBE * square)
        act_ref[:, columns] = act
        slope_ref[:, columns] = slope.astype(BF16)
        total = total + dot(act, out_ref[columns, :])
    made_ref[...] = total.astype(BF16)


def run_expert(rows, weight_in, weight_out):
    count, model = rows.shape
    hidden = weight_in.shape[1]
    whole = lambda dims: pl.BlockSpec(dims, lambda i: (0, 0), pipeline_mode=pl.Buffered(1))
    tile = lambda width: pl.BlockSpec((TILE, width), lambda i: (i, 0))
    return pl.pallas_call(
        expert_kernel,
        grid=(count // TILE,),
        in_specs=[tile(model), whole((model, hidden)), whole((hidden, model))],
        out_specs=[tile(model), tile(hidden), tile(hidden)],
        out_shape=[shape((count, model), BF16), shape((count, hidden), BF16), shape((count, hidden), BF16)],
        compiler_params=pltpu.CompilerParams(vmem_limit_bytes=56 << 20),
        name="expert",
    )(rows, weight_in, weight_out)


def expert_back_kernel(x_ref, g_ref, act_ref, slope_ref, in_ref, out_ref, back_ref, gin_ref, gout_ref, total_ref, gpre_ref):
    count = x_ref.shape[0]
    step = pl.program_id(0)

    @pl.when(step == 0)
    def _():
        total_ref[...] = jnp.zeros_like(total_ref)

    def tile(i, carry):
        rows = rows_of(i, TILE)
        grad_act = dot_nt(g_ref[rows, :], out_ref[...])
        grad_pre = (slope_ref[rows, :].astype(F32) * grad_act).astype(BF16)
        gpre_ref[rows, :] = grad_pre
        total_ref[rows, :] += dot_nt(grad_pre, in_ref[...])
        return carry

    lax.fori_loop(0, count // TILE, tile, 0)
    gin_ref[...] = dot_tn(x_ref[...], gpre_ref[...]).astype(BF16)
    gout_ref[...] = dot_tn(act_ref[...], g_ref[...]).astype(BF16)

    @pl.when(step == pl.num_programs(0) - 1)
    def _():
        back_ref[...] = total_ref[...].astype(BF16)


def run_expert_back(rows, grads, act, slope, weight_in, weight_out):
    count, model = rows.shape
    hidden = weight_in.shape[1]
    whole = pl.BlockSpec((count, model), lambda i: (0, 0), pipeline_mode=pl.Buffered(1))
    across = lambda height: pl.BlockSpec((height, WIDE), lambda i: (0, i))
    down = pl.BlockSpec((WIDE, model), lambda i: (i, 0))
    return pl.pallas_call(
        expert_back_kernel,
        grid=(hidden // WIDE,),
        in_specs=[whole, whole, across(count), across(count), across(model), down],
        out_specs=[pl.BlockSpec((count, model), lambda i: (0, 0)), across(model), down],
        out_shape=[shape((count, model), BF16), shape((model, hidden), BF16), shape((hidden, model), BF16)],
        scratch_shapes=[pltpu.VMEM((count, model), F32), pltpu.VMEM((count, WIDE), BF16)],
        compiler_params=pltpu.CompilerParams(vmem_limit_bytes=56 << 20),
        name="expert_back",
    )(rows, grads, act, slope, weight_in, weight_out)


def layer_norm(values, gain_row, shift_row):
    centred = values - jnp.mean(values, axis=-1, keepdims=True)
    spread = jnp.mean(centred * centred, axis=-1, keepdims=True)
    return centred * lax.rsqrt(spread + norm_eps) * gain_row + shift_row


def route_slots(picks_dev, capacity):
    flat_ids = picks_dev.reshape(-1)
    onehot = (flat_ids[:, None] == jnp.arange(EXPERTS, dtype=jnp.int32)[None, :]).astype(jnp.int32)
    before = jnp.cumsum(onehot, axis=0) - onehot
    ranking = jnp.sum(before * onehot, axis=1)
    slot_index = flat_ids * capacity + ranking
    routes_dev = flat_ids.shape[0]
    source = jnp.full((EXPERTS * capacity,), routes_dev, jnp.int32)
    source = source.at[slot_index].set(jnp.arange(routes_dev, dtype=jnp.int32))
    return (slot_index, source)


def attention_forward(current, qkv_full, out_full, gain_row, shift_row):
    model_width = current.shape[1]
    normed = layer_norm(current, gain_row, shift_row).astype(jnp.bfloat16)
    projected = jnp.dot(normed, qkv_full, preferred_element_type=jnp.float32).astype(jnp.bfloat16)
    split_parts = projected.reshape(SLOTS, SEQ, 3, HEADS, HEAD_DIM)
    scores = jnp.einsum(
        "ashd,athd->ahst",
        split_parts[:, :, 0],
        split_parts[:, :, 1],
        preferred_element_type=jnp.float32,
    ) * HEAD_DIM ** (-0.5)
    highest_score = jnp.max(scores, axis=-1, keepdims=True)
    exponent = jnp.exp(scores - highest_score)
    summed = jnp.sum(exponent, axis=-1, keepdims=True)
    weights = (exponent / summed).astype(jnp.bfloat16)
    log_total = highest_score + jnp.log(summed)
    attended = jnp.einsum(
        "ahst,athd->ashd", weights, split_parts[:, :, 2], preferred_element_type=jnp.float32
    )
    attended = attended.reshape(SLOTS * SEQ, model_width).astype(jnp.bfloat16)
    branch_out = jnp.dot(attended, out_full, preferred_element_type=jnp.float32)
    return (current + branch_out, (current, normed, projected, log_total, attended))


def attention_backward(grad_states, saved, qkv_full, out_full, gain_row, shift_row):
    current, normed, projected, log_total, attended = saved
    model_width = current.shape[1]
    grad_branch = grad_states.astype(jnp.bfloat16)
    grad_out = jnp.einsum("rd,re->de", attended, grad_branch, preferred_element_type=jnp.float32)
    grad_attended = jnp.einsum(
        "re,de->rd", grad_branch, out_full, preferred_element_type=jnp.float32
    ).astype(jnp.bfloat16)
    split_parts = projected.reshape(SLOTS, SEQ, 3, HEADS, HEAD_DIM)
    queries = split_parts[:, :, 0]
    keys_part = split_parts[:, :, 1]
    values_part = split_parts[:, :, 2]
    scaling = HEAD_DIM ** (-0.5)
    scores = (
        jnp.einsum("ashd,athd->ahst", queries, keys_part, preferred_element_type=jnp.float32)
        * scaling
    )
    chances = jnp.exp(scores - log_total)
    grad_heads = grad_attended.reshape(SLOTS, SEQ, HEADS, HEAD_DIM)
    grad_weights = jnp.einsum(
        "ashd,athd->ahst", grad_heads, values_part, preferred_element_type=jnp.float32
    )
    grad_values = jnp.einsum(
        "ahst,ashd->athd",
        chances.astype(jnp.bfloat16),
        grad_heads,
        preferred_element_type=jnp.float32,
    )
    centre_term = jnp.sum(grad_weights * chances, axis=-1, keepdims=True)
    grad_scores = (chances * (grad_weights - centre_term)).astype(jnp.bfloat16)
    grad_queries = (
        jnp.einsum("ahst,athd->ashd", grad_scores, keys_part, preferred_element_type=jnp.float32)
        * scaling
    )
    grad_keys = (
        jnp.einsum("ahst,ashd->athd", grad_scores, queries, preferred_element_type=jnp.float32)
        * scaling
    )
    grad_projected = jnp.stack([grad_queries, grad_keys, grad_values], axis=2)
    grad_projected = grad_projected.reshape(SLOTS * SEQ, 3 * model_width).astype(jnp.bfloat16)
    grad_qkv = jnp.einsum("rd,re->de", normed, grad_projected, preferred_element_type=jnp.float32)
    grad_normed = jnp.einsum(
        "re,de->rd", grad_projected, qkv_full, preferred_element_type=jnp.float32
    )
    unused_value, norm_pullback = jax.vjp(layer_norm, current, gain_row, shift_row)
    grad_input, grad_gain, grad_shift = norm_pullback(grad_normed)
    return (grad_states + grad_input, grad_qkv, grad_out, grad_gain, grad_shift)


def mixture_forward(current, gain_row, shift_row, router_full, in_shard, out_shard, picks_layer):
    row_count, model_width = current.shape
    experts_all = router_full.shape[1]
    normed = layer_norm(current, gain_row, shift_row).astype(jnp.bfloat16)
    logits = jnp.dot(normed, router_full, preferred_element_type=jnp.float32)
    chances = jax.nn.softmax(logits, axis=-1)
    matches = picks_layer[:, :, None] == jnp.arange(experts_all, dtype=jnp.int32)[None, None, :]
    gate_values = jnp.sum(jnp.where(matches, chances[:, None, :], 0.0), axis=-1)
    slot_index, source = route_slots(picks_layer, CAP)
    filled = source < TOP * row_count
    route_clip = jnp.minimum(source, TOP * row_count - 1)
    taken_rows = route_clip // TOP
    outgoing = jnp.where(filled[:, None], normed[taken_rows], jnp.zeros((), jnp.bfloat16))
    outgoing = outgoing.reshape(experts_all, CAP, model_width)
    arrived = lax.all_to_all(outgoing, "expert", split_axis=0, concat_axis=1, tiled=True)
    in_full, out_full = (
        lax.all_gather(in_shard, "shard", axis=1, tiled=True),
        lax.all_gather(out_shard, "shard", axis=1, tiled=True),
    )
    hidden_pre = jnp.einsum("erd,edh->erh", arrived, in_full, preferred_element_type=jnp.float32)
    activated = jax.nn.gelu(hidden_pre).astype(jnp.bfloat16)
    produced = jnp.einsum(
        "erh,ehd->erd", activated, out_full, preferred_element_type=jnp.float32
    ).astype(jnp.bfloat16)
    returned = lax.all_to_all(produced, "expert", split_axis=1, concat_axis=0, tiled=True)
    routed = returned.reshape(experts_all * CAP, model_width)[slot_index].reshape(
        row_count, TOP, model_width
    )
    updated = current + jnp.sum(gate_values[:, :, None] * routed.astype(jnp.float32), axis=1)
    saved = (
        current,
        normed,
        chances,
        matches,
        gate_values,
        slot_index,
        filled,
        route_clip,
        arrived,
        routed,
        in_full,
        out_full,
    )
    return (updated, saved)


def mixture_backward(grad_states, saved, gain_row, shift_row, router_full, in_shard, out_shard):
    (
        current,
        normed,
        chances,
        matches,
        gate_values,
        slot_index,
        filled,
        route_clip,
        arrived,
        routed,
        kept_in,
        kept_out,
    ) = saved
    row_count, model_width = current.shape
    experts_all = chances.shape[1]
    grad_routed = (gate_values[:, :, None] * grad_states[:, None, :]).astype(jnp.bfloat16)
    grad_routed = grad_routed.reshape(TOP * row_count, model_width)
    grad_gates = jnp.sum(grad_states[:, None, :] * routed.astype(jnp.float32), axis=-1)
    grad_outgoing = jnp.where(filled[:, None], grad_routed[route_clip], jnp.zeros((), jnp.bfloat16))
    grad_outgoing = grad_outgoing.reshape(experts_all, CAP, model_width)
    grad_result = lax.all_to_all(grad_outgoing, "expert", split_axis=0, concat_axis=1, tiled=True)
    in_full, out_full = (
        lax.all_gather(in_shard, "shard", axis=1, tiled=True),
        lax.all_gather(out_shard, "shard", axis=1, tiled=True),
    )
    hidden_pre = jnp.einsum("erd,edh->erh", arrived, in_full, preferred_element_type=jnp.float32)
    activated, gelu_pullback = jax.vjp(jax.nn.gelu, hidden_pre)
    grad_out_experts = jnp.einsum(
        "erh,erd->ehd",
        activated.astype(jnp.bfloat16),
        grad_result,
        preferred_element_type=jnp.float32,
    )
    grad_activated = jnp.einsum(
        "erd,ehd->erh", grad_result, out_full, preferred_element_type=jnp.float32
    )
    grad_pre = gelu_pullback(grad_activated)[0].astype(jnp.bfloat16)
    grad_in_experts = jnp.einsum(
        "erd,erh->edh", arrived, grad_pre, preferred_element_type=jnp.float32
    )
    grad_arrived = jnp.einsum(
        "erh,edh->erd", grad_pre, in_full, preferred_element_type=jnp.float32
    ).astype(jnp.bfloat16)
    grad_returned = lax.all_to_all(grad_arrived, "expert", split_axis=1, concat_axis=0, tiled=True)
    grad_in_share, grad_out_share = (
        lax.psum_scatter(
            grad_in_experts.astype(jnp.bfloat16), "shard", scatter_dimension=1, tiled=True
        ).astype(jnp.float32),
        lax.psum_scatter(
            grad_out_experts.astype(jnp.bfloat16), "shard", scatter_dimension=1, tiled=True
        ).astype(jnp.float32),
    )
    grad_routes = grad_returned.reshape(experts_all * CAP, model_width)[slot_index]
    grad_normed = jnp.sum(
        grad_routes.reshape(row_count, TOP, model_width).astype(jnp.float32), axis=1
    )
    grad_chances = jnp.sum(jnp.where(matches, grad_gates[:, :, None], 0.0), axis=1)
    grad_logits = chances * (grad_chances - jnp.sum(grad_chances * chances, axis=-1, keepdims=True))
    grad_logits = grad_logits.astype(jnp.bfloat16)
    grad_router = jnp.einsum("rd,re->de", normed, grad_logits, preferred_element_type=jnp.float32)
    grad_normed = grad_normed + jnp.einsum(
        "re,de->rd", grad_logits, router_full, preferred_element_type=jnp.float32
    )
    unused_value, norm_pullback = jax.vjp(layer_norm, current, gain_row, shift_row)
    grad_input, grad_gain, grad_shift = norm_pullback(grad_normed)
    return (
        grad_states + grad_input,
        grad_router,
        grad_gain,
        grad_shift,
        grad_in_share,
        grad_out_share,
    )


def shards(
    states,
    qkv_weight,
    out_weight,
    norm_gain,
    norm_bias,
    router_weight,
    expert_in,
    expert_out,
    chosen,
    image_count,
    teacher,
):
    qkv_full, out_full, gain_full, bias_full, router_full = (
        lax.all_gather(qkv_weight, "shard", axis=1, tiled=True),
        lax.all_gather(out_weight, "shard", axis=1, tiled=True),
        lax.all_gather(norm_gain, "shard", axis=1, tiled=True),
        lax.all_gather(norm_bias, "shard", axis=1, tiled=True),
        lax.all_gather(router_weight, "shard", axis=1, tiled=True),
    )
    gain_float = gain_full.astype(jnp.float32)
    bias_float = bias_full.astype(jnp.float32)
    layer_count = qkv_weight.shape[0]
    row_count, model_width = states.shape
    slot_image = jnp.arange(row_count, dtype=jnp.int32) // SEQ
    living = slot_image < image_count[0]
    counted = lax.psum(image_count[0].astype(jnp.float32) * SEQ, ("expert", "shard"))
    current = states.astype(jnp.float32)
    attention_kept = []
    mixture_kept = []
    for layer_index in range(layer_count):
        current, kept_attention = attention_forward(
            current,
            qkv_full[layer_index],
            out_full[layer_index],
            gain_float[layer_index, :, 0],
            bias_float[layer_index, :, 0],
        )
        current, kept_mixture = mixture_forward(
            current,
            gain_float[layer_index, :, 1],
            bias_float[layer_index, :, 1],
            router_full[layer_index],
            expert_in[layer_index],
            expert_out[layer_index],
            chosen[layer_index],
        )
        attention_kept.append(kept_attention)
        mixture_kept.append(kept_mixture)
    missed = current - teacher.astype(jnp.float32)
    grad_states = jnp.where(living[:, None], 2.0 * missed, 0.0) / counted
    qkv_list = [None] * layer_count
    out_list = [None] * layer_count
    gain_list = [None] * layer_count
    bias_list = [None] * layer_count
    router_list = [None] * layer_count
    in_list = [None] * layer_count
    experts_out_list = [None] * layer_count
    for layer_index in reversed(range(layer_count)):
        grad_states, grad_router, gain_second, shift_second, grad_in_share, grad_out_share = (
            mixture_backward(
                grad_states,
                mixture_kept[layer_index],
                gain_float[layer_index, :, 1],
                bias_float[layer_index, :, 1],
                router_full[layer_index],
                expert_in[layer_index],
                expert_out[layer_index],
            )
        )
        grad_states, grad_qkv, grad_out, gain_first, shift_first = attention_backward(
            grad_states,
            attention_kept[layer_index],
            qkv_full[layer_index],
            out_full[layer_index],
            gain_float[layer_index, :, 0],
            bias_float[layer_index, :, 0],
        )
        qkv_list[layer_index] = grad_qkv
        out_list[layer_index] = grad_out
        gain_list[layer_index] = jnp.stack([gain_first, gain_second], axis=-1)
        bias_list[layer_index] = jnp.stack([shift_first, shift_second], axis=-1)
        router_list[layer_index] = grad_router
        in_list[layer_index] = grad_in_share
        experts_out_list[layer_index] = grad_out_share
    mixer_grads = (
        jnp.stack(qkv_list),
        jnp.stack(out_list),
        jnp.stack(gain_list),
        jnp.stack(bias_list),
        jnp.stack(router_list),
    )
    summed = lax.psum(
        (mixer_grads[0], mixer_grads[1], mixer_grads[2], mixer_grads[3], mixer_grads[4]),
        ("expert", "shard"),
    )
    share_width = model_width // lax.axis_size("shard")
    start_index = lax.axis_index("shard") * share_width
    reduced = tuple(
        (lax.dynamic_slice_in_dim(member, start_index, share_width, 1) for member in summed)
    )
    return (
        current.astype(jnp.bfloat16),
        grad_states * counted,
        reduced[0],
        reduced[1],
        reduced[2],
        reduced[3],
        reduced[4],
        jnp.stack(in_list),
        jnp.stack(experts_out_list),
    )


def pad_rows(values, fill=0):
    width = values.shape[-1]
    images = values.reshape(SLOTS, SEQ, width)
    images = jnp.pad(images, ((0, 0), (0, SEQ_PAD - SEQ), (0, 0)), constant_values=fill)
    images = images.reshape(SLOTS * SEQ_PAD, width)
    return jnp.pad(images, ((0, ROWS - SLOTS * SEQ_PAD), (0, 0)), constant_values=fill)


def live_rows(values):
    images = values[: SLOTS * SEQ_PAD].reshape(SLOTS, SEQ_PAD, values.shape[-1])
    return images[:, :SEQ].reshape(SLOTS * SEQ, values.shape[-1])


def exchange(rows):
    blocks = rows.reshape(EXPERTS, CAP_PAD, rows.shape[-1])
    moved = lax.all_to_all(blocks, ("expert", "shard"), split_axis=0, concat_axis=0, tiled=True)
    return moved.reshape(rows.shape)


def own_expert(shard_part):
    moved = lax.all_to_all(shard_part, "shard", split_axis=0, concat_axis=0, tiled=True)
    return moved.reshape(-1, shard_part.shape[-1])


def share_expert(grad):
    shards_all = lax.axis_size("shard")
    blocks = grad.reshape(shards_all, grad.shape[0] // shards_all, grad.shape[1])
    moved = lax.all_to_all(blocks, "shard", split_axis=0, concat_axis=0, tiled=True)
    return moved.astype(F32)


def owners(
    states,
    qkv_weight,
    out_weight,
    norm_gain,
    norm_bias,
    router_weight,
    expert_in,
    expert_out,
    chosen,
    image_count,
    teacher,
):
    layers, share, _ = qkv_weight.shape
    model = states.shape[1]
    groups = lax.axis_size("expert")
    piece = share // groups
    spare = LANES - EXPERTS - 5
    marks = jnp.zeros((layers, share, 1 + spare), BF16)
    packed = jnp.concatenate(
        [qkv_weight, out_weight, router_weight, norm_gain, norm_bias, marks], axis=2
    )
    packed = lax.dynamic_slice_in_dim(packed, lax.axis_index("expert") * piece, piece, 1)
    mark_at = 4 * model + EXPERTS + 4
    packed = packed.at[0, 0, mark_at].set(image_count[0].astype(BF16))
    weights = [
        lax.all_gather(packed[layer], ("shard", "expert"), axis=0, tiled=True)
        for layer in range(layers)
    ]
    experts = [(own_expert(expert_in[layer]), own_expert(expert_out[layer])) for layer in range(layers)]
    counted = jnp.sum(weights[0][:, mark_at].astype(F32)) * SEQ
    slot_image = jnp.arange(states.shape[0], dtype=jnp.int32) // SEQ
    living = slot_image < image_count[0]
    scale = pad_rows(jnp.where(living, 2.0 / counted, 0.0)[:, None])
    picks = [
        jnp.pad(pad_rows(chosen[layer], -1), ((0, 0), (0, LANES - TOP)), constant_values=-1)
        for layer in range(layers)
    ]
    kept = []
    current = pad_rows(states.astype(F32))
    fronts = run_first(current, weights[0], picks[0])
    for layer in range(layers):
        x1, proj, logs, att, slots, turned, chances, gates, leaving = fronts
        arrived = exchange(leaving)
        made, act, slope = run_expert(arrived, *experts[layer])
        returned = exchange(made)
        entry = [current, x1, proj, logs, att, slots, turned, chances, gates, arrived, act, slope, None]
        kept.append(entry)
        if layer + 1 < layers:
            current, entry[12], *fronts = run_middle(
                x1, gates, slots, returned, weights[layer + 1], picks[layer + 1]
            )
    final, grad, grad_gates, leaving = run_last(
        x1, gates, slots, turned, returned, pad_rows(teacher), scale
    )
    smalls, ins, outs = [None] * layers, [None] * layers, [None] * layers
    for layer in reversed(range(layers)):
        current, x1, proj, logs, att, slots, turned, chances, gates, arrived, act, slope, _ = kept[layer]
        came = exchange(leaving)
        back_rows, grad_in, grad_out = run_expert_back(arrived, came, act, slope, *experts[layer])
        returned = exchange(back_rows)
        ins[layer], outs[layer] = share_expert(grad_in), share_expert(grad_out)
        common = (grad, returned, slots, picks[layer], grad_gates, chances, x1, current, proj, logs, att, weights[layer])
        if layer > 0:
            below = kept[layer - 1]
            grad, small, grad_gates, leaving = run_back_middle(*common, below[8], below[12], below[6])
        else:
            grad, small = run_back(*common)
        part = lax.psum_scatter(small, ("shard", "expert"), scatter_dimension=0, tiled=True)
        smalls[layer] = lax.all_gather(part, "expert", axis=0, tiled=True)
    small = jnp.stack(smalls)
    at = 4 * model
    return (
        live_rows(final),
        live_rows(grad) * counted,
        small[:, :, : 3 * model],
        small[:, :, 3 * model : at],
        small[:, :, at + EXPERTS : at + EXPERTS + 2],
        small[:, :, at + EXPERTS + 2 : at + EXPERTS + 4],
        small[:, :, at : at + EXPERTS],
        jnp.stack(ins),
        jnp.stack(outs),
    )


def plan_of(mesh):
    groups, shards_all = mesh.shape["expert"], mesh.shape["shard"]
    return owners if groups * shards_all == EXPERTS else shards


def solution(mesh):
    in_specs = (
        P(("expert", "shard"), None),
        P(None, "shard", None),
        P(None, "shard", None),
        P(None, "shard", None),
        P(None, "shard", None),
        P(None, "shard", None),
        P(None, "expert", "shard", None),
        P(None, "expert", "shard", None),
        P(None, ("expert", "shard"), None),
        P(("expert", "shard")),
        P(("expert", "shard"), None),
    )
    out_specs = (
        P(("expert", "shard"), None),
        P(("expert", "shard"), None),
        P(None, "shard", None),
        P(None, "shard", None),
        P(None, "shard", None),
        P(None, "shard", None),
        P(None, "shard", None),
        P(None, "expert", "shard", None),
        P(None, "expert", "shard", None),
    )
    return jax.shard_map(plan_of(mesh), mesh=mesh, in_specs=in_specs, out_specs=out_specs, check_vma=False)
```

```python
import functools
import jax
import jax.numpy as jnp
from jax import lax
from jax.experimental import pallas as pl
from jax.experimental.pallas import tpu as pltpu
from jax.sharding import PartitionSpec as P

HEADS = 8
HEAD_DIM = 64
EXPERTS = 32
TOP = 2
SEQ = 197
SLOTS = 3
CAP = 74
norm_eps = 1e-06

LANES = 128
SEQ_PAD = 208
ROWS = 640
CAP_PAD = 80
CHUNK = 64
SHARDS = 4
LIMIT = 62 << 20
F32 = jnp.float32
BF16 = jnp.bfloat16


def dot(a, b):
    return jnp.dot(a, b, preferred_element_type=F32)


def dot_nt(a, b):
    return lax.dot_general(a, b, (((1,), (1,)), ((), ())), preferred_element_type=F32)


def dot_tn(a, b):
    return lax.dot_general(a, b, (((0,), (0,)), ((), ())), preferred_element_type=F32)


def rows_of(step, size):
    return pl.ds(pl.multiple_of(step * size, size), size)


def each_chunk(body, size=CHUNK, total=ROWS):
    def step(i, carry):
        body(rows_of(i, size))
        return carry

    lax.fori_loop(0, total // size, step, 0)


def centre(values):
    centred = values - jnp.mean(values, axis=-1, keepdims=True)
    spread = jnp.mean(centred * centred, axis=-1, keepdims=True)
    return centred, lax.rsqrt(spread + norm_eps)


def norm_rows(x_ref, gain, shift, out_ref):
    def body(rows):
        centred, inverse = centre(x_ref[rows, :])
        out_ref[rows, :] = (centred * inverse * gain + shift).astype(BF16)

    each_chunk(body)


def norm_pullback(x_ref, gain, grad_ref, total_ref, out_ref, sums_ref):
    sums_ref[...] = jnp.zeros_like(sums_ref)

    def body(rows):
        centred, inverse = centre(x_ref[rows, :])
        unit = centred * inverse
        grad = grad_ref[rows, :]
        scaled = grad * gain
        first = jnp.mean(scaled, axis=-1, keepdims=True)
        second = jnp.mean(scaled * unit, axis=-1, keepdims=True)
        out_ref[rows, :] = total_ref[rows, :] + inverse * (scaled - first - unit * second)
        sums_ref[0:1, :] += jnp.sum(grad * unit, axis=0, keepdims=True)
        sums_ref[1:2, :] += jnp.sum(grad, axis=0, keepdims=True)

    each_chunk(body)


def weight_parts(w_ref, model):
    side = jnp.transpose(w_ref[:, 4 * model :].astype(F32))
    return [side[EXPERTS + i : EXPERTS + i + 1, :] for i in range(4)]


def attention_rows(x_ref, w_ref, gain, shift, x1_ref, proj_ref, log_ref, att_ref, normed_ref):
    model = x_ref.shape[1]
    norm_rows(x_ref, gain, shift, normed_ref)
    for part in range(3):
        columns = slice(part * model, (part + 1) * model)
        proj_ref[:, columns] = dot(normed_ref[...], w_ref[:, columns]).astype(BF16)
    att_ref[...] = jnp.zeros_like(att_ref)
    log_ref[...] = jnp.zeros_like(log_ref)
    low = lax.broadcasted_iota(jnp.int32, (SEQ_PAD, LANES), 1) < HEAD_DIM
    inside = lax.broadcasted_iota(jnp.int32, (SEQ_PAD, SEQ_PAD), 1) < SEQ
    lane = lax.broadcasted_iota(jnp.int32, (SEQ_PAD, LANES), 1)

    def image(i, carry):
        rows = rows_of(i, SEQ_PAD)
        logs = jnp.zeros((SEQ_PAD, LANES), F32)
        for pair in range(HEADS // 2):
            at = pair * LANES
            queries = proj_ref[rows, at : at + LANES]
            keys = proj_ref[rows, model + at : model + at + LANES]
            values = proj_ref[rows, 2 * model + at : 2 * model + at + LANES]
            results = []
            for side in range(2):
                mine = low if side == 0 else jnp.logical_not(low)
                masked = jnp.where(mine, queries, jnp.zeros_like(queries))
                scores = dot_nt(masked, keys) * HEAD_DIM ** (-0.5)
                scores = jnp.where(inside, scores, -1e30)
                highest = jnp.max(scores, axis=-1, keepdims=True)
                exponent = jnp.exp(scores - highest)
                summed = jnp.sum(exponent, axis=-1, keepdims=True)
                weights = (exponent / summed).astype(BF16)
                logs = jnp.where(lane == 2 * pair + side, highest + jnp.log(summed), logs)
                results.append(dot(weights, values))
            att_ref[rows, at : at + LANES] = jnp.where(low, results[0], results[1]).astype(BF16)
        log_ref[rows, :] = logs
        return carry

    lax.fori_loop(0, SLOTS, image, 0)
    x1_ref[...] = x_ref[...] + dot(att_ref[...], w_ref[:, 3 * model : 4 * model])


def route_rows(picks, slots_ref, turned_ref):
    lane = lax.broadcasted_iota(jnp.int32, (ROWS, LANES), 1)
    firsts, seconds = picks[:, 0:1], picks[:, 1:2]
    place_first, place_second = picks[:, 2:3], picks[:, 3:4]
    match_first, match_second = lane == firsts, lane == seconds
    either = jnp.where(match_first | match_second, 1.0, 0.0).astype(BF16)
    down = lax.broadcasted_iota(jnp.int32, (ROWS, ROWS), 0)
    across = lax.broadcasted_iota(jnp.int32, (ROWS, ROWS), 1)
    before = dot(jnp.where(across < down, 1.0, 0.0).astype(BF16), either)
    rank_first = jnp.sum(jnp.where(match_first, before, 0.0), axis=-1, keepdims=True)
    rank_second = jnp.sum(jnp.where(match_second, before, 0.0), axis=-1, keepdims=True)
    slot_first = jnp.where(place_first < 0, -1.0, place_first.astype(F32) * CAP_PAD + rank_first)
    slot_second = jnp.where(place_second < 0, -1.0, place_second.astype(F32) * CAP_PAD + rank_second)
    both = jnp.where(lane == 0, slot_first, jnp.where(lane == 1, slot_second, -1.0))
    slots_ref[...] = both.astype(jnp.int32)
    turned_ref[...] = jnp.transpose(both)[0:8, :].astype(jnp.int32)


def gate_rows(normed_ref, router_ref, picks, chances_ref, gates_ref):
    lane = lax.broadcasted_iota(jnp.int32, (ROWS, LANES), 1)
    logits = dot(normed_ref[...], router_ref[...])
    logits = jnp.where(lane < EXPERTS, logits, -1e30)
    exponent = jnp.exp(logits - jnp.max(logits, axis=-1, keepdims=True))
    chances = exponent / jnp.sum(exponent, axis=-1, keepdims=True)
    if chances_ref is not None:
        chances_ref[...] = chances
    gate_first = jnp.sum(jnp.where(lane == picks[:, 0:1], chances, 0.0), axis=-1, keepdims=True)
    gate_second = jnp.sum(jnp.where(lane == picks[:, 1:2], chances, 0.0), axis=-1, keepdims=True)
    gates_ref[...] = jnp.where(lane == 0, gate_first, jnp.where(lane == 1, gate_second, 0.0))


PLACES = EXPERTS // 2
GROUP = 4
BLOCK = GROUP * CAP_PAD
HALF = PLACES * CAP_PAD


def pick_block(turned_ref, group):
    slot = lax.broadcasted_iota(jnp.int32, (BLOCK, ROWS), 0) + group * BLOCK
    return slot == turned_ref[0:1, :], slot == turned_ref[1:2, :]


def as_weights(mask):
    return jnp.where(mask, 1.0, 0.0).astype(BF16)


def dispatch_block(turned_ref, rows_ref, group):
    first, second = pick_block(turned_ref, group)
    return dot(as_weights(first | second), rows_ref[...]).astype(BF16)


def dispatch_pair_block(turned_ref, pairs_ref, group):
    first, second = pick_block(turned_ref, group)
    both = jnp.concatenate([as_weights(first), as_weights(second)], axis=1)
    return dot(both, pairs_ref[...]).astype(BF16)


def rows_at(ref, lead, group):
    block = ref[(*lead, pl.ds(group * GROUP, GROUP))]
    return block.reshape(BLOCK, block.shape[-1])


def collect_pairs(slots_ref, found_ref, side, total_ref):
    for group in range(PLACES // GROUP):
        slot = lax.broadcasted_iota(jnp.int32, (ROWS, BLOCK), 1) + group * BLOCK
        rows = rows_at(found_ref, (side,), group)
        for which in range(TOP):
            part = dot(as_weights(slot == slots_ref[:, which : which + 1]), rows)
            to = slice(which * ROWS, (which + 1) * ROWS)
            if group == 0:
                total_ref[to, :] = part
            else:
                total_ref[to, :] += part


def collect_sums(slots_ref, found_ref, side, total_ref):
    for group in range(PLACES // GROUP):
        slot = lax.broadcasted_iota(jnp.int32, (ROWS, BLOCK), 1) + group * BLOCK
        chosen = (slot == slots_ref[:, 0:1]) | (slot == slots_ref[:, 1:2])
        part = dot(as_weights(chosen), rows_at(found_ref, (side,), group))
        if group == 0:
            total_ref[...] = part
        else:
            total_ref[...] += part


def later_rows(rows):
    return pl.ds(pl.multiple_of(rows.start + ROWS, CHUNK), CHUNK)


def gated_sums(gates_ref, total_ref, routed_ref, side, out_ref):
    def body(rows):
        later = later_rows(rows)
        first, second = total_ref[rows, :], total_ref[later, :]
        gates = gates_ref[side, rows, :]
        out_ref[rows, :] = (gates[:, 0:1] * first + gates[:, 1:2] * second).astype(out_ref.dtype)
        routed_ref[side, rows, :] = first.astype(BF16)
        routed_ref[side, later, :] = second.astype(BF16)

    each_chunk(body)


def gate_grads(grad_ref, gates_ref, routed_ref, side, pairs_ref, grad_gates_ref):
    lane = lax.broadcasted_iota(jnp.int32, (LANES, LANES), 1)

    def body(i, carry):
        rows = rows_of(i, LANES)
        later = pl.ds(pl.multiple_of(i * LANES + ROWS, LANES), LANES)
        grad = grad_ref[rows, :].astype(F32)
        gates = gates_ref[side, rows, :]
        pairs_ref[rows, :] = (gates[:, 0:1] * grad).astype(BF16)
        pairs_ref[later, :] = (gates[:, 1:2] * grad).astype(BF16)
        first = jnp.sum(grad * routed_ref[side, rows, :].astype(F32), axis=-1, keepdims=True)
        second = jnp.sum(grad * routed_ref[side, later, :].astype(F32), axis=-1, keepdims=True)
        both = jnp.where(lane == 0, first, jnp.where(lane == 1, second, 0.0))
        grad_gates_ref[:, rows] = jnp.transpose(both)[0:8, :]
        return carry

    lax.fori_loop(0, ROWS // LANES, body, 0)


def attention_pullback(grad_ref, w_ref, proj_ref, log_ref, att_ref, normed_ref, small_ref, gproj_ref, gatt_ref, back_ref, gnormed_ref):
    model = grad_ref.shape[1]

    def body(rows):
        back_ref[rows, :] = grad_ref[rows, :].astype(BF16)

    each_chunk(body)
    small_ref[:, 3 * model : 4 * model] = dot_tn(att_ref[...], back_ref[...])
    gatt_ref[...] = dot_nt(back_ref[...], w_ref[:, 3 * model : 4 * model]).astype(BF16)
    gproj_ref[SLOTS * SEQ_PAD :, :] = jnp.zeros((ROWS - SLOTS * SEQ_PAD, 3 * model), BF16)
    low = lax.broadcasted_iota(jnp.int32, (SEQ_PAD, LANES), 1) < HEAD_DIM
    inside = lax.broadcasted_iota(jnp.int32, (SEQ_PAD, SEQ_PAD), 1) < SEQ
    scaling = HEAD_DIM ** (-0.5)

    def image(i, carry):
        rows = rows_of(i, SEQ_PAD)
        for pair in range(HEADS // 2):
            at = pair * LANES
            queries = proj_ref[rows, at : at + LANES]
            keys = proj_ref[rows, model + at : model + at + LANES]
            values = proj_ref[rows, 2 * model + at : 2 * model + at + LANES]
            grad_heads = gatt_ref[rows, at : at + LANES]
            parts = []
            for side in range(2):
                mine = low if side == 0 else jnp.logical_not(low)
                zero = jnp.zeros_like(queries)
                head = 2 * pair + side
                scores = dot_nt(jnp.where(mine, queries, zero), keys) * scaling
                chances = jnp.where(inside, jnp.exp(scores - log_ref[rows, head : head + 1]), 0.0)
                grad_weights = dot_nt(jnp.where(mine, grad_heads, zero), values)
                centre_term = jnp.sum(grad_weights * chances, axis=-1, keepdims=True)
                grad_scores = (chances * (grad_weights - centre_term)).astype(BF16)
                parts.append(
                    (
                        dot(grad_scores, keys) * scaling,
                        dot_tn(grad_scores, queries) * scaling,
                        dot_tn(chances.astype(BF16), grad_heads),
                    )
                )
            for which in range(3):
                to = which * model + at
                gproj_ref[rows, to : to + LANES] = jnp.where(low, parts[0][which], parts[1][which]).astype(BF16)
        return carry

    lax.fori_loop(0, SLOTS, image, 0)
    for part in range(3):
        columns = slice(part * model, (part + 1) * model)
        small_ref[:, columns] = dot_tn(normed_ref[...], gproj_ref[:, columns])
    gnormed_ref[...] = dot_nt(gproj_ref[...], w_ref[:, : 3 * model])


def router_pullback(grad_gates_ref, picks_ref, chances_ref, w_ref, normed_ref, gnormed_ref, router_ref):
    model = normed_ref.shape[1]
    lane = lax.broadcasted_iota(jnp.int32, (ROWS, LANES), 1)
    picks, chances = picks_ref[...], chances_ref[...]
    turned = jnp.concatenate([grad_gates_ref[...], jnp.zeros((LANES - 8, ROWS), F32)], axis=0)
    grads = jnp.transpose(turned)
    spread = jnp.where(lane == picks[:, 0:1], grads[:, 0:1], 0.0) + jnp.where(lane == picks[:, 1:2], grads[:, 1:2], 0.0)
    logits = chances * (spread - jnp.sum(spread * chances, axis=-1, keepdims=True))
    logits = logits.astype(BF16)
    router_ref[...] = dot_tn(normed_ref[...], logits)
    gnormed_ref[...] += dot_nt(logits, w_ref[:, 4 * model :])


MESH = pl.DeviceIdType.MESH


def position():
    group, shard = lax.axis_index("expert"), lax.axis_index("shard")
    low = shard % 2
    return group, shard, low, group * 2 + low


def place_id(step):
    group, shard, low, me = position()
    there = (me + step + PLACES) % PLACES
    return (there // 2, shard - low + there % 2)


def twin_id():
    group, shard, _, _ = position()
    return (group, (shard + 2) % SHARDS)


def meet():
    barrier = pltpu.get_barrier_semaphore()
    for k in range(1, PLACES):
        pl.semaphore_signal(barrier, inc=1, device_id=place_id(k), device_id_type=MESH)
    pl.semaphore_signal(barrier, inc=1, device_id=twin_id(), device_id_type=MESH)
    pl.semaphore_wait(barrier, PLACES)


def to_twin(src, dst, sems, at):
    return pltpu.make_async_remote_copy(
        src_ref=src, dst_ref=dst, send_sem=sems.at[0, at], recv_sem=sems.at[1, at], device_id=twin_id(), device_id_type=MESH
    )


def block_copy(src, dst, sems, lane, side, k, sign):
    if k == 0:
        return pltpu.make_async_copy(src.at[side, 0], dst.at[side, 0], sems.at[lane, 1, side, 0])
    return pltpu.make_async_remote_copy(
        src_ref=src.at[side, k],
        dst_ref=dst.at[side, k],
        send_sem=sems.at[lane, 0, side, k],
        recv_sem=sems.at[lane, 1, side, k],
        device_id=place_id(sign * k),
        device_id_type=MESH,
    )


def start_blocks(src, dst, sems, lane, side, blocks, sign):
    for k in blocks:
        block_copy(src, dst, sems, lane, side, k, sign).start()


def await_blocks(src, dst, sems, lane, side, blocks, sign):
    for k in blocks:
        copy = block_copy(src, dst, sems, lane, side, k, sign)
        copy.wait() if k == 0 else copy.wait_recv()


def await_sent(src, dst, sems, lane, side, sign):
    for k in range(1, PLACES):
        block_copy(src, dst, sems, lane, side, k, sign).wait_send()


def spread(make_block, src, dst, sems, side):
    for group in range(PLACES // GROUP):
        src[side, group * GROUP : (group + 1) * GROUP] = make_block(group).reshape(GROUP, CAP_PAD, src.shape[-1])
        if group:
            start_blocks(src, dst, sems, 0, side, range((group - 1) * GROUP, group * GROUP), 1)
    start_blocks(src, dst, sems, 0, side, range(PLACES - GROUP, PLACES), 1)


TILE_PLACES = 8
TILE = TILE_PLACES * CAP_PAD
TILES = PLACES // TILE_PLACES
WIDE = 512
ROOT = 0.7978845608028654
CUBE = 0.044715


def mix_kernel(
    normed_ref, router_ref, mine_ref, theirs_ref, in_hbm, out_hbm,
    delta_ref, slots_ref, turned_ref, chances_ref, gates_ref, arrived_ref, routed_ref, act_hbm, slope_hbm,
    twin_rows, leaving, made, returned, total, twin_sum, other, act_ref, slope_ref, in_ref, out_ref,
    sems, twin_sems, load_sems, save_sems,
):
    loads = [pltpu.make_async_copy(in_hbm, in_ref, load_sems.at[0]), pltpu.make_async_copy(out_hbm, out_ref, load_sems.at[1])]
    for load in loads:
        load.start()
    meet()
    rows_copy = to_twin(normed_ref, twin_rows, twin_sems, 0)
    rows_copy.start()
    route_rows(mine_ref[...], slots_ref.at[0], turned_ref.at[0])
    spread(lambda group: dispatch_block(turned_ref.at[0], normed_ref, group), leaving, arrived_ref, sems, 0)
    route_rows(theirs_ref[...], slots_ref.at[1], turned_ref.at[1])
    gate_rows(normed_ref, router_ref, mine_ref[...], chances_ref, gates_ref.at[0])
    rows_copy.wait_recv()
    spread(lambda group: dispatch_block(turned_ref.at[1], twin_rows, group), leaving, arrived_ref, sems, 1)
    gate_rows(twin_rows, router_ref, theirs_ref[...], None, gates_ref.at[1])
    for load in loads:
        load.wait()

    def saves(slot, side, tile):
        to = pl.ds((side * TILES + tile) * TILE, TILE)
        return [
            pltpu.make_async_copy(act_ref.at[slot], act_hbm.at[to, :], save_sems.at[0, slot]),
            pltpu.make_async_copy(slope_ref.at[slot], slope_hbm.at[to, :], save_sems.at[1, slot]),
        ]

    for side in range(2):
        for tile in range(TILES):
            slot = tile % 2
            blocks = range(tile * TILE_PLACES, (tile + 1) * TILE_PLACES)
            await_blocks(leaving, arrived_ref, sems, 0, side, blocks, 1)
            if side:
                for save in saves(slot, 0, tile):
                    save.wait()
            rows = arrived_ref[side, tile * TILE_PLACES : (tile + 1) * TILE_PLACES].reshape(TILE, -1)

            def chunk(i, carry):
                columns = rows_of(i, WIDE)
                pre = dot(rows, in_ref[:, columns])
                square = pre * pre
                bend = jnp.tanh(pre * (ROOT + ROOT * CUBE * square))
                half = 0.5 + 0.5 * bend
                act = (pre * half).astype(BF16)
                slope = half + (0.5 * pre) * (1.0 - bend * bend) * (ROOT + 3.0 * ROOT * CUBE * square)
                act_ref[slot, :, columns] = act
                slope_ref[slot, :, columns] = slope.astype(BF16)
                return carry

            lax.fori_loop(0, in_ref.shape[1] // WIDE, chunk, 0)
            result = dot(act_ref[slot], out_ref[...]).astype(BF16)
            made[side, tile * TILE_PLACES : (tile + 1) * TILE_PLACES] = result.reshape(TILE_PLACES, CAP_PAD, -1)
            for save in saves(slot, side, tile):
                save.start()
            start_blocks(made, returned, sems, 1, side, blocks, -1)
    await_blocks(made, returned, sems, 1, 1, range(PLACES), -1)
    collect_pairs(slots_ref.at[1], returned, 1, total)
    gated_sums(gates_ref, total, routed_ref, 1, twin_sum)
    sum_copy = to_twin(twin_sum, other, twin_sems, 1)
    sum_copy.start()
    await_blocks(made, returned, sems, 1, 0, range(PLACES), -1)
    collect_pairs(slots_ref.at[0], returned, 0, total)
    gated_sums(gates_ref, total, routed_ref, 0, delta_ref)
    for tile in range(TILES):
        for save in saves(tile % 2, 1, tile):
            save.wait()
    for side in range(2):
        await_sent(leaving, arrived_ref, sems, 0, side, 1)
        await_sent(made, returned, sems, 1, side, -1)
    rows_copy.wait_send()
    sum_copy.wait()

    def body(rows):
        delta_ref[rows, :] += other[rows, :].astype(F32)

    each_chunk(body)


def in_vmem(count):
    return [pl.BlockSpec(memory_space=pltpu.VMEM)] * count


def anywhere(count):
    return [pl.BlockSpec(memory_space=pl.ANY)] * count


def blocks_of(model):
    return pltpu.VMEM((2, PLACES, CAP_PAD, model), BF16)


def run_mix(normed, router, mine, theirs, weight_in, weight_out):
    model, hidden = weight_in.shape
    outs = [
        shape((ROWS, model), F32),
        shape((2, ROWS, LANES), jnp.int32),
        shape((2, 8, ROWS), jnp.int32),
        shape((ROWS, LANES), F32),
        shape((2, ROWS, LANES), F32),
        shape((2, PLACES, CAP_PAD, model), BF16),
        shape((2, TOP * ROWS, model), BF16),
        shape((2 * HALF, hidden), BF16),
        shape((2 * HALF, hidden), BF16),
    ]
    return pl.pallas_call(
        mix_kernel,
        out_shape=outs,
        in_specs=in_vmem(4) + anywhere(2),
        out_specs=in_vmem(7) + anywhere(2),
        scratch_shapes=[
            pltpu.VMEM((ROWS, model), BF16),
            blocks_of(model),
            blocks_of(model),
            blocks_of(model),
            pltpu.VMEM((TOP * ROWS, model), F32),
            pltpu.VMEM((ROWS, model), BF16),
            pltpu.VMEM((ROWS, model), BF16),
            pltpu.VMEM((2, TILE, hidden), BF16),
            pltpu.VMEM((2, TILE, hidden), BF16),
            pltpu.VMEM((model, hidden), BF16),
            pltpu.VMEM((hidden, model), BF16),
            pltpu.SemaphoreType.DMA((2, 2, 2, PLACES)),
            pltpu.SemaphoreType.DMA((2, 2)),
            pltpu.SemaphoreType.DMA((2,)),
            pltpu.SemaphoreType.DMA((2, 2)),
        ],
        compiler_params=pltpu.CompilerParams(vmem_limit_bytes=LIMIT, collective_id=1, has_side_effects=True),
        name="mix",
    )(normed, router, mine, theirs, weight_in, weight_out)


def unmix_kernel(
    grad_ref, sent_ref, gates_ref, routed_ref, slots_ref, turned_ref, arrived_hbm, act_hbm, slope_hbm, in_hbm, out_hbm,
    sums_ref, grad_gates_ref, gin_ref, gout_ref,
    twin_rows, leaving, came, made, returned, pairs, twin_sum, other, twin_gates, other_gates, pre_ref, slope_ref, act_ref, arrived_ref, in_ref, out_ref,
    sems, twin_sems, load_sems, slope_sems, act_sems,
):
    loads = [
        pltpu.make_async_copy(src, dst, load_sems.at[i])
        for i, (src, dst) in enumerate(((in_hbm, in_ref), (out_hbm, out_ref), (arrived_hbm, arrived_ref)))
    ]
    for load in loads:
        load.start()

    def slopes(side, tile):
        at = pl.ds((side * TILES + tile) * TILE, TILE)
        return pltpu.make_async_copy(slope_hbm.at[at, :], slope_ref.at[tile % 2], slope_sems.at[tile % 2])

    def acts(chunk):
        return pltpu.make_async_copy(act_hbm.at[:, pl.ds(chunk * WIDE, WIDE)], act_ref.at[chunk % 2], act_sems.at[chunk % 2])

    for tile in range(TILES):
        slopes(0, tile).start()
    for chunk in range(2):
        acts(chunk).start()
    meet()
    rows_copy = to_twin(sent_ref, twin_rows, twin_sems, 0)
    rows_copy.start()
    gate_grads(grad_ref, gates_ref, routed_ref, 0, pairs, grad_gates_ref)
    spread(lambda group: dispatch_pair_block(turned_ref.at[0], pairs, group), leaving, came, sems, 0)
    rows_copy.wait_recv()
    gate_grads(twin_rows, gates_ref, routed_ref, 1, pairs, twin_gates)
    gates_copy = to_twin(twin_gates, other_gates, twin_sems, 2)
    spread(lambda group: dispatch_pair_block(turned_ref.at[1], pairs, group), leaving, came, sems, 1)
    gates_copy.start()
    for load in loads:
        load.wait()
    hidden = in_ref.shape[1]
    for side in range(2):
        for tile in range(TILES):
            blocks = range(tile * TILE_PLACES, (tile + 1) * TILE_PLACES)
            await_blocks(leaving, came, sems, 0, side, blocks, 1)
            slopes(side, tile).wait()
            rows = came[side, tile * TILE_PLACES : (tile + 1) * TILE_PLACES].reshape(TILE, -1)
            at = (side * TILES + tile) * TILE

            def chunk(i, carry):
                columns = rows_of(i, WIDE)
                grad_act = dot_nt(rows, out_ref[columns, :])
                pre_ref[at : at + TILE, columns] = (slope_ref[tile % 2, :, columns].astype(F32) * grad_act).astype(BF16)
                return carry

            lax.fori_loop(0, hidden // WIDE, chunk, 0)
            if side == 0:
                slopes(1, tile).start()
            result = dot_nt(pre_ref[at : at + TILE, :], in_ref[...]).astype(BF16)
            made[side, tile * TILE_PLACES : (tile + 1) * TILE_PLACES] = result.reshape(TILE_PLACES, CAP_PAD, -1)
            start_blocks(made, returned, sems, 1, side, blocks, -1)
    await_blocks(made, returned, sems, 1, 1, range(PLACES), -1)
    collect_sums(slots_ref.at[1], returned, 1, sums_ref)
    twin_sum[...] = sums_ref[...].astype(BF16)
    sum_copy = to_twin(twin_sum, other, twin_sems, 1)
    sum_copy.start()
    arrived = arrived_ref[...].reshape(2 * HALF, -1)
    grads = came[...].reshape(2 * HALF, -1)
    for chunk in range(hidden // WIDE):
        columns = slice(chunk * WIDE, (chunk + 1) * WIDE)
        gin_ref[:, columns] = dot_tn(arrived, pre_ref[:, columns]).astype(BF16)
        acts(chunk).wait()
        gout_ref[columns, :] = dot_tn(act_ref[chunk % 2], grads).astype(BF16)
        if chunk + 2 < hidden // WIDE:
            acts(chunk + 2).start()
    await_blocks(made, returned, sems, 1, 0, range(PLACES), -1)
    collect_sums(slots_ref.at[0], returned, 0, sums_ref)
    for side in range(2):
        await_sent(leaving, came, sems, 0, side, 1)
        await_sent(made, returned, sems, 1, side, -1)
    rows_copy.wait_send()
    gates_copy.wait()
    grad_gates_ref[...] += other_gates[...]
    sum_copy.wait()

    def body(rows):
        sums_ref[rows, :] += other[rows, :].astype(F32)

    each_chunk(body)


def run_unmix(grad, sent, gates, routed, slots, turned, arrived, act, slope, weight_in, weight_out):
    model, hidden = weight_in.shape
    outs = [shape((ROWS, model), F32), shape((8, ROWS), F32), shape((model, hidden), BF16), shape((hidden, model), BF16)]
    return pl.pallas_call(
        unmix_kernel,
        out_shape=outs,
        in_specs=in_vmem(6) + anywhere(5),
        out_specs=in_vmem(4),
        scratch_shapes=[
            pltpu.VMEM((ROWS, model), BF16),
            blocks_of(model),
            blocks_of(model),
            blocks_of(model),
            blocks_of(model),
            pltpu.VMEM((TOP * ROWS, model), BF16),
            pltpu.VMEM((ROWS, model), BF16),
            pltpu.VMEM((ROWS, model), BF16),
            pltpu.VMEM((8, ROWS), F32),
            pltpu.VMEM((8, ROWS), F32),
            pltpu.VMEM((2 * HALF, hidden), BF16),
            pltpu.VMEM((2, TILE, hidden), BF16),
            pltpu.VMEM((2, 2 * HALF, WIDE), BF16),
            blocks_of(model),
            pltpu.VMEM((model, hidden), BF16),
            pltpu.VMEM((hidden, model), BF16),
            pltpu.SemaphoreType.DMA((2, 2, 2, PLACES)),
            pltpu.SemaphoreType.DMA((2, 3)),
            pltpu.SemaphoreType.DMA((3,)),
            pltpu.SemaphoreType.DMA((2,)),
            pltpu.SemaphoreType.DMA((2,)),
        ],
        compiler_params=pltpu.CompilerParams(vmem_limit_bytes=LIMIT, collective_id=2, has_side_effects=True),
        name="unmix",
    )(grad, sent, gates, routed, slots, turned, arrived, act, slope, weight_in, weight_out)


def front(x_ref, w_ref, outs):
    x1_ref, proj_ref, log_ref, att_ref, normed_ref = outs
    gain1, gain2, shift1, shift2 = weight_parts(w_ref, x_ref.shape[1])
    attention_rows(x_ref, w_ref, gain1, shift1, x1_ref, proj_ref, log_ref, att_ref, normed_ref)
    norm_rows(x1_ref, gain2, shift2, normed_ref)


def first_kernel(x_ref, w_ref, *outs):
    front(x_ref, w_ref, outs)


def middle_kernel(x1_ref, delta_ref, w_ref, x_ref, *rest):
    def body(rows):
        x_ref[rows, :] = x1_ref[rows, :] + delta_ref[rows, :]

    each_chunk(body)
    front(x_ref, w_ref, rest)


def last_kernel(x1_ref, delta_ref, teacher_ref, scale_ref, final_ref, grad_ref, sent_ref):
    def body(rows):
        values = x1_ref[rows, :] + delta_ref[rows, :]
        final_ref[rows, :] = values.astype(BF16)
        grad = (values - teacher_ref[rows, :].astype(F32)) * scale_ref[rows, :]
        grad_ref[rows, :] = grad
        sent_ref[rows, :] = grad.astype(BF16)

    each_chunk(body)


def back_kernel(grad_in_ref, sums_ref, picks_ref, grad_gates_ref, chances_ref, x1_ref, x_ref, proj_ref, log_ref, att_ref, w_ref, grad_ref, sent_ref, small_ref, normed_ref, gnormed_ref, gproj_ref, gatt_ref, back_ref, mid_ref, sums_a, sums_b, router_ref):
    model = x_ref.shape[1]
    gain1, gain2, shift1, shift2 = weight_parts(w_ref, model)
    gnormed_ref[...] = sums_ref[...]
    norm_rows(x1_ref, gain2, shift2, normed_ref)
    router_pullback(grad_gates_ref, picks_ref, chances_ref, w_ref, normed_ref, gnormed_ref, router_ref)
    norm_pullback(x1_ref, gain2, gnormed_ref, grad_in_ref, mid_ref, sums_b)
    norm_rows(x_ref, gain1, shift1, normed_ref)
    attention_pullback(mid_ref, w_ref, proj_ref, log_ref, att_ref, normed_ref, small_ref, gproj_ref, gatt_ref, back_ref, gnormed_ref)
    norm_pullback(x_ref, gain1, gnormed_ref, mid_ref, grad_ref, sums_a)
    sent_ref[...] = grad_ref[...].astype(BF16)
    rows = lax.broadcasted_iota(jnp.int32, (LANES, model), 0)
    side = jnp.zeros((LANES, model), F32)
    for i, value in enumerate((sums_a[0:1, :], sums_b[0:1, :], sums_a[1:2, :], sums_b[1:2, :])):
        side = jnp.where(rows == EXPERTS + i, value, side)
    lane = lax.broadcasted_iota(jnp.int32, (model, LANES), 1)
    small_ref[:, 4 * model :] = jnp.where(lane < EXPERTS, router_ref[...], jnp.transpose(side))


def shape(dims, kind):
    return jax.ShapeDtypeStruct(dims, kind)


def call(kernel, outs, scratch, name, after=(), limit=56):
    after = list(after)

    def run(*ins):
        count = len(ins)

        def body(*refs):
            kernel(*refs[:count], *refs[count + len(after) :])

        return pl.pallas_call(
            body,
            out_shape=outs,
            in_specs=[pl.BlockSpec(memory_space=pltpu.VMEM)] * count + [pl.BlockSpec(memory_space=pl.ANY)] * len(after),
            scratch_shapes=scratch,
            compiler_params=pltpu.CompilerParams(vmem_limit_bytes=limit << 20),
            name=name,
        )(*ins, *after)

    return run


def front_outs(model):
    return [
        shape((ROWS, model), F32),
        shape((ROWS, 3 * model), BF16),
        shape((ROWS, LANES), F32),
        shape((ROWS, model), BF16),
        shape((ROWS, model), BF16),
    ]


def run_first(x, w):
    return call(first_kernel, front_outs(x.shape[1]), [], "first")(x, w)


def run_middle(x1, delta, w):
    model = x1.shape[1]
    outs = [shape((ROWS, model), F32)] + front_outs(model)
    return call(middle_kernel, outs, [], "middle")(x1, delta, w)


def run_last(*ins):
    model = ins[0].shape[1]
    outs = [shape((ROWS, model), BF16), shape((ROWS, model), F32), shape((ROWS, model), BF16)]
    return call(last_kernel, outs, [], "last")(*ins)


def run_back(*ins):
    model = ins[0].shape[1]
    outs = [shape((ROWS, model), F32), shape((ROWS, model), BF16), shape((model, 4 * model + LANES), F32)]
    scratch = [
        pltpu.VMEM((ROWS, model), BF16),
        pltpu.VMEM((ROWS, model), F32),
        pltpu.VMEM((ROWS, 3 * model), BF16),
        pltpu.VMEM((ROWS, model), BF16),
        pltpu.VMEM((ROWS, model), BF16),
        pltpu.VMEM((ROWS, model), F32),
        pltpu.VMEM((2, model), F32),
        pltpu.VMEM((2, model), F32),
        pltpu.VMEM((model, LANES), F32),
    ]
    return call(back_kernel, outs, scratch, "back")(*ins)


def layer_copy_kernel(layer, whole_ref, after_ref, out_ref, sem):
    copy = pltpu.make_async_copy(whole_ref.at[layer], out_ref, sem)
    copy.start()
    copy.wait()


def layer_part(whole, layer, after):
    return pl.pallas_call(
        functools.partial(layer_copy_kernel, layer),
        out_shape=shape(whole.shape[1:], whole.dtype),
        in_specs=[pl.BlockSpec(memory_space=pl.ANY)] * 2,
        scratch_shapes=[pltpu.SemaphoreType.DMA],
        name="layer_part",
    )(whole, after)


def layer_norm(values, gain_row, shift_row):
    centred = values - jnp.mean(values, axis=-1, keepdims=True)
    spread = jnp.mean(centred * centred, axis=-1, keepdims=True)
    return centred * lax.rsqrt(spread + norm_eps) * gain_row + shift_row


def route_slots(picks_dev, capacity):
    flat_ids = picks_dev.reshape(-1)
    onehot = (flat_ids[:, None] == jnp.arange(EXPERTS, dtype=jnp.int32)[None, :]).astype(jnp.int32)
    before = jnp.cumsum(onehot, axis=0) - onehot
    ranking = jnp.sum(before * onehot, axis=1)
    slot_index = flat_ids * capacity + ranking
    routes_dev = flat_ids.shape[0]
    source = jnp.full((EXPERTS * capacity,), routes_dev, jnp.int32)
    source = source.at[slot_index].set(jnp.arange(routes_dev, dtype=jnp.int32))
    return (slot_index, source)


def attention_forward(current, qkv_full, out_full, gain_row, shift_row):
    model_width = current.shape[1]
    normed = layer_norm(current, gain_row, shift_row).astype(jnp.bfloat16)
    projected = jnp.dot(normed, qkv_full, preferred_element_type=jnp.float32).astype(jnp.bfloat16)
    split_parts = projected.reshape(SLOTS, SEQ, 3, HEADS, HEAD_DIM)
    scores = jnp.einsum(
        "ashd,athd->ahst",
        split_parts[:, :, 0],
        split_parts[:, :, 1],
        preferred_element_type=jnp.float32,
    ) * HEAD_DIM ** (-0.5)
    highest_score = jnp.max(scores, axis=-1, keepdims=True)
    exponent = jnp.exp(scores - highest_score)
    summed = jnp.sum(exponent, axis=-1, keepdims=True)
    weights = (exponent / summed).astype(jnp.bfloat16)
    log_total = highest_score + jnp.log(summed)
    attended = jnp.einsum(
        "ahst,athd->ashd", weights, split_parts[:, :, 2], preferred_element_type=jnp.float32
    )
    attended = attended.reshape(SLOTS * SEQ, model_width).astype(jnp.bfloat16)
    branch_out = jnp.dot(attended, out_full, preferred_element_type=jnp.float32)
    return (current + branch_out, (current, normed, projected, log_total, attended))


def attention_backward(grad_states, saved, qkv_full, out_full, gain_row, shift_row):
    current, normed, projected, log_total, attended = saved
    model_width = current.shape[1]
    grad_branch = grad_states.astype(jnp.bfloat16)
    grad_out = jnp.einsum("rd,re->de", attended, grad_branch, preferred_element_type=jnp.float32)
    grad_attended = jnp.einsum(
        "re,de->rd", grad_branch, out_full, preferred_element_type=jnp.float32
    ).astype(jnp.bfloat16)
    split_parts = projected.reshape(SLOTS, SEQ, 3, HEADS, HEAD_DIM)
    queries = split_parts[:, :, 0]
    keys_part = split_parts[:, :, 1]
    values_part = split_parts[:, :, 2]
    scaling = HEAD_DIM ** (-0.5)
    scores = (
        jnp.einsum("ashd,athd->ahst", queries, keys_part, preferred_element_type=jnp.float32)
        * scaling
    )
    chances = jnp.exp(scores - log_total)
    grad_heads = grad_attended.reshape(SLOTS, SEQ, HEADS, HEAD_DIM)
    grad_weights = jnp.einsum(
        "ashd,athd->ahst", grad_heads, values_part, preferred_element_type=jnp.float32
    )
    grad_values = jnp.einsum(
        "ahst,ashd->athd",
        chances.astype(jnp.bfloat16),
        grad_heads,
        preferred_element_type=jnp.float32,
    )
    centre_term = jnp.sum(grad_weights * chances, axis=-1, keepdims=True)
    grad_scores = (chances * (grad_weights - centre_term)).astype(jnp.bfloat16)
    grad_queries = (
        jnp.einsum("ahst,athd->ashd", grad_scores, keys_part, preferred_element_type=jnp.float32)
        * scaling
    )
    grad_keys = (
        jnp.einsum("ahst,ashd->athd", grad_scores, queries, preferred_element_type=jnp.float32)
        * scaling
    )
    grad_projected = jnp.stack([grad_queries, grad_keys, grad_values], axis=2)
    grad_projected = grad_projected.reshape(SLOTS * SEQ, 3 * model_width).astype(jnp.bfloat16)
    grad_qkv = jnp.einsum("rd,re->de", normed, grad_projected, preferred_element_type=jnp.float32)
    grad_normed = jnp.einsum(
        "re,de->rd", grad_projected, qkv_full, preferred_element_type=jnp.float32
    )
    unused_value, norm_pullback = jax.vjp(layer_norm, current, gain_row, shift_row)
    grad_input, grad_gain, grad_shift = norm_pullback(grad_normed)
    return (grad_states + grad_input, grad_qkv, grad_out, grad_gain, grad_shift)


def mixture_forward(current, gain_row, shift_row, router_full, in_shard, out_shard, picks_layer):
    row_count, model_width = current.shape
    experts_all = router_full.shape[1]
    normed = layer_norm(current, gain_row, shift_row).astype(jnp.bfloat16)
    logits = jnp.dot(normed, router_full, preferred_element_type=jnp.float32)
    chances = jax.nn.softmax(logits, axis=-1)
    matches = picks_layer[:, :, None] == jnp.arange(experts_all, dtype=jnp.int32)[None, None, :]
    gate_values = jnp.sum(jnp.where(matches, chances[:, None, :], 0.0), axis=-1)
    slot_index, source = route_slots(picks_layer, CAP)
    filled = source < TOP * row_count
    route_clip = jnp.minimum(source, TOP * row_count - 1)
    taken_rows = route_clip // TOP
    outgoing = jnp.where(filled[:, None], normed[taken_rows], jnp.zeros((), jnp.bfloat16))
    outgoing = outgoing.reshape(experts_all, CAP, model_width)
    arrived = lax.all_to_all(outgoing, "expert", split_axis=0, concat_axis=1, tiled=True)
    in_full, out_full = (
        lax.all_gather(in_shard, "shard", axis=1, tiled=True),
        lax.all_gather(out_shard, "shard", axis=1, tiled=True),
    )
    hidden_pre = jnp.einsum("erd,edh->erh", arrived, in_full, preferred_element_type=jnp.float32)
    activated = jax.nn.gelu(hidden_pre).astype(jnp.bfloat16)
    produced = jnp.einsum(
        "erh,ehd->erd", activated, out_full, preferred_element_type=jnp.float32
    ).astype(jnp.bfloat16)
    returned = lax.all_to_all(produced, "expert", split_axis=1, concat_axis=0, tiled=True)
    routed = returned.reshape(experts_all * CAP, model_width)[slot_index].reshape(
        row_count, TOP, model_width
    )
    updated = current + jnp.sum(gate_values[:, :, None] * routed.astype(jnp.float32), axis=1)
    saved = (
        current,
        normed,
        chances,
        matches,
        gate_values,
        slot_index,
        filled,
        route_clip,
        arrived,
        routed,
        in_full,
        out_full,
    )
    return (updated, saved)


def mixture_backward(grad_states, saved, gain_row, shift_row, router_full, in_shard, out_shard):
    (
        current,
        normed,
        chances,
        matches,
        gate_values,
        slot_index,
        filled,
        route_clip,
        arrived,
        routed,
        kept_in,
        kept_out,
    ) = saved
    row_count, model_width = current.shape
    experts_all = chances.shape[1]
    grad_routed = (gate_values[:, :, None] * grad_states[:, None, :]).astype(jnp.bfloat16)
    grad_routed = grad_routed.reshape(TOP * row_count, model_width)
    grad_gates = jnp.sum(grad_states[:, None, :] * routed.astype(jnp.float32), axis=-1)
    grad_outgoing = jnp.where(filled[:, None], grad_routed[route_clip], jnp.zeros((), jnp.bfloat16))
    grad_outgoing = grad_outgoing.reshape(experts_all, CAP, model_width)
    grad_result = lax.all_to_all(grad_outgoing, "expert", split_axis=0, concat_axis=1, tiled=True)
    in_full, out_full = (
        lax.all_gather(in_shard, "shard", axis=1, tiled=True),
        lax.all_gather(out_shard, "shard", axis=1, tiled=True),
    )
    hidden_pre = jnp.einsum("erd,edh->erh", arrived, in_full, preferred_element_type=jnp.float32)
    activated, gelu_pullback = jax.vjp(jax.nn.gelu, hidden_pre)
    grad_out_experts = jnp.einsum(
        "erh,erd->ehd",
        activated.astype(jnp.bfloat16),
        grad_result,
        preferred_element_type=jnp.float32,
    )
    grad_activated = jnp.einsum(
        "erd,ehd->erh", grad_result, out_full, preferred_element_type=jnp.float32
    )
    grad_pre = gelu_pullback(grad_activated)[0].astype(jnp.bfloat16)
    grad_in_experts = jnp.einsum(
        "erd,erh->edh", arrived, grad_pre, preferred_element_type=jnp.float32
    )
    grad_arrived = jnp.einsum(
        "erh,edh->erd", grad_pre, in_full, preferred_element_type=jnp.float32
    ).astype(jnp.bfloat16)
    grad_returned = lax.all_to_all(grad_arrived, "expert", split_axis=1, concat_axis=0, tiled=True)
    grad_in_share, grad_out_share = (
        lax.psum_scatter(
            grad_in_experts.astype(jnp.bfloat16), "shard", scatter_dimension=1, tiled=True
        ).astype(jnp.float32),
        lax.psum_scatter(
            grad_out_experts.astype(jnp.bfloat16), "shard", scatter_dimension=1, tiled=True
        ).astype(jnp.float32),
    )
    grad_routes = grad_returned.reshape(experts_all * CAP, model_width)[slot_index]
    grad_normed = jnp.sum(
        grad_routes.reshape(row_count, TOP, model_width).astype(jnp.float32), axis=1
    )
    grad_chances = jnp.sum(jnp.where(matches, grad_gates[:, :, None], 0.0), axis=1)
    grad_logits = chances * (grad_chances - jnp.sum(grad_chances * chances, axis=-1, keepdims=True))
    grad_logits = grad_logits.astype(jnp.bfloat16)
    grad_router = jnp.einsum("rd,re->de", normed, grad_logits, preferred_element_type=jnp.float32)
    grad_normed = grad_normed + jnp.einsum(
        "re,de->rd", grad_logits, router_full, preferred_element_type=jnp.float32
    )
    unused_value, norm_pullback = jax.vjp(layer_norm, current, gain_row, shift_row)
    grad_input, grad_gain, grad_shift = norm_pullback(grad_normed)
    return (
        grad_states + grad_input,
        grad_router,
        grad_gain,
        grad_shift,
        grad_in_share,
        grad_out_share,
    )


def shards(
    states,
    qkv_weight,
    out_weight,
    norm_gain,
    norm_bias,
    router_weight,
    expert_in,
    expert_out,
    chosen,
    image_count,
    teacher,
):
    qkv_full, out_full, gain_full, bias_full, router_full = (
        lax.all_gather(qkv_weight, "shard", axis=1, tiled=True),
        lax.all_gather(out_weight, "shard", axis=1, tiled=True),
        lax.all_gather(norm_gain, "shard", axis=1, tiled=True),
        lax.all_gather(norm_bias, "shard", axis=1, tiled=True),
        lax.all_gather(router_weight, "shard", axis=1, tiled=True),
    )
    gain_float = gain_full.astype(jnp.float32)
    bias_float = bias_full.astype(jnp.float32)
    layer_count = qkv_weight.shape[0]
    row_count, model_width = states.shape
    slot_image = jnp.arange(row_count, dtype=jnp.int32) // SEQ
    living = slot_image < image_count[0]
    counted = lax.psum(image_count[0].astype(jnp.float32) * SEQ, ("expert", "shard"))
    current = states.astype(jnp.float32)
    attention_kept = []
    mixture_kept = []
    for layer_index in range(layer_count):
        current, kept_attention = attention_forward(
            current,
            qkv_full[layer_index],
            out_full[layer_index],
            gain_float[layer_index, :, 0],
            bias_float[layer_index, :, 0],
        )
        current, kept_mixture = mixture_forward(
            current,
            gain_float[layer_index, :, 1],
            bias_float[layer_index, :, 1],
            router_full[layer_index],
            expert_in[layer_index],
            expert_out[layer_index],
            chosen[layer_index],
        )
        attention_kept.append(kept_attention)
        mixture_kept.append(kept_mixture)
    missed = current - teacher.astype(jnp.float32)
    grad_states = jnp.where(living[:, None], 2.0 * missed, 0.0) / counted
    qkv_list = [None] * layer_count
    out_list = [None] * layer_count
    gain_list = [None] * layer_count
    bias_list = [None] * layer_count
    router_list = [None] * layer_count
    in_list = [None] * layer_count
    experts_out_list = [None] * layer_count
    for layer_index in reversed(range(layer_count)):
        grad_states, grad_router, gain_second, shift_second, grad_in_share, grad_out_share = (
            mixture_backward(
                grad_states,
                mixture_kept[layer_index],
                gain_float[layer_index, :, 1],
                bias_float[layer_index, :, 1],
                router_full[layer_index],
                expert_in[layer_index],
                expert_out[layer_index],
            )
        )
        grad_states, grad_qkv, grad_out, gain_first, shift_first = attention_backward(
            grad_states,
            attention_kept[layer_index],
            qkv_full[layer_index],
            out_full[layer_index],
            gain_float[layer_index, :, 0],
            bias_float[layer_index, :, 0],
        )
        qkv_list[layer_index] = grad_qkv
        out_list[layer_index] = grad_out
        gain_list[layer_index] = jnp.stack([gain_first, gain_second], axis=-1)
        bias_list[layer_index] = jnp.stack([shift_first, shift_second], axis=-1)
        router_list[layer_index] = grad_router
        in_list[layer_index] = grad_in_share
        experts_out_list[layer_index] = grad_out_share
    mixer_grads = (
        jnp.stack(qkv_list),
        jnp.stack(out_list),
        jnp.stack(gain_list),
        jnp.stack(bias_list),
        jnp.stack(router_list),
    )
    summed = lax.psum(
        (mixer_grads[0], mixer_grads[1], mixer_grads[2], mixer_grads[3], mixer_grads[4]),
        ("expert", "shard"),
    )
    share_width = model_width // lax.axis_size("shard")
    start_index = lax.axis_index("shard") * share_width
    reduced = tuple(
        (lax.dynamic_slice_in_dim(member, start_index, share_width, 1) for member in summed)
    )
    return (
        current.astype(jnp.bfloat16),
        grad_states * counted,
        reduced[0],
        reduced[1],
        reduced[2],
        reduced[3],
        reduced[4],
        jnp.stack(in_list),
        jnp.stack(experts_out_list),
    )


def pad_rows(values, fill=0):
    width = values.shape[-1]
    images = values.reshape(SLOTS, SEQ, width)
    images = jnp.pad(images, ((0, 0), (0, SEQ_PAD - SEQ), (0, 0)), constant_values=fill)
    images = images.reshape(SLOTS * SEQ_PAD, width)
    return jnp.pad(images, ((0, ROWS - SLOTS * SEQ_PAD), (0, 0)), constant_values=fill)


def live_rows(values):
    images = values[: SLOTS * SEQ_PAD].reshape(SLOTS, SEQ_PAD, values.shape[-1])
    return images[:, :SEQ].reshape(SLOTS * SEQ, values.shape[-1])


def across(values):
    return lax.ppermute(values, "shard", [(i, (i + SHARDS // 2) % SHARDS) for i in range(SHARDS)])


def own_expert(shard_part):
    moved = lax.all_to_all(shard_part, "shard", split_axis=0, concat_axis=0, tiled=True)
    return moved.reshape(-1, shard_part.shape[-1])


def share_expert(grad):
    blocks = grad.reshape(SHARDS, grad.shape[0] // SHARDS, grad.shape[1])
    return lax.all_to_all(blocks, "shard", split_axis=0, concat_axis=0, tiled=True)


def pick_rows(chosen_layer):
    _, shard, _, me = position()
    side = chosen_layer % SHARDS
    place = (chosen_layer // SHARDS * 2 + side % 2 - me + PLACES) % PLACES
    place = jnp.where(side // 2 == shard // 2, place, -1)
    lanes = pad_rows(jnp.concatenate([chosen_layer, place], axis=1), -1)
    return jnp.pad(lanes, ((0, 0), (0, LANES - 2 * TOP)), constant_values=-1)


def owners(
    states,
    qkv_weight,
    out_weight,
    norm_gain,
    norm_bias,
    router_weight,
    expert_in,
    expert_out,
    chosen,
    image_count,
    teacher,
):
    layers, share, _ = qkv_weight.shape
    model = states.shape[1]
    groups = lax.axis_size("expert")
    piece = share // groups
    spare = LANES - EXPERTS - 5
    marks = jnp.zeros((layers, share, 1 + spare), BF16)
    packed = jnp.concatenate([qkv_weight, out_weight, router_weight, norm_gain, norm_bias, marks], axis=2)
    packed = lax.dynamic_slice_in_dim(packed, lax.axis_index("expert") * piece, piece, 1)
    mark_at = 4 * model + EXPERTS + 4
    packed = packed.at[0, 0, mark_at].set(image_count[0].astype(BF16))
    weights = [lax.all_gather(packed[layer], ("shard", "expert"), axis=0, tiled=True) for layer in range(layers)]
    first_in = own_expert(layer_part(expert_in, 0, image_count))
    first_out = own_expert(layer_part(expert_out, 0, first_in))
    experts = [(first_in, first_out)]
    counted = jnp.sum(weights[0][:, mark_at].astype(F32)) * SEQ
    slot_image = jnp.arange(states.shape[0], dtype=jnp.int32) // SEQ
    living = slot_image < image_count[0]
    scale = pad_rows(jnp.where(living, 2.0 / counted, 0.0)[:, None])
    others = across(chosen)
    picks = [[pick_rows(source[layer]) for source in (chosen, others)] for layer in range(layers)]
    kept = []
    current = pad_rows(states.astype(F32))
    x1, proj, logs, att, normed = run_first(current, weights[0])
    for layer in range(layers):
        if layer + 1 < layers:
            next_in = own_expert(layer_part(expert_in, layer + 1, experts[layer][1]))
            next_out = own_expert(layer_part(expert_out, layer + 1, next_in))
            experts.append((next_in, next_out))
        mixed = run_mix(normed, weights[layer][:, 4 * model :], *picks[layer], *experts[layer])
        delta, slots, turned, chances, gates, arrived, routed, act, slope = mixed
        kept.append((current, x1, proj, logs, att, slots, turned, chances, gates, arrived, routed, act, slope))
        if layer + 1 < layers:
            current, x1, proj, logs, att, normed = run_middle(x1, delta, weights[layer + 1])
    final, grad, sent = run_last(x1, delta, pad_rows(teacher), scale)
    smalls, ins, outs = [None] * layers, [None] * layers, [None] * layers
    for layer in reversed(range(layers)):
        current, x1, proj, logs, att, slots, turned, chances, gates, arrived, routed, act, slope = kept[layer]
        sums, grad_gates, grad_in, grad_out = run_unmix(
            grad, sent, gates, routed, slots, turned, arrived, act, slope, *experts[layer]
        )
        ins[layer], outs[layer] = share_expert(grad_in), share_expert(grad_out)
        grad, sent, small = run_back(
            grad, sums, picks[layer][0], grad_gates, chances, x1, current, proj, logs, att, weights[layer]
        )
        part = lax.psum_scatter(small, ("shard", "expert"), scatter_dimension=0, tiled=True)
        smalls[layer] = lax.all_gather(part, "expert", axis=0, tiled=True)
    small = jnp.stack(smalls)
    at = 4 * model
    return (
        live_rows(final),
        live_rows(grad) * counted,
        small[:, :, : 3 * model],
        small[:, :, 3 * model : at],
        small[:, :, at + EXPERTS : at + EXPERTS + 2],
        small[:, :, at + EXPERTS + 2 : at + EXPERTS + 4],
        small[:, :, at : at + EXPERTS],
        jnp.stack(ins).astype(F32),
        jnp.stack(outs).astype(F32),
    )


def plan_of(mesh):
    return owners if owns(mesh) else shards


def owns(mesh):
    groups, shards_all = mesh.shape["expert"], mesh.shape["shard"]
    return shards_all == SHARDS and groups * shards_all == EXPERTS


def solution(mesh):
    in_specs = (
        P(("expert", "shard"), None),
        P(None, "shard", None),
        P(None, "shard", None),
        P(None, "shard", None),
        P(None, "shard", None),
        P(None, "shard", None),
        P(None, "expert", "shard", None),
        P(None, "expert", "shard", None),
        P(None, ("expert", "shard"), None),
        P(("expert", "shard")),
        P(("expert", "shard"), None),
    )
    out_specs = (
        P(("expert", "shard"), None),
        P(("expert", "shard"), None),
        P(None, "shard", None),
        P(None, "shard", None),
        P(None, "shard", None),
        P(None, "shard", None),
        P(None, "shard", None),
        P(None, "expert", "shard", None),
        P(None, "expert", "shard", None),
    )
    step = jax.shard_map(plan_of(mesh), mesh=mesh, in_specs=in_specs, out_specs=out_specs, check_vma=False)
    return step
```

```python
import functools
import jax
import jax.numpy as jnp
from jax import lax
from jax.experimental import pallas as pl
from jax.experimental.pallas import tpu as pltpu
from jax.sharding import PartitionSpec as P


HEADS = 8
HEAD_DIM = 64
EXPERTS = 32
TOP = 2
SEQ = 197
SLOTS = 3
CAP = 74
norm_eps = 1e-06

LANES = 128
SEQ_PAD = 208
ROWS = 640
CAP_PAD = 80
CHUNK = 64
SHARDS = 4
LIMIT = 62 << 20
F32 = jnp.float32
BF16 = jnp.bfloat16


def dot(a, b):
    return jnp.dot(a, b, preferred_element_type=F32)


def dot_nt(a, b):
    return lax.dot_general(a, b, (((1,), (1,)), ((), ())), preferred_element_type=F32)


def dot_tn(a, b):
    return lax.dot_general(a, b, (((0,), (0,)), ((), ())), preferred_element_type=F32)


def rows_of(step, size):
    return pl.ds(pl.multiple_of(step * size, size), size)


def each_chunk(body, size=CHUNK, total=ROWS):
    def step(i, carry):
        body(rows_of(i, size))
        return carry

    lax.fori_loop(0, total // size, step, 0)


def centre(values):
    centred = values - jnp.mean(values, axis=-1, keepdims=True)
    spread = jnp.mean(centred * centred, axis=-1, keepdims=True)
    return centred, lax.rsqrt(spread + norm_eps)


def norm_rows(x_ref, gain, shift, out_ref):
    def body(rows):
        centred, inverse = centre(x_ref[rows, :])
        out_ref[rows, :] = (centred * inverse * gain + shift).astype(BF16)

    each_chunk(body)


def norm_pullback(x_ref, gain, grad_ref, total_ref, out_ref, sums_ref):
    sums_ref[...] = jnp.zeros_like(sums_ref)

    def body(rows):
        centred, inverse = centre(x_ref[rows, :])
        unit = centred * inverse
        grad = grad_ref[rows, :]
        scaled = grad * gain
        first = jnp.mean(scaled, axis=-1, keepdims=True)
        second = jnp.mean(scaled * unit, axis=-1, keepdims=True)
        out_ref[rows, :] = total_ref[rows, :] + inverse * (scaled - first - unit * second)
        sums_ref[0:1, :] += jnp.sum(grad * unit, axis=0, keepdims=True)
        sums_ref[1:2, :] += jnp.sum(grad, axis=0, keepdims=True)

    each_chunk(body)


def weight_parts(w_ref, model):
    side = jnp.transpose(w_ref[:, 4 * model :].astype(F32))
    return [side[EXPERTS + i : EXPERTS + i + 1, :] for i in range(4)]


def attention_rows(x_ref, w_ref, gain, shift, x1_ref, proj_ref, log_ref, att_ref, normed_ref):
    model = x_ref.shape[1]
    norm_rows(x_ref, gain, shift, normed_ref)
    for part in range(3):
        columns = slice(part * model, (part + 1) * model)
        proj_ref[:, columns] = dot(normed_ref[...], w_ref[:, columns]).astype(BF16)
    att_ref[...] = jnp.zeros_like(att_ref)
    log_ref[...] = jnp.zeros_like(log_ref)
    low = lax.broadcasted_iota(jnp.int32, (SEQ_PAD, LANES), 1) < HEAD_DIM
    inside = lax.broadcasted_iota(jnp.int32, (SEQ_PAD, SEQ_PAD), 1) < SEQ
    lane = lax.broadcasted_iota(jnp.int32, (SEQ_PAD, LANES), 1)

    def image(i, carry):
        rows = rows_of(i, SEQ_PAD)
        logs = jnp.zeros((SEQ_PAD, LANES), F32)
        for pair in range(HEADS // 2):
            at = pair * LANES
            queries = proj_ref[rows, at : at + LANES]
            keys = proj_ref[rows, model + at : model + at + LANES]
            values = proj_ref[rows, 2 * model + at : 2 * model + at + LANES]
            results = []
            for side in range(2):
                mine = low if side == 0 else jnp.logical_not(low)
                masked = jnp.where(mine, queries, jnp.zeros_like(queries))
                scores = dot_nt(masked, keys) * HEAD_DIM ** (-0.5)
                scores = jnp.where(inside, scores, -1e30)
                highest = jnp.max(scores, axis=-1, keepdims=True)
                exponent = jnp.exp(scores - highest)
                summed = jnp.sum(exponent, axis=-1, keepdims=True)
                weights = (exponent / summed).astype(BF16)
                logs = jnp.where(lane == 2 * pair + side, highest + jnp.log(summed), logs)
                results.append(dot(weights, values))
            att_ref[rows, at : at + LANES] = jnp.where(low, results[0], results[1]).astype(BF16)
        log_ref[rows, :] = logs
        return carry

    lax.fori_loop(0, SLOTS, image, 0)
    x1_ref[...] = x_ref[...] + dot(att_ref[...], w_ref[:, 3 * model : 4 * model])


def route_rows(picks, slots_ref, turned_ref):
    lane = lax.broadcasted_iota(jnp.int32, (ROWS, LANES), 1)
    firsts, seconds = picks[:, 0:1], picks[:, 1:2]
    place_first, place_second = picks[:, 2:3], picks[:, 3:4]
    match_first, match_second = lane == firsts, lane == seconds
    either = jnp.where(match_first | match_second, 1.0, 0.0).astype(BF16)
    down = lax.broadcasted_iota(jnp.int32, (ROWS, ROWS), 0)
    across = lax.broadcasted_iota(jnp.int32, (ROWS, ROWS), 1)
    before = dot(jnp.where(across < down, 1.0, 0.0).astype(BF16), either)
    rank_first = jnp.sum(jnp.where(match_first, before, 0.0), axis=-1, keepdims=True)
    rank_second = jnp.sum(jnp.where(match_second, before, 0.0), axis=-1, keepdims=True)
    slot_first = jnp.where(place_first < 0, -1.0, place_first.astype(F32) * CAP_PAD + rank_first)
    slot_second = jnp.where(place_second < 0, -1.0, place_second.astype(F32) * CAP_PAD + rank_second)
    both = jnp.where(lane == 0, slot_first, jnp.where(lane == 1, slot_second, -1.0))
    slots_ref[...] = both.astype(jnp.int32)
    turned_ref[...] = jnp.transpose(both)[0:8, :].astype(jnp.int32)


def gate_rows(normed_ref, router_ref, picks, chances_ref, gates_ref):
    lane = lax.broadcasted_iota(jnp.int32, (ROWS, LANES), 1)
    logits = dot(normed_ref[...], router_ref[...])
    logits = jnp.where(lane < EXPERTS, logits, -1e30)
    exponent = jnp.exp(logits - jnp.max(logits, axis=-1, keepdims=True))
    chances = exponent / jnp.sum(exponent, axis=-1, keepdims=True)
    if chances_ref is not None:
        chances_ref[...] = chances
    gate_first = jnp.sum(jnp.where(lane == picks[:, 0:1], chances, 0.0), axis=-1, keepdims=True)
    gate_second = jnp.sum(jnp.where(lane == picks[:, 1:2], chances, 0.0), axis=-1, keepdims=True)
    gates_ref[...] = jnp.where(lane == 0, gate_first, jnp.where(lane == 1, gate_second, 0.0))


PLACES = EXPERTS // 2
GROUP = 4
BLOCK = GROUP * CAP_PAD
HALF = PLACES * CAP_PAD


def pick_block(turned_ref, group):
    slot = lax.broadcasted_iota(jnp.int32, (BLOCK, ROWS), 0) + group * BLOCK
    return slot == turned_ref[0:1, :], slot == turned_ref[1:2, :]


def as_weights(mask):
    return jnp.where(mask, 1.0, 0.0).astype(BF16)


def dispatch_block(turned_ref, rows_ref, group):
    first, second = pick_block(turned_ref, group)
    return dot(as_weights(first | second), rows_ref[...]).astype(BF16)


def dispatch_pair_block(turned_ref, pairs_ref, group):
    first, second = pick_block(turned_ref, group)
    both = jnp.concatenate([as_weights(first), as_weights(second)], axis=1)
    return dot(both, pairs_ref[...]).astype(BF16)


def rows_at(ref, lead, group):
    block = ref[(*lead, pl.ds(group * GROUP, GROUP))]
    return block.reshape(BLOCK, block.shape[-1])


def collect_pairs(slots_ref, found_ref, side, total_ref):
    for group in range(PLACES // GROUP):
        slot = lax.broadcasted_iota(jnp.int32, (ROWS, BLOCK), 1) + group * BLOCK
        rows = rows_at(found_ref, (side,), group)
        for which in range(TOP):
            part = dot(as_weights(slot == slots_ref[:, which : which + 1]), rows)
            to = slice(which * ROWS, (which + 1) * ROWS)
            if group == 0:
                total_ref[to, :] = part
            else:
                total_ref[to, :] += part


def collect_sums(slots_ref, found_ref, side, total_ref):
    for group in range(PLACES // GROUP):
        slot = lax.broadcasted_iota(jnp.int32, (ROWS, BLOCK), 1) + group * BLOCK
        chosen = (slot == slots_ref[:, 0:1]) | (slot == slots_ref[:, 1:2])
        part = dot(as_weights(chosen), rows_at(found_ref, (side,), group))
        if group == 0:
            total_ref[...] = part
        else:
            total_ref[...] += part


def later_rows(rows):
    return pl.ds(pl.multiple_of(rows.start + ROWS, CHUNK), CHUNK)


def gated_sums(gates_ref, total_ref, routed_ref, side, out_ref):
    def body(rows):
        later = later_rows(rows)
        first, second = total_ref[rows, :], total_ref[later, :]
        gates = gates_ref[side, rows, :]
        out_ref[rows, :] = (gates[:, 0:1] * first + gates[:, 1:2] * second).astype(out_ref.dtype)
        routed_ref[side, rows, :] = first.astype(BF16)
        routed_ref[side, later, :] = second.astype(BF16)

    each_chunk(body)


def gate_grads(grad_ref, gates_ref, routed_ref, side, pairs_ref, grad_gates_ref):
    lane = lax.broadcasted_iota(jnp.int32, (LANES, LANES), 1)

    def body(i, carry):
        rows = rows_of(i, LANES)
        later = pl.ds(pl.multiple_of(i * LANES + ROWS, LANES), LANES)
        grad = grad_ref[rows, :].astype(F32)
        gates = gates_ref[side, rows, :]
        pairs_ref[rows, :] = (gates[:, 0:1] * grad).astype(BF16)
        pairs_ref[later, :] = (gates[:, 1:2] * grad).astype(BF16)
        first = jnp.sum(grad * routed_ref[side, rows, :].astype(F32), axis=-1, keepdims=True)
        second = jnp.sum(grad * routed_ref[side, later, :].astype(F32), axis=-1, keepdims=True)
        both = jnp.where(lane == 0, first, jnp.where(lane == 1, second, 0.0))
        grad_gates_ref[:, rows] = jnp.transpose(both)[0:8, :]
        return carry

    lax.fori_loop(0, ROWS // LANES, body, 0)


def attention_pullback(grad_ref, w_ref, proj_ref, log_ref, att_ref, normed_ref, small_ref, gproj_ref, gatt_ref, back_ref, gnormed_ref):
    model = grad_ref.shape[1]

    def body(rows):
        back_ref[rows, :] = grad_ref[rows, :].astype(BF16)

    each_chunk(body)
    small_ref[:, 3 * model : 4 * model] = dot_tn(att_ref[...], back_ref[...])
    gatt_ref[...] = dot_nt(back_ref[...], w_ref[:, 3 * model : 4 * model]).astype(BF16)
    gproj_ref[SLOTS * SEQ_PAD :, :] = jnp.zeros((ROWS - SLOTS * SEQ_PAD, 3 * model), BF16)
    low = lax.broadcasted_iota(jnp.int32, (SEQ_PAD, LANES), 1) < HEAD_DIM
    inside = lax.broadcasted_iota(jnp.int32, (SEQ_PAD, SEQ_PAD), 1) < SEQ
    scaling = HEAD_DIM ** (-0.5)

    def image(i, carry):
        rows = rows_of(i, SEQ_PAD)
        for pair in range(HEADS // 2):
            at = pair * LANES
            queries = proj_ref[rows, at : at + LANES]
            keys = proj_ref[rows, model + at : model + at + LANES]
            values = proj_ref[rows, 2 * model + at : 2 * model + at + LANES]
            grad_heads = gatt_ref[rows, at : at + LANES]
            parts = []
            for side in range(2):
                mine = low if side == 0 else jnp.logical_not(low)
                zero = jnp.zeros_like(queries)
                head = 2 * pair + side
                scores = dot_nt(jnp.where(mine, queries, zero), keys) * scaling
                chances = jnp.where(inside, jnp.exp(scores - log_ref[rows, head : head + 1]), 0.0)
                grad_weights = dot_nt(jnp.where(mine, grad_heads, zero), values)
                centre_term = jnp.sum(grad_weights * chances, axis=-1, keepdims=True)
                grad_scores = (chances * (grad_weights - centre_term)).astype(BF16)
                parts.append(
                    (
                        dot(grad_scores, keys) * scaling,
                        dot_tn(grad_scores, queries) * scaling,
                        dot_tn(chances.astype(BF16), grad_heads),
                    )
                )
            for which in range(3):
                to = which * model + at
                gproj_ref[rows, to : to + LANES] = jnp.where(low, parts[0][which], parts[1][which]).astype(BF16)
        return carry

    lax.fori_loop(0, SLOTS, image, 0)
    for part in range(3):
        columns = slice(part * model, (part + 1) * model)
        small_ref[:, columns] = dot_tn(normed_ref[...], gproj_ref[:, columns])
    gnormed_ref[...] = dot_nt(gproj_ref[...], w_ref[:, : 3 * model])


def router_pullback(grad_gates_ref, picks_ref, chances_ref, w_ref, normed_ref, gnormed_ref, router_ref):
    model = normed_ref.shape[1]
    lane = lax.broadcasted_iota(jnp.int32, (ROWS, LANES), 1)
    picks, chances = picks_ref[...], chances_ref[...]
    turned = jnp.concatenate([grad_gates_ref[...], jnp.zeros((LANES - 8, ROWS), F32)], axis=0)
    grads = jnp.transpose(turned)
    spread = jnp.where(lane == picks[:, 0:1], grads[:, 0:1], 0.0) + jnp.where(lane == picks[:, 1:2], grads[:, 1:2], 0.0)
    logits = chances * (spread - jnp.sum(spread * chances, axis=-1, keepdims=True))
    logits = logits.astype(BF16)
    router_ref[...] = dot_tn(normed_ref[...], logits)
    gnormed_ref[...] += dot_nt(logits, w_ref[:, 4 * model :])


MESH = pl.DeviceIdType.MESH


def position():
    group, shard = lax.axis_index("expert"), lax.axis_index("shard")
    low = shard % 2
    return group, shard, low, group * 2 + low


def place_id(step):
    _, shard, low, me = position()
    there = (me + step + PLACES) % PLACES
    return (there // 2, shard - low + there % 2)


def twin_id():
    group, shard, _, _ = position()
    return (group, (shard + 2) % SHARDS)


def meet():
    barrier = pltpu.get_barrier_semaphore()
    for k in range(1, PLACES):
        pl.semaphore_signal(barrier, inc=1, device_id=place_id(k), device_id_type=MESH)
    group, shard, low, _ = position()
    for k in range(2):
        there = (shard - low + SHARDS // 2 + k) % SHARDS
        pl.semaphore_signal(barrier, inc=1, device_id=(group, there), device_id_type=MESH)
    pl.semaphore_wait(barrier, PLACES + 1)


def to_twin(src, dst, sems, at):
    return pltpu.make_async_remote_copy(
        src_ref=src, dst_ref=dst, send_sem=sems.at[0, at], recv_sem=sems.at[1, at], device_id=twin_id(), device_id_type=MESH
    )


def shard_rows(ref, shard):
    rows = ref.shape[0] // SHARDS
    return pl.ds(pl.multiple_of(shard * rows, rows), rows)


def share_blocks(source, target, sems, own_source=None):
    group, shard, _, _ = position()
    copies = [pltpu.make_async_copy(source(shard) if own_source is None else own_source, target(shard), sems.at[1, 0])]
    for k in (2, 1, 3):
        to = (shard + k) % SHARDS
        copies.append(
            pltpu.make_async_remote_copy(
                src_ref=source(to),
                dst_ref=target(shard),
                send_sem=sems.at[0, k],
                recv_sem=sems.at[1, k],
                device_id=(group, to),
                device_id_type=MESH,
            )
        )
    return copies


def block_copy(src, dst, sems, lane, side, k, sign):
    if k == 0:
        return pltpu.make_async_copy(src.at[side, 0], dst.at[side, 0], sems.at[lane, 1, side, 0])
    return pltpu.make_async_remote_copy(
        src_ref=src.at[side, k],
        dst_ref=dst.at[side, k],
        send_sem=sems.at[lane, 0, side, k],
        recv_sem=sems.at[lane, 1, side, k],
        device_id=place_id(sign * k),
        device_id_type=MESH,
    )


def start_blocks(src, dst, sems, lane, side, blocks, sign):
    for k in blocks:
        block_copy(src, dst, sems, lane, side, k, sign).start()


def await_blocks(src, dst, sems, lane, side, blocks, sign):
    for k in blocks:
        copy = block_copy(src, dst, sems, lane, side, k, sign)
        copy.wait() if k == 0 else copy.wait_recv()


def await_sent(src, dst, sems, lane, side, sign):
    for k in range(1, PLACES):
        block_copy(src, dst, sems, lane, side, k, sign).wait_send()


def spread(make_block, src, dst, sems, side):
    for group in range(PLACES // GROUP):
        src[side, group * GROUP : (group + 1) * GROUP] = make_block(group).reshape(GROUP, CAP_PAD, src.shape[-1])
        if group:
            start_blocks(src, dst, sems, 0, side, range((group - 1) * GROUP, group * GROUP), 1)
    start_blocks(src, dst, sems, 0, side, range(PLACES - GROUP, PLACES), 1)


TILE_PLACES = 8
TILE = TILE_PLACES * CAP_PAD
TILES = PLACES // TILE_PLACES
WIDE = 512
ROOT = 0.7978845608028654
CUBE = 0.044715


def mix_kernel(
    layer, normed_ref, router_ref, mine_ref, theirs_ref, piece_ref, in_hbm, outs_hbm, ins_hbm,
    delta_ref, slots_ref, turned_ref, chances_ref, gates_ref, arrived_ref, routed_ref, full_ref, act_hbm, slope_hbm, next_hbm, kept_hbm,
    twin_rows, leaving, made, returned, total, twin_sum, other, act_ref, slope_ref, in_ref, out_ref, stage_ref,
    sems, twin_sems, load_sems, save_sems, out_sems, next_sems, *more_sems,
):
    _, shard, _, _ = position()
    more = layer + 1 < ins_hbm.shape[0]
    stage = pltpu.make_async_copy(ins_hbm.at[layer + 1 if more else layer, shard], stage_ref, load_sems.at[1])
    load = pltpu.make_async_copy(in_hbm, in_ref, load_sems.at[0])
    load.start()
    stage.start()
    out_copies = share_blocks(lambda to: outs_hbm.at[layer, to], lambda own: out_ref.at[shard_rows(out_ref, own)], out_sems)
    meet()
    rows_copy = to_twin(normed_ref, twin_rows, twin_sems, 0)
    rows_copy.start()
    for copy in out_copies:
        copy.start()
    next_copies = []
    if more:
        gather = Gather(piece_ref, full_ref, *more_sems)
        gather.start()
        stage.wait()
        next_copies = share_blocks(
            lambda to: ins_hbm.at[layer + 1, to], lambda own: next_hbm.at[shard_rows(next_hbm, own)], next_sems, stage_ref
        )
    route_rows(mine_ref[...], slots_ref.at[0], turned_ref.at[0])
    spread(lambda group: dispatch_block(turned_ref.at[0], normed_ref, group), leaving, arrived_ref, sems, 0)
    route_rows(theirs_ref[...], slots_ref.at[1], turned_ref.at[1])
    gate_rows(normed_ref, router_ref, mine_ref[...], chances_ref, gates_ref.at[0])
    rows_copy.wait_recv()
    spread(lambda group: dispatch_block(turned_ref.at[1], twin_rows, group), leaving, arrived_ref, sems, 1)
    if more:
        gather.spread()
    for copy in next_copies:
        copy.start()
    gate_rows(twin_rows, router_ref, theirs_ref[...], None, gates_ref.at[1])
    load.wait()

    def saves(slot, side, tile):
        to = pl.ds((side * TILES + tile) * TILE, TILE)
        return [
            pltpu.make_async_copy(act_ref.at[slot], act_hbm.at[to, :], save_sems.at[0, slot]),
            pltpu.make_async_copy(slope_ref.at[slot], slope_hbm.at[to, :], save_sems.at[1, slot]),
        ]

    for side in range(2):
        for tile in range(TILES):
            slot = tile % 2
            blocks = range(tile * TILE_PLACES, (tile + 1) * TILE_PLACES)
            await_blocks(leaving, arrived_ref, sems, 0, side, blocks, 1)
            if side:
                for save in saves(slot, 0, tile):
                    save.wait()
            rows = arrived_ref[side, tile * TILE_PLACES : (tile + 1) * TILE_PLACES].reshape(TILE, -1)

            def chunk(i, carry):
                columns = rows_of(i, WIDE)
                pre = dot(rows, in_ref[:, columns])
                square = pre * pre
                bend = jnp.tanh(pre * (ROOT + ROOT * CUBE * square))
                half = 0.5 + 0.5 * bend
                act = (pre * half).astype(BF16)
                slope = half + (0.5 * pre) * (1.0 - bend * bend) * (ROOT + 3.0 * ROOT * CUBE * square)
                act_ref[slot, :, columns] = act
                slope_ref[slot, :, columns] = slope.astype(BF16)
                return carry

            lax.fori_loop(0, in_ref.shape[1] // WIDE, chunk, 0)
            if not (side or tile):
                for copy in out_copies:
                    copy.wait()
                keep = pltpu.make_async_copy(out_ref, kept_hbm, load_sems.at[2])
                keep.start()
            result = dot(act_ref[slot], out_ref[...]).astype(BF16)
            made[side, tile * TILE_PLACES : (tile + 1) * TILE_PLACES] = result.reshape(TILE_PLACES, CAP_PAD, -1)
            for save in saves(slot, side, tile):
                save.start()
            start_blocks(made, returned, sems, 1, side, blocks, -1)
    if more:
        gather.pair()
    await_blocks(made, returned, sems, 1, 1, range(PLACES), -1)
    collect_pairs(slots_ref.at[1], returned, 1, total)
    gated_sums(gates_ref, total, routed_ref, 1, twin_sum)
    sum_copy = to_twin(twin_sum, other, twin_sems, 1)
    sum_copy.start()
    await_blocks(made, returned, sems, 1, 0, range(PLACES), -1)
    collect_pairs(slots_ref.at[0], returned, 0, total)
    gated_sums(gates_ref, total, routed_ref, 0, delta_ref)
    for tile in range(TILES):
        for save in saves(tile % 2, 1, tile):
            save.wait()
    for side in range(2):
        await_sent(leaving, arrived_ref, sems, 0, side, 1)
        await_sent(made, returned, sems, 1, side, -1)
    rows_copy.wait_send()
    sum_copy.wait()
    keep.wait()
    for copy in next_copies:
        copy.wait()
    if more:
        gather.finish()
    else:
        stage.wait()

    def body(rows):
        delta_ref[rows, :] += other[rows, :].astype(F32)

    each_chunk(body)


def in_vmem(count):
    return [pl.BlockSpec(memory_space=pltpu.VMEM)] * count


def anywhere(count):
    return [pl.BlockSpec(memory_space=pl.ANY)] * count


def blocks_of(model):
    return pltpu.VMEM((2, PLACES, CAP_PAD, model), BF16)


def run_mix(layer, normed, router, mine, theirs, piece, weight_in, expert_out, expert_in):
    model, hidden = weight_in.shape
    outs = [
        shape((ROWS, model), F32),
        shape((2, ROWS, LANES), jnp.int32),
        shape((2, 8, ROWS), jnp.int32),
        shape((ROWS, LANES), F32),
        shape((2, ROWS, LANES), F32),
        shape((2, PLACES, CAP_PAD, model), BF16),
        shape((2, TOP * ROWS, model), BF16),
        full_shape(piece),
        shape((2 * HALF, hidden), BF16),
        shape((2 * HALF, hidden), BF16),
        shape((model, hidden), BF16),
        shape((hidden, model), BF16),
    ]
    return pl.pallas_call(
        functools.partial(mix_kernel, layer),
        out_shape=outs,
        in_specs=in_vmem(5) + anywhere(3),
        out_specs=in_vmem(8) + anywhere(4),
        scratch_shapes=[
            pltpu.VMEM((ROWS, model), BF16),
            blocks_of(model),
            blocks_of(model),
            blocks_of(model),
            pltpu.VMEM((TOP * ROWS, model), F32),
            pltpu.VMEM((ROWS, model), BF16),
            pltpu.VMEM((ROWS, model), BF16),
            pltpu.VMEM((2, TILE, hidden), BF16),
            pltpu.VMEM((2, TILE, hidden), BF16),
            pltpu.VMEM((model, hidden), BF16),
            pltpu.VMEM((hidden, model), BF16),
            pltpu.VMEM((model // SHARDS, hidden), BF16),
            pltpu.SemaphoreType.DMA((2, 2, 2, PLACES)),
            pltpu.SemaphoreType.DMA((2, 2)),
            pltpu.SemaphoreType.DMA((3,)),
            pltpu.SemaphoreType.DMA((2, 2)),
            pltpu.SemaphoreType.DMA((2, SHARDS)),
            pltpu.SemaphoreType.DMA((2, SHARDS)),
        ]
        + gather_sems(),
        compiler_params=pltpu.CompilerParams(vmem_limit_bytes=LIMIT, collective_id=1 + layer, has_side_effects=True),
        name="mix",
    )(normed, router, mine, theirs, piece, weight_in, expert_out, expert_in)


def unmix_kernel(
    carry, grad_ref, sent_ref, gates_ref, routed_ref, slots_ref, turned_ref, arrived_hbm, act_hbm, slope_hbm, in_hbm, out_hbm, carried_hbm,
    sums_ref, grad_gates_ref, gin_ref, gout_ref, shared_hbm,
    twin_rows, leaving, came, made, returned, pairs, twin_sum, other, twin_gates, other_gates, pre_ref, slope_ref, act_ref, arrived_ref, in_ref, out_ref, stage_ref,
    sems, twin_sems, load_sems, slope_sems, act_sems, share_sems,
):
    _, shard, _, _ = position()
    if carry:
        stage = pltpu.make_async_copy(carried_hbm.at[shard], stage_ref, load_sems.at[3])
        stage.start()
    loads = [
        pltpu.make_async_copy(src, dst, load_sems.at[i])
        for i, (src, dst) in enumerate(((in_hbm, in_ref), (out_hbm, out_ref), (arrived_hbm, arrived_ref)))
    ]
    for load in loads:
        load.start()

    def slopes(side, tile):
        at = pl.ds((side * TILES + tile) * TILE, TILE)
        return pltpu.make_async_copy(slope_hbm.at[at, :], slope_ref.at[tile % 2], slope_sems.at[tile % 2])

    def acts(chunk):
        return pltpu.make_async_copy(act_hbm.at[:, pl.ds(chunk * WIDE, WIDE)], act_ref.at[chunk % 2], act_sems.at[chunk % 2])

    for tile in range(TILES):
        slopes(0, tile).start()
    for chunk in range(2):
        acts(chunk).start()
    meet()
    rows_copy = to_twin(sent_ref, twin_rows, twin_sems, 0)
    rows_copy.start()
    share_copies = []
    if carry:
        stage.wait()
        share_copies = share_blocks(lambda to: carried_hbm.at[to], lambda own: shared_hbm.at[own], share_sems, stage_ref)
        for copy in share_copies:
            copy.start()
    gate_grads(grad_ref, gates_ref, routed_ref, 0, pairs, grad_gates_ref)
    spread(lambda group: dispatch_pair_block(turned_ref.at[0], pairs, group), leaving, came, sems, 0)
    rows_copy.wait_recv()
    gate_grads(twin_rows, gates_ref, routed_ref, 1, pairs, twin_gates)
    gates_copy = to_twin(twin_gates, other_gates, twin_sems, 2)
    spread(lambda group: dispatch_pair_block(turned_ref.at[1], pairs, group), leaving, came, sems, 1)
    gates_copy.start()
    for load in loads:
        load.wait()
    hidden = in_ref.shape[1]
    for side in range(2):
        for tile in range(TILES):
            blocks = range(tile * TILE_PLACES, (tile + 1) * TILE_PLACES)
            await_blocks(leaving, came, sems, 0, side, blocks, 1)
            slopes(side, tile).wait()
            rows = came[side, tile * TILE_PLACES : (tile + 1) * TILE_PLACES].reshape(TILE, -1)
            at = (side * TILES + tile) * TILE

            def chunk(i, carry):
                columns = rows_of(i, WIDE)
                grad_act = dot_nt(rows, out_ref[columns, :])
                pre_ref[at : at + TILE, columns] = (slope_ref[tile % 2, :, columns].astype(F32) * grad_act).astype(BF16)
                return carry

            lax.fori_loop(0, hidden // WIDE, chunk, 0)
            if side == 0:
                slopes(1, tile).start()
            result = dot_nt(pre_ref[at : at + TILE, :], in_ref[...]).astype(BF16)
            made[side, tile * TILE_PLACES : (tile + 1) * TILE_PLACES] = result.reshape(TILE_PLACES, CAP_PAD, -1)
            start_blocks(made, returned, sems, 1, side, blocks, -1)
    await_blocks(made, returned, sems, 1, 1, range(PLACES), -1)
    collect_sums(slots_ref.at[1], returned, 1, sums_ref)
    twin_sum[...] = sums_ref[...].astype(BF16)
    sum_copy = to_twin(twin_sum, other, twin_sems, 1)
    sum_copy.start()
    arrived = arrived_ref[...].reshape(2 * HALF, -1)
    grads = came[...].reshape(2 * HALF, -1)
    for chunk in range(hidden // WIDE):
        columns = slice(chunk * WIDE, (chunk + 1) * WIDE)
        gin_ref[:, columns] = dot_tn(arrived, pre_ref[:, columns]).astype(BF16)
        acts(chunk).wait()
        gout_ref[columns, :] = dot_tn(act_ref[chunk % 2], grads).astype(BF16)
        if chunk + 2 < hidden // WIDE:
            acts(chunk + 2).start()
    await_blocks(made, returned, sems, 1, 0, range(PLACES), -1)
    collect_sums(slots_ref.at[0], returned, 0, sums_ref)
    for side in range(2):
        await_sent(leaving, came, sems, 0, side, 1)
        await_sent(made, returned, sems, 1, side, -1)
    rows_copy.wait_send()
    gates_copy.wait()
    grad_gates_ref[...] += other_gates[...]
    sum_copy.wait()
    for copy in share_copies:
        copy.wait()

    def body(rows):
        sums_ref[rows, :] += other[rows, :].astype(F32)

    each_chunk(body)


def run_unmix(grad, sent, gates, routed, slots, turned, arrived, act, slope, weight_in, weight_out, carried, carry):
    model, hidden = weight_in.shape
    outs = [shape((ROWS, model), F32), shape((8, ROWS), F32), shape((model, hidden), BF16), shape((hidden, model), BF16)]
    outs.append(shape(carried.shape, BF16))
    return pl.pallas_call(
        functools.partial(unmix_kernel, carry),
        out_shape=outs,
        in_specs=in_vmem(6) + anywhere(6),
        out_specs=in_vmem(4) + anywhere(1),
        scratch_shapes=[
            pltpu.VMEM((ROWS, model), BF16),
            blocks_of(model),
            blocks_of(model),
            blocks_of(model),
            blocks_of(model),
            pltpu.VMEM((TOP * ROWS, model), BF16),
            pltpu.VMEM((ROWS, model), BF16),
            pltpu.VMEM((ROWS, model), BF16),
            pltpu.VMEM((8, ROWS), F32),
            pltpu.VMEM((8, ROWS), F32),
            pltpu.VMEM((2 * HALF, hidden), BF16),
            pltpu.VMEM((2, TILE, hidden), BF16),
            pltpu.VMEM((2, 2 * HALF, WIDE), BF16),
            blocks_of(model),
            pltpu.VMEM((model, hidden), BF16),
            pltpu.VMEM((hidden, model), BF16),
            pltpu.VMEM(carried.shape[1:], BF16),
            pltpu.SemaphoreType.DMA((2, 2, 2, PLACES)),
            pltpu.SemaphoreType.DMA((2, 3)),
            pltpu.SemaphoreType.DMA((4,)),
            pltpu.SemaphoreType.DMA((2,)),
            pltpu.SemaphoreType.DMA((2,)),
            pltpu.SemaphoreType.DMA((2, SHARDS)),
        ],
        compiler_params=pltpu.CompilerParams(vmem_limit_bytes=LIMIT, collective_id=3 + int(carry), has_side_effects=True),
        name="unmix",
    )(grad, sent, gates, routed, slots, turned, arrived, act, slope, weight_in, weight_out, carried)


def flips():
    group = lax.axis_index("expert")
    along = 2 - 4 * (group // 2 % 2)
    up = 4 - 8 * (group // 4)
    return [group + along, group + up, group + along + up]


def other_core():
    group = lax.axis_index("expert")
    return group + 1 - 2 * (group % 2)


def remote(src, dst, send_sem, recv_sem, device):
    return pltpu.make_async_remote_copy(
        src_ref=src, dst_ref=dst, send_sem=send_sem, recv_sem=recv_sem, device_id=device, device_id_type=MESH
    )


def meet_axes():
    group, shard = lax.axis_index("expert"), lax.axis_index("shard")
    barrier = pltpu.get_barrier_semaphore()
    devices = [(group, (shard + k) % SHARDS) for k in range(1, SHARDS)]
    devices += [(there, shard) for there in flips() + [other_core()]]
    for device in devices:
        pl.semaphore_signal(barrier, inc=1, device_id=device, device_id_type=MESH)
    pl.semaphore_wait(barrier, len(devices))


class Gather:
    def __init__(self, piece, full, far_sems, flat_sems, core_sems, own_sem):
        self.group, self.shard = lax.axis_index("expert"), lax.axis_index("shard")
        self.piece, self.full = piece, full
        self.far_sems, self.flat_sems, self.core_sems = far_sems, flat_sems, core_sems
        self.planes = [(self.shard + SHARDS - k) % SHARDS for k in range(SHARDS)]
        self.own = pltpu.make_async_copy(piece, self.rows(self.shard, self.group), own_sem)
        self.sent = []

    def rows(self, plane, there):
        size = self.piece.shape[0]
        span = self.full.shape[0] // SHARDS
        return self.full.at[pl.ds(pl.multiple_of(plane * span + there * size, size), size)]

    def go(self, copy):
        copy.start()
        self.sent.append(copy)

    def far(self, k):
        to = (self.group, (self.shard + k) % SHARDS)
        return remote(self.piece, self.rows(self.shard, self.group), self.far_sems.at[0, k], self.far_sems.at[1, k], to)

    def flat(self, at, p, k):
        return remote(at, at, self.flat_sems.at[0, p, k], self.flat_sems.at[1, p, k], (flips()[p], self.shard))

    def core(self, at, p, k):
        return remote(at, at, self.core_sems.at[0, p, k], self.core_sems.at[1, p, k], (other_core(), self.shard))

    def start(self):
        self.own.start()
        for k in (2, 1, 3):
            self.go(self.far(k))
        self.own.wait()

    def spread(self):
        for k in (0, 1, 3, 2):
            at = self.rows(self.planes[k], self.group)
            if k:
                self.far(k).wait_recv()
            for p in range(3):
                self.go(self.flat(at, p, k))
            self.go(self.core(at, 3, k))

    def pair(self):
        for k in (0, 1, 3, 2):
            for p, there in enumerate(flips()):
                at = self.rows(self.planes[k], there)
                self.flat(at, p, k).wait_recv()
                self.go(self.core(at, p, k))

    def finish(self):
        turn = 1 - 2 * (self.group % 2)
        for k in range(SHARDS):
            for p, there in enumerate(flips() + [self.group]):
                self.core(self.rows(self.planes[k], there + turn), p, k).wait_recv()
        for copy in self.sent:
            copy.wait_send()


def gather_sems():
    return [
        pltpu.SemaphoreType.DMA((2, SHARDS)),
        pltpu.SemaphoreType.DMA((2, 3, SHARDS)),
        pltpu.SemaphoreType.DMA((2, 4, SHARDS)),
        pltpu.SemaphoreType.DMA,
    ]


def full_shape(piece):
    return shape((piece.shape[0] * EXPERTS, piece.shape[1]), piece.dtype)


def gather_kernel(piece_ref, picks_ref, full_ref, twin_picks_ref, *sems):
    group, shard = lax.axis_index("expert"), lax.axis_index("shard")
    meet_axes()
    gather = Gather(piece_ref, full_ref, *sems[:4])
    picks_copy = remote(picks_ref, twin_picks_ref, sems[4].at[0], sems[4].at[1], (group, (shard + 2) % SHARDS))
    gather.start()
    picks_copy.start()
    gather.spread()
    gather.pair()
    gather.finish()
    picks_copy.wait()


def run_gather(piece, picks):
    return pl.pallas_call(
        gather_kernel,
        out_shape=[full_shape(piece), shape(picks.shape, picks.dtype)],
        in_specs=in_vmem(2),
        out_specs=in_vmem(2),
        scratch_shapes=gather_sems() + [pltpu.SemaphoreType.DMA((2,))],
        compiler_params=pltpu.CompilerParams(vmem_limit_bytes=32 << 20, collective_id=5, has_side_effects=True),
        name="gather",
    )(piece, picks)


def finish_kernel(
    layers, *refs
):
    smalls, (carried_hbm, out_ref, shared_hbm) = refs[:layers], refs[layers : layers + 3]
    core_ref, leave_ref, came_ref, far_ref, far_came_ref, piece_ref, stage_ref = refs[layers + 3 : layers + 10]
    core_sems, flat_sems, far_sems, back_sems, pair_sems, share_sems, stage_sem = refs[layers + 10 :]
    group, shard = lax.axis_index("expert"), lax.axis_index("shard")
    turn = 1 - 2 * (group % 2)
    chip = group // 2
    size = piece_ref.shape[1]
    height = SHARDS * size
    stage = pltpu.make_async_copy(carried_hbm.at[shard], stage_ref, stage_sem)
    stage.start()
    meet_axes()
    pending = []

    def go(copy):
        copy.start()
        pending.append(copy)

    def part(layer, there):
        return smalls[layer].at[pl.ds(pl.multiple_of(there * height, height), height)]

    def core_copy(layer, at):
        chip_at = at // 2
        src = part(layer, chip_at * 2 + 1 - group % 2)
        return remote(src, core_ref.at[layer, chip_at], core_sems.at[0, layer, chip_at], core_sems.at[1, layer, chip_at], (other_core(), shard))

    def flat_copy(p):
        return remote(leave_ref.at[p], came_ref.at[p], flat_sems.at[0, p], flat_sems.at[1, p], (flips()[p], shard))

    order = flips() + [group]
    for there in order:
        for layer in range(layers):
            go(core_copy(layer, there))
    stage.wait()
    shares = share_blocks(lambda to: carried_hbm.at[to], lambda own: shared_hbm.at[own], share_sems, stage_ref)
    for copy in shares[:2]:
        copy.start()
    for p, there in enumerate(order[:3]):
        for layer in range(layers):
            core_copy(layer, there).wait_recv()
            leave_ref[p, layer] = (part(layer, there)[...] + core_ref[layer, there // 2]).astype(BF16)
        if p:
            go(flat_copy(p - 1))
    for layer in range(layers):
        core_copy(layer, group).wait_recv()
    go(flat_copy(2))
    for p in range(3):
        flat_copy(p).wait_recv()
    for layer in range(layers):
        total = part(layer, group)[...] + core_ref[layer, chip]
        for p in range(3):
            total = total + came_ref[p, layer].astype(F32)
        for plane in range(SHARDS):
            far_ref[plane, layer] = total[plane * size : (plane + 1) * size].astype(far_ref.dtype)
        core_ref[layer, chip] = total

    def far_copy(k):
        to = (shard + k) % SHARDS
        return remote(far_ref.at[to], far_came_ref.at[k], far_sems.at[0, k], far_sems.at[1, k], (group, to))

    for k in (2, 1, 3):
        go(far_copy(k))
    for copy in shares[2:]:
        copy.start()
    for k in (1, 3, 2):
        far_copy(k).wait_recv()
    for layer in range(layers):
        total = core_ref[layer, chip, pl.ds(pl.multiple_of(shard * size, size), size), :]
        for k in (1, 2, 3):
            total = total + far_came_ref[k, layer].astype(F32)
        piece_ref[layer] = total

    def place(there):
        return out_ref.at[:, pl.ds(pl.multiple_of(there * size, size), size)]

    place(group)[...] = piece_ref[...]

    def back_copy(p, at):
        return remote(piece_ref, at, back_sems.at[0, p], back_sems.at[1, p], (flips()[p], shard))

    def pair_copy(p, src, at):
        return remote(src, at, pair_sems.at[0, p], pair_sems.at[1, p], (other_core(), shard))

    for p in range(3):
        go(back_copy(p, place(group)))
    go(pair_copy(3, piece_ref, place(group)))
    for p, there in enumerate(flips()):
        back_copy(p, place(there)).wait_recv()
        go(pair_copy(p, place(there), place(there)))
    for p, there in enumerate(order):
        pair_copy(p, piece_ref, place(there + turn)).wait_recv()
    for copy in pending:
        copy.wait_send()
    for copy in shares:
        copy.wait()


def run_finish(smalls, carried):
    layers = len(smalls)
    groups = EXPERTS // SHARDS
    rows, width = smalls[0].shape
    span = rows // SHARDS
    size = span // groups
    chips = groups // 2
    height = SHARDS * size
    return pl.pallas_call(
        functools.partial(finish_kernel, layers),
        out_shape=[shape((layers, span, width), F32), shape(carried.shape, BF16)],
        in_specs=in_vmem(layers) + anywhere(1),
        out_specs=in_vmem(1) + anywhere(1),
        scratch_shapes=[
            pltpu.VMEM((layers, chips, height, width), F32),
            pltpu.VMEM((3, layers, height, width), BF16),
            pltpu.VMEM((3, layers, height, width), BF16),
            pltpu.VMEM((SHARDS, layers, size, width), BF16),
            pltpu.VMEM((SHARDS, layers, size, width), BF16),
            pltpu.VMEM((layers, size, width), F32),
            pltpu.VMEM(carried.shape[1:], BF16),
            pltpu.SemaphoreType.DMA((2, layers, chips)),
            pltpu.SemaphoreType.DMA((2, 3)),
            pltpu.SemaphoreType.DMA((2, SHARDS)),
            pltpu.SemaphoreType.DMA((2, 3)),
            pltpu.SemaphoreType.DMA((2, 4)),
            pltpu.SemaphoreType.DMA((2, SHARDS)),
            pltpu.SemaphoreType.DMA,
        ],
        compiler_params=pltpu.CompilerParams(vmem_limit_bytes=48 << 20, collective_id=6, has_side_effects=True),
        name="finish",
    )(*smalls, carried)


def front(x_ref, w_ref, outs):
    x1_ref, proj_ref, log_ref, att_ref, normed_ref = outs
    gain1, gain2, shift1, shift2 = weight_parts(w_ref, x_ref.shape[1])
    attention_rows(x_ref, w_ref, gain1, shift1, x1_ref, proj_ref, log_ref, att_ref, normed_ref)
    norm_rows(x1_ref, gain2, shift2, normed_ref)


def first_kernel(x_ref, w_ref, *outs):
    front(x_ref, w_ref, outs)


def middle_kernel(x1_ref, delta_ref, w_ref, x_ref, *rest):
    def body(rows):
        x_ref[rows, :] = x1_ref[rows, :] + delta_ref[rows, :]

    each_chunk(body)
    front(x_ref, w_ref, rest)


def last_kernel(x1_ref, delta_ref, teacher_ref, scale_ref, final_ref, grad_ref, sent_ref):
    def body(rows):
        values = x1_ref[rows, :] + delta_ref[rows, :]
        final_ref[rows, :] = values.astype(BF16)
        grad = (values - teacher_ref[rows, :].astype(F32)) * scale_ref[rows, :]
        grad_ref[rows, :] = grad
        sent_ref[rows, :] = grad.astype(BF16)

    each_chunk(body)


def back_kernel(grad_in_ref, sums_ref, picks_ref, grad_gates_ref, chances_ref, x1_ref, x_ref, proj_ref, log_ref, att_ref, w_ref, grad_ref, sent_ref, parts_ref, normed_ref, gnormed_ref, gproj_ref, gatt_ref, back_ref, mid_ref, sums_a, sums_b, router_ref, small_ref):
    model = x_ref.shape[1]
    gain1, gain2, shift1, shift2 = weight_parts(w_ref, model)
    gnormed_ref[...] = sums_ref[...]
    norm_rows(x1_ref, gain2, shift2, normed_ref)
    router_pullback(grad_gates_ref, picks_ref, chances_ref, w_ref, normed_ref, gnormed_ref, router_ref)
    norm_pullback(x1_ref, gain2, gnormed_ref, grad_in_ref, mid_ref, sums_b)
    norm_rows(x_ref, gain1, shift1, normed_ref)
    attention_pullback(mid_ref, w_ref, proj_ref, log_ref, att_ref, normed_ref, small_ref, gproj_ref, gatt_ref, back_ref, gnormed_ref)
    norm_pullback(x_ref, gain1, gnormed_ref, mid_ref, grad_ref, sums_a)
    sent_ref[...] = grad_ref[...].astype(BF16)
    rows = lax.broadcasted_iota(jnp.int32, (LANES, model), 0)
    side = jnp.zeros((LANES, model), F32)
    for i, value in enumerate((sums_a[0:1, :], sums_b[0:1, :], sums_a[1:2, :], sums_b[1:2, :])):
        side = jnp.where(rows == EXPERTS + i, value, side)
    lane = lax.broadcasted_iota(jnp.int32, (model, LANES), 1)
    small_ref[:, 4 * model :] = jnp.where(lane < EXPERTS, router_ref[...], jnp.transpose(side))
    size = model // EXPERTS
    for at in range(EXPERTS):
        shard, group = at % SHARDS, at // SHARDS
        row = (shard * (EXPERTS // SHARDS) + group) * size
        parts_ref[at * size : (at + 1) * size, :] = small_ref[row : row + size, :]


def shape(dims, kind):
    return jax.ShapeDtypeStruct(dims, kind)


def call(kernel, outs, scratch, after=(), limit=56):
    after = list(after)

    def run(*ins):
        count = len(ins)

        def body(*refs):
            kernel(*refs[:count], *refs[count + len(after) :])

        return pl.pallas_call(
            body,
            out_shape=outs,
            in_specs=[pl.BlockSpec(memory_space=pltpu.VMEM)] * count + [pl.BlockSpec(memory_space=pl.ANY)] * len(after),
            scratch_shapes=scratch,
            compiler_params=pltpu.CompilerParams(vmem_limit_bytes=limit << 20),
        )(*ins, *after)

    return run


def front_outs(model):
    return [
        shape((ROWS, model), F32),
        shape((ROWS, 3 * model), BF16),
        shape((ROWS, LANES), F32),
        shape((ROWS, model), BF16),
        shape((ROWS, model), BF16),
    ]


def run_first(x, w):
    return call(first_kernel, front_outs(x.shape[1]), [])(x, w)


def run_middle(x1, delta, w):
    model = x1.shape[1]
    outs = [shape((ROWS, model), F32)] + front_outs(model)
    return call(middle_kernel, outs, [])(x1, delta, w)


def run_last(*ins):
    model = ins[0].shape[1]
    outs = [shape((ROWS, model), BF16), shape((ROWS, model), F32), shape((ROWS, model), BF16)]
    return call(last_kernel, outs, [])(*ins)


def run_back(*ins):
    model = ins[0].shape[1]
    outs = [shape((ROWS, model), F32), shape((ROWS, model), BF16), shape((model, 4 * model + LANES), F32)]
    scratch = [
        pltpu.VMEM((ROWS, model), BF16),
        pltpu.VMEM((ROWS, model), F32),
        pltpu.VMEM((ROWS, 3 * model), BF16),
        pltpu.VMEM((ROWS, model), BF16),
        pltpu.VMEM((ROWS, model), BF16),
        pltpu.VMEM((ROWS, model), F32),
        pltpu.VMEM((2, model), F32),
        pltpu.VMEM((2, model), F32),
        pltpu.VMEM((model, LANES), F32),
        pltpu.VMEM((model, 4 * model + LANES), F32),
    ]
    return call(back_kernel, outs, scratch)(*ins)


def layer_copy_kernel(layer, whole_ref, after_ref, out_ref, sem):
    copy = pltpu.make_async_copy(whole_ref.at[layer], out_ref, sem)
    copy.start()
    copy.wait()


def layer_part(whole, layer, after):
    return pl.pallas_call(
        functools.partial(layer_copy_kernel, layer),
        out_shape=shape(whole.shape[1:], whole.dtype),
        in_specs=[pl.BlockSpec(memory_space=pl.ANY)] * 2,
        scratch_shapes=[pltpu.SemaphoreType.DMA],
        name="layer_part",
    )(whole, after)


def layer_norm(values, gain_row, shift_row):
    centred = values - jnp.mean(values, axis=-1, keepdims=True)
    spread = jnp.mean(centred * centred, axis=-1, keepdims=True)
    return centred * lax.rsqrt(spread + norm_eps) * gain_row + shift_row


def route_slots(picks_dev, capacity):
    flat_ids = picks_dev.reshape(-1)
    onehot = (flat_ids[:, None] == jnp.arange(EXPERTS, dtype=jnp.int32)[None, :]).astype(jnp.int32)
    before = jnp.cumsum(onehot, axis=0) - onehot
    ranking = jnp.sum(before * onehot, axis=1)
    slot_index = flat_ids * capacity + ranking
    routes_dev = flat_ids.shape[0]
    source = jnp.full((EXPERTS * capacity,), routes_dev, jnp.int32)
    source = source.at[slot_index].set(jnp.arange(routes_dev, dtype=jnp.int32))
    return (slot_index, source)


def attention_forward(current, qkv_full, out_full, gain_row, shift_row):
    model_width = current.shape[1]
    normed = layer_norm(current, gain_row, shift_row).astype(jnp.bfloat16)
    projected = jnp.dot(normed, qkv_full, preferred_element_type=jnp.float32).astype(jnp.bfloat16)
    split_parts = projected.reshape(SLOTS, SEQ, 3, HEADS, HEAD_DIM)
    scores = jnp.einsum(
        "ashd,athd->ahst",
        split_parts[:, :, 0],
        split_parts[:, :, 1],
        preferred_element_type=jnp.float32,
    ) * HEAD_DIM ** (-0.5)
    highest_score = jnp.max(scores, axis=-1, keepdims=True)
    exponent = jnp.exp(scores - highest_score)
    summed = jnp.sum(exponent, axis=-1, keepdims=True)
    weights = (exponent / summed).astype(jnp.bfloat16)
    log_total = highest_score + jnp.log(summed)
    attended = jnp.einsum(
        "ahst,athd->ashd", weights, split_parts[:, :, 2], preferred_element_type=jnp.float32
    )
    attended = attended.reshape(SLOTS * SEQ, model_width).astype(jnp.bfloat16)
    branch_out = jnp.dot(attended, out_full, preferred_element_type=jnp.float32)
    return (current + branch_out, (current, normed, projected, log_total, attended))


def attention_backward(grad_states, saved, qkv_full, out_full, gain_row, shift_row):
    current, normed, projected, log_total, attended = saved
    model_width = current.shape[1]
    grad_branch = grad_states.astype(jnp.bfloat16)
    grad_out = jnp.einsum("rd,re->de", attended, grad_branch, preferred_element_type=jnp.float32)
    grad_attended = jnp.einsum(
        "re,de->rd", grad_branch, out_full, preferred_element_type=jnp.float32
    ).astype(jnp.bfloat16)
    split_parts = projected.reshape(SLOTS, SEQ, 3, HEADS, HEAD_DIM)
    queries = split_parts[:, :, 0]
    keys_part = split_parts[:, :, 1]
    values_part = split_parts[:, :, 2]
    scaling = HEAD_DIM ** (-0.5)
    scores = (
        jnp.einsum("ashd,athd->ahst", queries, keys_part, preferred_element_type=jnp.float32)
        * scaling
    )
    chances = jnp.exp(scores - log_total)
    grad_heads = grad_attended.reshape(SLOTS, SEQ, HEADS, HEAD_DIM)
    grad_weights = jnp.einsum(
        "ashd,athd->ahst", grad_heads, values_part, preferred_element_type=jnp.float32
    )
    grad_values = jnp.einsum(
        "ahst,ashd->athd",
        chances.astype(jnp.bfloat16),
        grad_heads,
        preferred_element_type=jnp.float32,
    )
    centre_term = jnp.sum(grad_weights * chances, axis=-1, keepdims=True)
    grad_scores = (chances * (grad_weights - centre_term)).astype(jnp.bfloat16)
    grad_queries = (
        jnp.einsum("ahst,athd->ashd", grad_scores, keys_part, preferred_element_type=jnp.float32)
        * scaling
    )
    grad_keys = (
        jnp.einsum("ahst,ashd->athd", grad_scores, queries, preferred_element_type=jnp.float32)
        * scaling
    )
    grad_projected = jnp.stack([grad_queries, grad_keys, grad_values], axis=2)
    grad_projected = grad_projected.reshape(SLOTS * SEQ, 3 * model_width).astype(jnp.bfloat16)
    grad_qkv = jnp.einsum("rd,re->de", normed, grad_projected, preferred_element_type=jnp.float32)
    grad_normed = jnp.einsum(
        "re,de->rd", grad_projected, qkv_full, preferred_element_type=jnp.float32
    )
    _, norm_pullback = jax.vjp(layer_norm, current, gain_row, shift_row)
    grad_input, grad_gain, grad_shift = norm_pullback(grad_normed)
    return (grad_states + grad_input, grad_qkv, grad_out, grad_gain, grad_shift)


def mixture_forward(current, gain_row, shift_row, router_full, in_shard, out_shard, picks_layer):
    row_count, model_width = current.shape
    experts_all = router_full.shape[1]
    normed = layer_norm(current, gain_row, shift_row).astype(jnp.bfloat16)
    logits = jnp.dot(normed, router_full, preferred_element_type=jnp.float32)
    chances = jax.nn.softmax(logits, axis=-1)
    matches = picks_layer[:, :, None] == jnp.arange(experts_all, dtype=jnp.int32)[None, None, :]
    gate_values = jnp.sum(jnp.where(matches, chances[:, None, :], 0.0), axis=-1)
    slot_index, source = route_slots(picks_layer, CAP)
    filled = source < TOP * row_count
    route_clip = jnp.minimum(source, TOP * row_count - 1)
    taken_rows = route_clip // TOP
    outgoing = jnp.where(filled[:, None], normed[taken_rows], jnp.zeros((), jnp.bfloat16))
    outgoing = outgoing.reshape(experts_all, CAP, model_width)
    arrived = lax.all_to_all(outgoing, "expert", split_axis=0, concat_axis=1, tiled=True)
    in_full, out_full = (
        lax.all_gather(in_shard, "shard", axis=1, tiled=True),
        lax.all_gather(out_shard, "shard", axis=1, tiled=True),
    )
    hidden_pre = jnp.einsum("erd,edh->erh", arrived, in_full, preferred_element_type=jnp.float32)
    activated = jax.nn.gelu(hidden_pre).astype(jnp.bfloat16)
    produced = jnp.einsum(
        "erh,ehd->erd", activated, out_full, preferred_element_type=jnp.float32
    ).astype(jnp.bfloat16)
    returned = lax.all_to_all(produced, "expert", split_axis=1, concat_axis=0, tiled=True)
    routed = returned.reshape(experts_all * CAP, model_width)[slot_index].reshape(
        row_count, TOP, model_width
    )
    updated = current + jnp.sum(gate_values[:, :, None] * routed.astype(jnp.float32), axis=1)
    saved = (
        current,
        normed,
        chances,
        matches,
        gate_values,
        slot_index,
        filled,
        route_clip,
        arrived,
        routed,
        in_full,
        out_full,
    )
    return (updated, saved)


def mixture_backward(grad_states, saved, gain_row, shift_row, router_full, in_shard, out_shard):
    (current, normed, chances, matches, gate_values, slot_index, filled, route_clip, arrived, routed, _, _) = saved
    row_count, model_width = current.shape
    experts_all = chances.shape[1]
    grad_routed = (gate_values[:, :, None] * grad_states[:, None, :]).astype(jnp.bfloat16)
    grad_routed = grad_routed.reshape(TOP * row_count, model_width)
    grad_gates = jnp.sum(grad_states[:, None, :] * routed.astype(jnp.float32), axis=-1)
    grad_outgoing = jnp.where(filled[:, None], grad_routed[route_clip], jnp.zeros((), jnp.bfloat16))
    grad_outgoing = grad_outgoing.reshape(experts_all, CAP, model_width)
    grad_result = lax.all_to_all(grad_outgoing, "expert", split_axis=0, concat_axis=1, tiled=True)
    in_full, out_full = (
        lax.all_gather(in_shard, "shard", axis=1, tiled=True),
        lax.all_gather(out_shard, "shard", axis=1, tiled=True),
    )
    hidden_pre = jnp.einsum("erd,edh->erh", arrived, in_full, preferred_element_type=jnp.float32)
    activated, gelu_pullback = jax.vjp(jax.nn.gelu, hidden_pre)
    grad_out_experts = jnp.einsum(
        "erh,erd->ehd",
        activated.astype(jnp.bfloat16),
        grad_result,
        preferred_element_type=jnp.float32,
    )
    grad_activated = jnp.einsum(
        "erd,ehd->erh", grad_result, out_full, preferred_element_type=jnp.float32
    )
    grad_pre = gelu_pullback(grad_activated)[0].astype(jnp.bfloat16)
    grad_in_experts = jnp.einsum(
        "erd,erh->edh", arrived, grad_pre, preferred_element_type=jnp.float32
    )
    grad_arrived = jnp.einsum(
        "erh,edh->erd", grad_pre, in_full, preferred_element_type=jnp.float32
    ).astype(jnp.bfloat16)
    grad_returned = lax.all_to_all(grad_arrived, "expert", split_axis=1, concat_axis=0, tiled=True)
    grad_in_share, grad_out_share = (
        lax.psum_scatter(
            grad_in_experts.astype(jnp.bfloat16), "shard", scatter_dimension=1, tiled=True
        ).astype(jnp.float32),
        lax.psum_scatter(
            grad_out_experts.astype(jnp.bfloat16), "shard", scatter_dimension=1, tiled=True
        ).astype(jnp.float32),
    )
    grad_routes = grad_returned.reshape(experts_all * CAP, model_width)[slot_index]
    grad_normed = jnp.sum(
        grad_routes.reshape(row_count, TOP, model_width).astype(jnp.float32), axis=1
    )
    grad_chances = jnp.sum(jnp.where(matches, grad_gates[:, :, None], 0.0), axis=1)
    grad_logits = chances * (grad_chances - jnp.sum(grad_chances * chances, axis=-1, keepdims=True))
    grad_logits = grad_logits.astype(jnp.bfloat16)
    grad_router = jnp.einsum("rd,re->de", normed, grad_logits, preferred_element_type=jnp.float32)
    grad_normed = grad_normed + jnp.einsum(
        "re,de->rd", grad_logits, router_full, preferred_element_type=jnp.float32
    )
    _, norm_pullback = jax.vjp(layer_norm, current, gain_row, shift_row)
    grad_input, grad_gain, grad_shift = norm_pullback(grad_normed)
    return (
        grad_states + grad_input,
        grad_router,
        grad_gain,
        grad_shift,
        grad_in_share,
        grad_out_share,
    )


def shards(
    states,
    qkv_weight,
    out_weight,
    norm_gain,
    norm_bias,
    router_weight,
    expert_in,
    expert_out,
    chosen,
    image_count,
    teacher,
):
    qkv_full, out_full, gain_full, bias_full, router_full = (
        lax.all_gather(qkv_weight, "shard", axis=1, tiled=True),
        lax.all_gather(out_weight, "shard", axis=1, tiled=True),
        lax.all_gather(norm_gain, "shard", axis=1, tiled=True),
        lax.all_gather(norm_bias, "shard", axis=1, tiled=True),
        lax.all_gather(router_weight, "shard", axis=1, tiled=True),
    )
    gain_float = gain_full.astype(jnp.float32)
    bias_float = bias_full.astype(jnp.float32)
    layer_count = qkv_weight.shape[0]
    row_count, model_width = states.shape
    slot_image = jnp.arange(row_count, dtype=jnp.int32) // SEQ
    living = slot_image < image_count[0]
    counted = lax.psum(image_count[0].astype(jnp.float32) * SEQ, ("expert", "shard"))
    current = states.astype(jnp.float32)
    attention_kept = []
    mixture_kept = []
    for layer_index in range(layer_count):
        current, kept_attention = attention_forward(
            current,
            qkv_full[layer_index],
            out_full[layer_index],
            gain_float[layer_index, :, 0],
            bias_float[layer_index, :, 0],
        )
        current, kept_mixture = mixture_forward(
            current,
            gain_float[layer_index, :, 1],
            bias_float[layer_index, :, 1],
            router_full[layer_index],
            expert_in[layer_index],
            expert_out[layer_index],
            chosen[layer_index],
        )
        attention_kept.append(kept_attention)
        mixture_kept.append(kept_mixture)
    missed = current - teacher.astype(jnp.float32)
    grad_states = jnp.where(living[:, None], 2.0 * missed, 0.0) / counted
    qkv_list = [None] * layer_count
    out_list = [None] * layer_count
    gain_list = [None] * layer_count
    bias_list = [None] * layer_count
    router_list = [None] * layer_count
    in_list = [None] * layer_count
    experts_out_list = [None] * layer_count
    for layer_index in reversed(range(layer_count)):
        grad_states, grad_router, gain_second, shift_second, grad_in_share, grad_out_share = (
            mixture_backward(
                grad_states,
                mixture_kept[layer_index],
                gain_float[layer_index, :, 1],
                bias_float[layer_index, :, 1],
                router_full[layer_index],
                expert_in[layer_index],
                expert_out[layer_index],
            )
        )
        grad_states, grad_qkv, grad_out, gain_first, shift_first = attention_backward(
            grad_states,
            attention_kept[layer_index],
            qkv_full[layer_index],
            out_full[layer_index],
            gain_float[layer_index, :, 0],
            bias_float[layer_index, :, 0],
        )
        qkv_list[layer_index] = grad_qkv
        out_list[layer_index] = grad_out
        gain_list[layer_index] = jnp.stack([gain_first, gain_second], axis=-1)
        bias_list[layer_index] = jnp.stack([shift_first, shift_second], axis=-1)
        router_list[layer_index] = grad_router
        in_list[layer_index] = grad_in_share
        experts_out_list[layer_index] = grad_out_share
    mixer_grads = (
        jnp.stack(qkv_list),
        jnp.stack(out_list),
        jnp.stack(gain_list),
        jnp.stack(bias_list),
        jnp.stack(router_list),
    )
    summed = lax.psum(
        (mixer_grads[0], mixer_grads[1], mixer_grads[2], mixer_grads[3], mixer_grads[4]),
        ("expert", "shard"),
    )
    share_width = model_width // lax.axis_size("shard")
    start_index = lax.axis_index("shard") * share_width
    reduced = tuple(
        (lax.dynamic_slice_in_dim(member, start_index, share_width, 1) for member in summed)
    )
    return (
        current.astype(jnp.bfloat16),
        grad_states * counted,
        reduced[0],
        reduced[1],
        reduced[2],
        reduced[3],
        reduced[4],
        jnp.stack(in_list),
        jnp.stack(experts_out_list),
    )


def pad_rows(values, fill=0):
    width = values.shape[-1]
    images = values.reshape(SLOTS, SEQ, width)
    images = jnp.pad(images, ((0, 0), (0, SEQ_PAD - SEQ), (0, 0)), constant_values=fill)
    images = images.reshape(SLOTS * SEQ_PAD, width)
    return jnp.pad(images, ((0, ROWS - SLOTS * SEQ_PAD), (0, 0)), constant_values=fill)


def live_rows(values):
    images = values[: SLOTS * SEQ_PAD].reshape(SLOTS, SEQ_PAD, values.shape[-1])
    return images[:, :SEQ].reshape(SLOTS * SEQ, values.shape[-1])


def own_expert(shard_part):
    moved = lax.all_to_all(shard_part, "shard", split_axis=0, concat_axis=0, tiled=True)
    return moved.reshape(-1, shard_part.shape[-1])


def share_expert(grad):
    blocks = grad.reshape(SHARDS, grad.shape[0] // SHARDS, grad.shape[1])
    return lax.all_to_all(blocks, "shard", split_axis=0, concat_axis=0, tiled=True)


def pick_rows(experts):
    _, shard, _, me = position()
    side = experts % SHARDS
    place = (experts // SHARDS * 2 + side % 2 - me + PLACES) % PLACES
    place = jnp.where((experts >= 0) & (side // 2 == shard // 2), place, -1)
    lanes = jnp.concatenate([experts, place], axis=1)
    return jnp.pad(lanes, ((0, 0), (0, LANES - 2 * TOP)), constant_values=-1)


def owners(
    states,
    qkv_weight,
    out_weight,
    norm_gain,
    norm_bias,
    router_weight,
    expert_in,
    expert_out,
    chosen,
    image_count,
    teacher,
):
    layers, share, _ = qkv_weight.shape
    model = states.shape[1]
    groups = lax.axis_size("expert")
    piece = share // groups
    spare = LANES - EXPERTS - 5
    marks = jnp.zeros((layers, share, 1 + spare), BF16)
    packed = jnp.concatenate([qkv_weight, out_weight, router_weight, norm_gain, norm_bias, marks], axis=2)
    packed = lax.dynamic_slice_in_dim(packed, lax.axis_index("expert") * piece, piece, 1)
    mark_at = 4 * model + EXPERTS + 4
    packed = packed.at[0, 0, mark_at].set(image_count[0].astype(BF16))
    mine = [pad_rows(chosen[layer], -1) for layer in range(layers)]
    turned_picks = jnp.concatenate([rows.T for rows in mine] + [jnp.zeros((8 - TOP * layers, ROWS), jnp.int32)])
    first_weights, twin_picks = run_gather(packed[0], turned_picks)
    weights = [first_weights]
    weight_in = own_expert(layer_part(expert_in, 0, image_count))
    counted = jnp.sum(weights[0][:, mark_at].astype(F32)) * SEQ
    slot_image = jnp.arange(states.shape[0], dtype=jnp.int32) // SEQ
    living = slot_image < image_count[0]
    scale = pad_rows(jnp.where(living, 2.0 / counted, 0.0)[:, None])
    theirs = [twin_picks[TOP * layer : TOP * (layer + 1)].T for layer in range(layers)]
    picks = [(pick_rows(mine[layer]), pick_rows(theirs[layer])) for layer in range(layers)]
    kept = []
    current = pad_rows(states.astype(F32))
    x1, proj, logs, att, normed = run_first(current, weights[0])
    for layer in range(layers):
        router = weights[layer][:, 4 * model :]
        mixed = run_mix(
            layer, normed, router, *picks[layer], packed[min(layer + 1, layers - 1)], weight_in, expert_out, expert_in
        )
        delta, slots, turned, chances, gates, arrived, routed, full, act, slope, next_in, weight_out = mixed
        weights.append(full)
        kept.append((current, x1, proj, logs, att, slots, turned, chances, gates, arrived, routed, act, slope, weight_in, weight_out))
        weight_in = next_in
        if layer + 1 < layers:
            current, x1, proj, logs, att, normed = run_middle(x1, delta, weights[layer + 1])
    final, grad, sent = run_last(x1, delta, pad_rows(teacher), scale)
    smalls, ins, outs = [None] * layers, [None] * layers, [None] * layers
    carried = jnp.zeros((SHARDS, expert_out.shape[2], model), BF16)
    for layer in reversed(range(layers)):
        current, x1, proj, logs, att, slots, turned, chances, gates, arrived, routed, act, slope, *own = kept[layer]
        carry = layer + 1 < layers
        sums, grad_gates, grad_in, grad_out, shared = run_unmix(
            grad, sent, gates, routed, slots, turned, arrived, act, slope, *own, carried, carry
        )
        if carry:
            outs[layer + 1] = shared
        carried = grad_out.reshape(carried.shape)
        ins[layer] = share_expert(grad_in)
        grad, sent, smalls[layer] = run_back(
            grad, sums, picks[layer][0], grad_gates, chances, x1, current, proj, logs, att, weights[layer]
        )
    small, outs[0] = run_finish(smalls, carried)
    at = 4 * model
    return (
        live_rows(final),
        live_rows(grad) * counted,
        small[:, :, : 3 * model],
        small[:, :, 3 * model : at],
        small[:, :, at + EXPERTS : at + EXPERTS + 2],
        small[:, :, at + EXPERTS + 2 : at + EXPERTS + 4],
        small[:, :, at : at + EXPERTS],
        jnp.stack(ins).astype(F32),
        jnp.stack(outs).astype(F32),
    )


def plan_of(mesh):
    return owners if owns(mesh) else shards


def owns(mesh):
    groups, shards_all = mesh.shape["expert"], mesh.shape["shard"]
    return shards_all == SHARDS and groups * shards_all == EXPERTS


def solution(mesh):
    in_specs = (
        P(("expert", "shard"), None),
        P(None, "shard", None),
        P(None, "shard", None),
        P(None, "shard", None),
        P(None, "shard", None),
        P(None, "shard", None),
        P(None, "expert", "shard", None),
        P(None, "expert", "shard", None),
        P(None, ("expert", "shard"), None),
        P(("expert", "shard")),
        P(("expert", "shard"), None),
    )
    out_specs = (
        P(("expert", "shard"), None),
        P(("expert", "shard"), None),
        P(None, "shard", None),
        P(None, "shard", None),
        P(None, "shard", None),
        P(None, "shard", None),
        P(None, "shard", None),
        P(None, "expert", "shard", None),
        P(None, "expert", "shard", None),
    )
    return jax.shard_map(plan_of(mesh), mesh=mesh, in_specs=in_specs, out_specs=out_specs, check_vma=False)
```

```python
import functools
import types
import jax
import jax.numpy as jnp
from jax import lax
from jax.experimental import pallas as pl
from jax.experimental.pallas import tpu as pltpu
from jax.sharding import PartitionSpec as P


HEADS = 8
HEAD_DIM = 64
EXPERTS = 32
TOP = 2
SEQ = 197
SLOTS = 3
CAP = 74
norm_eps = 1e-06

LANES = 128
SEQ_PAD = 208
ROWS = 640
CAP_PAD = 80
CHUNK = 64
SHARDS = 4
LIMIT = 62 << 20
F32 = jnp.float32
BF16 = jnp.bfloat16


def dot(a, b):
    return jnp.dot(a, b, preferred_element_type=F32)


def dot_nt(a, b):
    return lax.dot_general(a, b, (((1,), (1,)), ((), ())), preferred_element_type=F32)


def dot_tn(a, b):
    return lax.dot_general(a, b, (((0,), (0,)), ((), ())), preferred_element_type=F32)


def rows_of(step, size):
    return pl.ds(pl.multiple_of(step * size, size), size)


def each_chunk(body, size=CHUNK, total=ROWS):
    def step(i, carry):
        body(rows_of(i, size))
        return carry

    lax.fori_loop(0, total // size, step, 0)


def centre(values):
    centred = values - jnp.mean(values, axis=-1, keepdims=True)
    spread = jnp.mean(centred * centred, axis=-1, keepdims=True)
    return centred, lax.rsqrt(spread + norm_eps)


def norm_rows(x_ref, gain, shift, out_ref):
    def body(rows):
        centred, inverse = centre(x_ref[rows, :])
        out_ref[rows, :] = (centred * inverse * gain + shift).astype(BF16)

    each_chunk(body)


def norm_pullback(x_ref, gain, grad_ref, total_ref, out_ref, sums_ref):
    sums_ref[...] = jnp.zeros_like(sums_ref)

    def body(rows):
        centred, inverse = centre(x_ref[rows, :])
        unit = centred * inverse
        grad = grad_ref[rows, :]
        scaled = grad * gain
        first = jnp.mean(scaled, axis=-1, keepdims=True)
        second = jnp.mean(scaled * unit, axis=-1, keepdims=True)
        out_ref[rows, :] = total_ref[rows, :] + inverse * (scaled - first - unit * second)
        sums_ref[0:1, :] += jnp.sum(grad * unit, axis=0, keepdims=True)
        sums_ref[1:2, :] += jnp.sum(grad, axis=0, keepdims=True)

    each_chunk(body)


def weight_parts(w_ref, model):
    side = jnp.transpose(w_ref[:, 4 * model :].astype(F32))
    return [side[EXPERTS + i : EXPERTS + i + 1, :] for i in range(4)]


def attention_rows(x_ref, w_ref, gain, shift, x1_ref, proj_ref, log_ref, att_ref, normed_ref):
    model = x_ref.shape[1]
    norm_rows(x_ref, gain, shift, normed_ref)
    for part in range(3):
        columns = slice(part * model, (part + 1) * model)
        proj_ref[:, columns] = dot(normed_ref[...], w_ref[:, columns]).astype(BF16)
    att_ref[...] = jnp.zeros_like(att_ref)
    log_ref[...] = jnp.zeros_like(log_ref)
    low = lax.broadcasted_iota(jnp.int32, (SEQ_PAD, LANES), 1) < HEAD_DIM
    inside = lax.broadcasted_iota(jnp.int32, (SEQ_PAD, SEQ_PAD), 1) < SEQ
    lane = lax.broadcasted_iota(jnp.int32, (SEQ_PAD, LANES), 1)

    def image(i, carry):
        rows = rows_of(i, SEQ_PAD)
        logs = jnp.zeros((SEQ_PAD, LANES), F32)
        for pair in range(HEADS // 2):
            at = pair * LANES
            queries = proj_ref[rows, at : at + LANES]
            keys = proj_ref[rows, model + at : model + at + LANES]
            values = proj_ref[rows, 2 * model + at : 2 * model + at + LANES]
            results = []
            for side in range(2):
                mine = low if side == 0 else jnp.logical_not(low)
                masked = jnp.where(mine, queries, jnp.zeros_like(queries))
                scores = dot_nt(masked, keys) * HEAD_DIM ** (-0.5)
                scores = jnp.where(inside, scores, -1e30)
                highest = jnp.max(scores, axis=-1, keepdims=True)
                exponent = jnp.exp(scores - highest)
                summed = jnp.sum(exponent, axis=-1, keepdims=True)
                weights = (exponent / summed).astype(BF16)
                logs = jnp.where(lane == 2 * pair + side, highest + jnp.log(summed), logs)
                results.append(dot(weights, values))
            att_ref[rows, at : at + LANES] = jnp.where(low, results[0], results[1]).astype(BF16)
        log_ref[rows, :] = logs
        return carry

    lax.fori_loop(0, SLOTS, image, 0)
    x1_ref[...] = x_ref[...] + dot(att_ref[...], w_ref[:, 3 * model : 4 * model])


def route_rows(picks, slots_ref, turned_ref):
    lane = lax.broadcasted_iota(jnp.int32, (ROWS, LANES), 1)
    firsts, seconds = picks[:, 0:1], picks[:, 1:2]
    place_first, place_second = picks[:, 2:3], picks[:, 3:4]
    match_first, match_second = lane == firsts, lane == seconds
    either = jnp.where(match_first | match_second, 1.0, 0.0).astype(BF16)
    down = lax.broadcasted_iota(jnp.int32, (ROWS, ROWS), 0)
    across = lax.broadcasted_iota(jnp.int32, (ROWS, ROWS), 1)
    before = dot(jnp.where(across < down, 1.0, 0.0).astype(BF16), either)
    rank_first = jnp.sum(jnp.where(match_first, before, 0.0), axis=-1, keepdims=True)
    rank_second = jnp.sum(jnp.where(match_second, before, 0.0), axis=-1, keepdims=True)
    slot_first = jnp.where(place_first < 0, -1.0, place_first.astype(F32) * CAP_PAD + rank_first)
    slot_second = jnp.where(place_second < 0, -1.0, place_second.astype(F32) * CAP_PAD + rank_second)
    both = jnp.where(lane == 0, slot_first, jnp.where(lane == 1, slot_second, -1.0))
    slots_ref[...] = both.astype(jnp.int32)
    turned_ref[...] = jnp.transpose(both)[0:8, :].astype(jnp.int32)


def gate_rows(normed_ref, router_ref, picks, chances_ref, gates_ref):
    lane = lax.broadcasted_iota(jnp.int32, (ROWS, LANES), 1)
    logits = dot(normed_ref[...], router_ref[...])
    logits = jnp.where(lane < EXPERTS, logits, -1e30)
    exponent = jnp.exp(logits - jnp.max(logits, axis=-1, keepdims=True))
    chances = exponent / jnp.sum(exponent, axis=-1, keepdims=True)
    if chances_ref is not None:
        chances_ref[...] = chances
    gate_first = jnp.sum(jnp.where(lane == picks[:, 0:1], chances, 0.0), axis=-1, keepdims=True)
    gate_second = jnp.sum(jnp.where(lane == picks[:, 1:2], chances, 0.0), axis=-1, keepdims=True)
    gates_ref[...] = jnp.where(lane == 0, gate_first, jnp.where(lane == 1, gate_second, 0.0))


PLACES = EXPERTS // 2
GROUP = 4
BLOCK = GROUP * CAP_PAD
HALF = PLACES * CAP_PAD


def pick_block(turned_ref, group):
    slot = lax.broadcasted_iota(jnp.int32, (BLOCK, ROWS), 0) + group * BLOCK
    return slot == turned_ref[0:1, :], slot == turned_ref[1:2, :]


def as_weights(mask):
    return jnp.where(mask, 1.0, 0.0).astype(BF16)


def dispatch_block(turned_ref, rows_ref, group):
    first, second = pick_block(turned_ref, group)
    return dot(as_weights(first | second), rows_ref[...]).astype(BF16)


def dispatch_pair_block(turned_ref, pairs_ref, group):
    first, second = pick_block(turned_ref, group)
    both = jnp.concatenate([as_weights(first), as_weights(second)], axis=1)
    return dot(both, pairs_ref[...]).astype(BF16)


def ready_dispatch(turned_ref, ready_ref, pairs):
    def step(run, carry):
        first, second = pick_block(turned_ref, run)
        rows = rows_of(run, BLOCK)
        if pairs:
            ready_ref[rows, :ROWS] = as_weights(first)
            ready_ref[rows, ROWS:] = as_weights(second)
        else:
            ready_ref[rows, :ROWS] = as_weights(first | second)
        return carry

    lax.fori_loop(0, PLACES // GROUP, step, 0)


def ready_collect(slots_ref, ready_ref, pairs):
    def body(rows):
        slot = lax.broadcasted_iota(jnp.int32, (CHUNK, HALF), 1)
        slots = slots_ref[rows, :]
        first, second = slot == slots[:, 0:1], slot == slots[:, 1:2]
        if pairs:
            ready_ref[rows, :] = as_weights(first)
            ready_ref[later_rows(rows), :] = as_weights(second)
        else:
            ready_ref[rows, :] = as_weights(first | second)

    each_chunk(body)


def collect_ready(ready_ref, found_ref, side, total_ref):
    def step(run, carry):
        rows = rows_of(run, BLOCK)
        total_ref[rows, :] = dot(ready_ref[rows, :], found_ref[side].reshape(HALF, found_ref.shape[-1]))
        return carry

    lax.fori_loop(0, total_ref.shape[0] // BLOCK, step, 0)


def rows_at(ref, lead, group):
    block = ref[(*lead, pl.ds(group * GROUP, GROUP))]
    return block.reshape(BLOCK, block.shape[-1])


def collect_pairs(slots_ref, found_ref, side, total_ref):
    total_ref[...] = jnp.zeros_like(total_ref)

    def step(group, carry):
        slot = lax.broadcasted_iota(jnp.int32, (ROWS, BLOCK), 1) + group * BLOCK
        rows = rows_at(found_ref, (side,), group)
        for which in range(TOP):
            part = dot(as_weights(slot == slots_ref[:, which : which + 1]), rows)
            total_ref[which * ROWS : (which + 1) * ROWS, :] += part
        return carry

    lax.fori_loop(0, PLACES // GROUP, step, 0)


def collect_sums(slots_ref, found_ref, side, total_ref):
    total_ref[...] = jnp.zeros_like(total_ref)

    def step(group, carry):
        slot = lax.broadcasted_iota(jnp.int32, (ROWS, BLOCK), 1) + group * BLOCK
        chosen = (slot == slots_ref[:, 0:1]) | (slot == slots_ref[:, 1:2])
        total_ref[...] += dot(as_weights(chosen), rows_at(found_ref, (side,), group))
        return carry

    lax.fori_loop(0, PLACES // GROUP, step, 0)


def later_rows(rows):
    return pl.ds(pl.multiple_of(rows.start + ROWS, CHUNK), CHUNK)


def gated_sums(gates_ref, total_ref, routed_ref, side, out_ref):
    def body(rows):
        later = later_rows(rows)
        first, second = total_ref[rows, :], total_ref[later, :]
        gates = gates_ref[side, rows, :]
        out_ref[rows, :] = (gates[:, 0:1] * first + gates[:, 1:2] * second).astype(out_ref.dtype)
        routed_ref[side, rows, :] = first.astype(BF16)
        routed_ref[side, later, :] = second.astype(BF16)

    each_chunk(body)


def gate_grads(grad_ref, gates_ref, routed_ref, side, pairs_ref, grad_gates_ref):
    lane = lax.broadcasted_iota(jnp.int32, (LANES, LANES), 1)

    def body(i, carry):
        rows = rows_of(i, LANES)
        later = pl.ds(pl.multiple_of(i * LANES + ROWS, LANES), LANES)
        grad = grad_ref[rows, :].astype(F32)
        gates = gates_ref[side, rows, :]
        pairs_ref[rows, :] = (gates[:, 0:1] * grad).astype(BF16)
        pairs_ref[later, :] = (gates[:, 1:2] * grad).astype(BF16)
        first = jnp.sum(grad * routed_ref[side, rows, :].astype(F32), axis=-1, keepdims=True)
        second = jnp.sum(grad * routed_ref[side, later, :].astype(F32), axis=-1, keepdims=True)
        both = jnp.where(lane == 0, first, jnp.where(lane == 1, second, 0.0))
        grad_gates_ref[:, rows] = jnp.transpose(both)[0:8, :]
        return carry

    lax.fori_loop(0, ROWS // LANES, body, 0)


def attention_pullback(grad_ref, w_ref, proj_ref, log_ref, att_ref, normed_ref, small_ref, gproj_ref, gatt_ref, back_ref, gnormed_ref):
    model = grad_ref.shape[1]

    def body(rows):
        back_ref[rows, :] = grad_ref[rows, :].astype(BF16)

    each_chunk(body)
    small_ref[:, 3 * model : 4 * model] = dot_tn(att_ref[...], back_ref[...])
    gatt_ref[...] = dot_nt(back_ref[...], w_ref[:, 3 * model : 4 * model]).astype(BF16)
    gproj_ref[SLOTS * SEQ_PAD :, :] = jnp.zeros((ROWS - SLOTS * SEQ_PAD, 3 * model), BF16)
    low = lax.broadcasted_iota(jnp.int32, (SEQ_PAD, LANES), 1) < HEAD_DIM
    inside = lax.broadcasted_iota(jnp.int32, (SEQ_PAD, SEQ_PAD), 1) < SEQ
    scaling = HEAD_DIM ** (-0.5)

    def image(i, carry):
        rows = rows_of(i, SEQ_PAD)
        for pair in range(HEADS // 2):
            at = pair * LANES
            queries = proj_ref[rows, at : at + LANES]
            keys = proj_ref[rows, model + at : model + at + LANES]
            values = proj_ref[rows, 2 * model + at : 2 * model + at + LANES]
            grad_heads = gatt_ref[rows, at : at + LANES]
            parts = []
            for side in range(2):
                mine = low if side == 0 else jnp.logical_not(low)
                zero = jnp.zeros_like(queries)
                head = 2 * pair + side
                scores = dot_nt(jnp.where(mine, queries, zero), keys) * scaling
                chances = jnp.where(inside, jnp.exp(scores - log_ref[rows, head : head + 1]), 0.0)
                grad_weights = dot_nt(jnp.where(mine, grad_heads, zero), values)
                centre_term = jnp.sum(grad_weights * chances, axis=-1, keepdims=True)
                grad_scores = (chances * (grad_weights - centre_term)).astype(BF16)
                parts.append(
                    (
                        dot(grad_scores, keys) * scaling,
                        dot_tn(grad_scores, queries) * scaling,
                        dot_tn(chances.astype(BF16), grad_heads),
                    )
                )
            for which in range(3):
                to = which * model + at
                gproj_ref[rows, to : to + LANES] = jnp.where(low, parts[0][which], parts[1][which]).astype(BF16)
        return carry

    lax.fori_loop(0, SLOTS, image, 0)
    for part in range(3):
        columns = slice(part * model, (part + 1) * model)
        small_ref[:, columns] = dot_tn(normed_ref[...], gproj_ref[:, columns])
    gnormed_ref[...] = dot_nt(gproj_ref[...], w_ref[:, : 3 * model])


def router_pullback(grad_gates_ref, picks_ref, chances_ref, w_ref, normed_ref, gnormed_ref, router_ref):
    model = normed_ref.shape[1]
    lane = lax.broadcasted_iota(jnp.int32, (ROWS, LANES), 1)
    picks, chances = picks_ref[...], chances_ref[...]
    turned = jnp.concatenate([grad_gates_ref[...], jnp.zeros((LANES - 8, ROWS), F32)], axis=0)
    grads = jnp.transpose(turned)
    spread = jnp.where(lane == picks[:, 0:1], grads[:, 0:1], 0.0) + jnp.where(lane == picks[:, 1:2], grads[:, 1:2], 0.0)
    logits = chances * (spread - jnp.sum(spread * chances, axis=-1, keepdims=True))
    logits = logits.astype(BF16)
    router_ref[...] = dot_tn(normed_ref[...], logits)
    gnormed_ref[...] += dot_nt(logits, w_ref[:, 4 * model :])


MESH = pl.DeviceIdType.MESH


def position():
    group, shard = lax.axis_index("expert"), lax.axis_index("shard")
    low = shard % 2
    return group, shard, low, group * 2 + low


def place_id(step):
    _, shard, low, me = position()
    there = (me + step + PLACES) % PLACES
    return (there // 2, shard - low + there % 2)


def twin_id():
    group, shard, _, _ = position()
    return (group, (shard + 2) % SHARDS)


def meet():
    barrier = pltpu.get_barrier_semaphore()
    for k in range(1, PLACES):
        pl.semaphore_signal(barrier, inc=1, device_id=place_id(k), device_id_type=MESH)
    group, shard, low, _ = position()
    for k in range(2):
        there = (shard - low + SHARDS // 2 + k) % SHARDS
        pl.semaphore_signal(barrier, inc=1, device_id=(group, there), device_id_type=MESH)
    pl.semaphore_wait(barrier, PLACES + 1)


SENT = 200


def to_twin(src, dst, sems, at):
    return pltpu.make_async_remote_copy(
        src_ref=src, dst_ref=dst, send_sem=sems.at[0, at], recv_sem=sems.at[1, at], device_id=twin_id(), device_id_type=MESH
    )


class RowSwap:
    def __init__(self, src, dst, sems, at):
        self.dst = dst
        self.copies = []
        for image in range(SLOTS):
            rows = pl.ds(image * SEQ_PAD, SENT)
            self.copies.append(to_twin(src.at[rows], dst.at[rows], sems, at + image))

    @staticmethod
    def clear(dst):
        for image in range(SLOTS):
            stop = (image + 1) * SEQ_PAD
            start = stop - (SEQ_PAD - SENT)
            stop = ROWS if image == SLOTS - 1 else stop
            dst[start:stop, :] = jnp.zeros((stop - start, dst.shape[1]), dst.dtype)

    def start(self):
        for copy in self.copies:
            copy.start()

    def wait_recv(self):
        for copy in self.copies:
            copy.wait_recv()

    def wait_send(self):
        for copy in self.copies:
            copy.wait_send()


def shard_rows(ref, shard):
    rows = ref.shape[0] // SHARDS
    return pl.ds(pl.multiple_of(shard * rows, rows), rows)


def share_blocks(source, target, sems, own_source=None):
    group, shard, _, _ = position()
    copies = [pltpu.make_async_copy(source(shard) if own_source is None else own_source, target(shard), sems.at[1, 0])]
    for k in (2, 1, 3):
        to = (shard + k) % SHARDS
        copies.append(
            pltpu.make_async_remote_copy(
                src_ref=source(to),
                dst_ref=target(shard),
                send_sem=sems.at[0, k],
                recv_sem=sems.at[1, k],
                device_id=(group, to),
                device_id_type=MESH,
            )
        )
    return copies


def stay_copy(src, dst, sems, lane, side):
    return pltpu.make_async_copy(src.at[side, 0], dst.at[side, 0], sems.at[lane, 1, side, 0])


def block_copy(src, dst, sems, lane, side, k, sign):
    return pltpu.make_async_remote_copy(
        src_ref=src.at[side, k],
        dst_ref=dst.at[side, k],
        send_sem=sems.at[lane, 0, side, k],
        recv_sem=sems.at[lane, 1, side, k],
        device_id=place_id(sign * k),
        device_id_type=MESH,
    )


def start_blocks(src, dst, sems, lane, side, run, count, sign):
    first = run * count

    @pl.when(run == 0)
    def _():
        stay_copy(src, dst, sems, lane, side).start()

    @pl.when(run != 0)
    def _():
        block_copy(src, dst, sems, lane, side, first, sign).start()

    for j in range(1, count):
        block_copy(src, dst, sems, lane, side, first + j, sign).start()


def await_blocks(src, dst, sems, lane, side, run, count, sign):
    first = run * count

    @pl.when(run == 0)
    def _():
        stay_copy(src, dst, sems, lane, side).wait()

    @pl.when(run != 0)
    def _():
        block_copy(src, dst, sems, lane, side, first, sign).wait_recv()

    for j in range(1, count):
        block_copy(src, dst, sems, lane, side, first + j, sign).wait_recv()


def await_sent(src, dst, sems, lane, side, sign):
    def step(k, carry):
        block_copy(src, dst, sems, lane, side, k, sign).wait_send()
        return carry

    lax.fori_loop(1, PLACES, step, 0)


def spread(make_block, src, dst, sems, side):
    runs = PLACES // GROUP

    def step(run, carry):
        src[side, pl.ds(run * GROUP, GROUP)] = make_block(run).reshape(GROUP, CAP_PAD, src.shape[-1])

        @pl.when(run > 0)
        def _():
            start_blocks(src, dst, sems, 0, side, run - 1, GROUP, 1)

        return carry

    lax.fori_loop(0, runs, step, 0)
    start_blocks(src, dst, sems, 0, side, runs - 1, GROUP, 1)


def all_back(src, dst, sems, side):
    for run in range(TILES):
        await_blocks(src, dst, sems, 1, side, run, TILE_PLACES, -1)


def pick_lanes(rows_ref, layer):
    _, shard, _, me = position()
    turned = jnp.transpose(jnp.concatenate([rows_ref[...].astype(F32), jnp.zeros((LANES - 8, ROWS), F32)], axis=0))
    lane = lax.broadcasted_iota(jnp.int32, (ROWS, LANES), 1)
    lanes = jnp.full((ROWS, LANES), -1, jnp.int32)
    for which in range(TOP):
        at = TOP * layer + which
        expert = turned[:, at : at + 1].astype(jnp.int32)
        side = expert & (SHARDS - 1)
        place = ((expert >> 2) * 2 + (side & 1) + (PLACES - me)) & (PLACES - 1)
        place = jnp.where((expert >= 0) & ((side >> 1) == shard // 2), place, -1)
        lanes = jnp.where(lane == which, expert, jnp.where(lane == TOP + which, place, lanes))
    return lanes


TILE_PLACES = 8
TILE = TILE_PLACES * CAP_PAD
TILES = PLACES // TILE_PLACES
WIDE = 512
ROOT = 0.7978845608028654
CUBE = 0.044715


class Refs:
    def __init__(self, names, refs):
        self.__dict__.update(zip(names, refs))


def layer_kernel(layer, more, names, kept_names, *refs):
    r = Refs(names, refs)
    h = Refs(kept_names, refs[len(names) :])
    _, shard, _, _ = position()
    opens = layer == 0
    saved = []

    def save(ref, kept, at):
        copy = pltpu.make_async_copy(ref, kept, r.keep_sems.at[at])
        copy.start()
        saved.append(copy)

    model = r.x1_ref.shape[1]
    RowSwap.clear(r.twin_rows)
    RowSwap.clear(r.other)
    r.normed_ref[SLOTS * SEQ_PAD :, :] = jnp.zeros((ROWS - SLOTS * SEQ_PAD, model), BF16)
    if more:
        stage = pltpu.make_async_copy(r.ins_hbm.at[layer + 1, shard], r.stage_ref, r.load_sems.at[1])
        stage.start()
    out_copies = share_blocks(
        lambda to: r.outs_hbm.at[layer, to], lambda own: r.out_ref.at[shard_rows(r.out_ref, own)], r.out_sems
    )
    meet()
    if opens:
        gather = Gather(r.piece_ref, r.w_ref, r.open_far, r.open_flat, r.open_core, r.open_own)
        gather.start()
        picks_copy = to_twin(r.picks_ref, r.theirs_ref, r.pick_sems, 0)
        picks_copy.start()
        in_copies = share_blocks(
            lambda to: r.ins_hbm.at[layer, to], lambda own: r.in_ref.at[shard_rows(r.in_ref, own)], r.in_sems
        )
        for copy in in_copies:
            copy.start()
        states = r.states_ref[...].astype(F32)
        r.x_ref[...] = jnp.zeros_like(r.x_ref)
        for image in range(SLOTS):
            r.x_ref[image * SEQ_PAD : image * SEQ_PAD + SEQ, :] = states[image * SEQ : (image + 1) * SEQ]
        gather.spread()
        gather.pair()
        gather.finish()
        picks_copy.wait()
    else:
        load = pltpu.make_async_copy(r.in_hbm, r.in_ref, r.load_sems.at[0])
        load.start()
        for copy in out_copies[:2]:
            copy.start()

        def body(rows):
            r.x_ref[rows, :] = r.below_ref[rows, :] + r.step_ref[rows, :]

        each_chunk(body)
    gain1, gain2, shift1, shift2 = weight_parts(r.w_ref, model)
    attention_rows(r.x_ref, r.w_ref, gain1, shift1, r.x1_ref, r.proj_ref, r.log_ref, r.att_ref, r.normed_ref)
    norm_rows(r.x1_ref, gain2, shift2, r.normed_ref)
    row_swap = RowSwap(r.normed_ref, r.twin_rows, r.twin_sems, 0)
    row_swap.start()
    for at, (ref, kept) in enumerate(
        ((r.x_ref, h.x_ref), (r.x1_ref, h.x1_ref), (r.proj_ref, h.proj_ref), (r.log_ref, h.log_ref), (r.att_ref, h.att_ref))
    ):
        save(ref, kept, at)
    if more:
        gather = Gather(r.next_piece_ref, r.next_w_ref, r.next_far, r.next_flat, r.next_core, r.next_own)
        gather.start()
        stage.wait()
        next_copies = share_blocks(
            lambda to: r.ins_hbm.at[layer + 1, to],
            lambda own: r.next_hbm.at[shard_rows(r.next_hbm, own)],
            r.next_in_sems,
            r.stage_ref,
        )
    router_ref = r.w_ref.at[:, 4 * model :]
    r.lanes_ref[...] = pick_lanes(r.picks_ref, layer)
    route_rows(r.lanes_ref[...], r.slots_ref.at[0], r.turned_ref.at[0])
    spread(lambda run: dispatch_block(r.turned_ref.at[0], r.normed_ref, run), r.leaving, r.arrived_ref, r.sems, 0)
    for copy in out_copies if opens else out_copies[2:]:
        copy.start()
    gate_rows(r.normed_ref, router_ref, r.lanes_ref[...], r.chances_ref, r.gates_ref.at[0])
    r.twin_lanes[...] = pick_lanes(r.theirs_ref, layer)
    route_rows(r.twin_lanes[...], r.slots_ref.at[1], r.turned_ref.at[1])
    ready_dispatch(r.turned_ref.at[1], r.ready_ref, False)
    row_swap.wait_recv()

    def twin_block(run):
        return dot(r.ready_ref[rows_of(run, BLOCK), :ROWS], r.twin_rows[...]).astype(BF16)

    spread(twin_block, r.leaving, r.arrived_ref, r.sems, 1)
    if more:
        gather.spread()
        for copy in next_copies:
            copy.start()
    gate_rows(r.twin_rows, router_ref, r.twin_lanes[...], None, r.gates_ref.at[1])

    def saves(side, tile):
        to = pl.ds((side * TILES + tile) * TILE, TILE)
        return [
            pltpu.make_async_copy(r.act_ref.at[tile], r.act_hbm.at[to, :], r.save_sems.at[0, tile]),
            pltpu.make_async_copy(r.slope_ref.at[tile], r.slope_hbm.at[to, :], r.save_sems.at[1, tile]),
        ]

    def inner(side, tile):
        await_blocks(r.leaving, r.arrived_ref, r.sems, 0, side, tile, TILE_PLACES, 1)
        rows = r.arrived_ref[side, pl.ds(tile * TILE_PLACES, TILE_PLACES)].reshape(TILE, model)

        def chunk(i, carry):
            columns = rows_of(i, WIDE)
            pre = dot(rows, r.in_ref[:, columns])
            square = pre * pre
            bend = jnp.tanh(pre * (ROOT + ROOT * CUBE * square))
            half = 0.5 + 0.5 * bend
            act = (pre * half).astype(BF16)
            slope = half + (0.5 * pre) * (1.0 - bend * bend) * (ROOT + 3.0 * ROOT * CUBE * square)
            r.act_ref[tile, :, columns] = act
            r.slope_ref[tile, :, columns] = slope.astype(BF16)
            return carry

        lax.fori_loop(0, r.in_ref.shape[1] // WIDE, chunk, 0)

    def outer(side, tile):
        result = dot(r.act_ref[tile], r.out_ref[...]).astype(BF16)
        r.made[side, pl.ds(tile * TILE_PLACES, TILE_PLACES)] = result.reshape(TILE_PLACES, CAP_PAD, model)
        for save in saves(side, tile):
            save.start()
        start_blocks(r.made, r.returned, r.sems, 1, side, tile, TILE_PLACES, -1)

    def each_tile(body):
        def step(tile, carry):
            body(tile)
            return carry

        lax.fori_loop(0, TILES, step, 0)

    if opens:
        for copy in in_copies:
            copy.wait()
        keep_in = pltpu.make_async_copy(r.in_ref, r.kept_in_hbm, r.load_sems.at[0])
        keep_in.start()
    else:
        load.wait()
    each_tile(lambda tile: inner(1, tile))
    for copy in out_copies:
        copy.wait()
    keep = pltpu.make_async_copy(r.out_ref, r.kept_hbm, r.load_sems.at[2])
    keep.start()
    each_tile(lambda tile: outer(1, tile))

    def own_tile(tile):
        for copy in saves(1, tile):
            copy.wait()
        inner(0, tile)
        outer(0, tile)

    own_tile(0)
    ready_collect(r.slots_ref.at[1], r.ready_ref, True)
    all_back(r.made, r.returned, r.sems, 1)
    collect_ready(r.ready_ref, r.returned, 1, r.total)
    gated_sums(r.gates_ref, r.total, r.routed_ref, 1, r.twin_sum)
    sum_swap = RowSwap(r.twin_sum, r.other, r.twin_sems, SLOTS)
    sum_swap.start()
    own_tile(1)
    save(r.arrived_ref, h.arrived_ref, 5)
    if more:
        gather.pair()
    all_back(r.made, r.returned, r.sems, 0)
    collect_pairs(r.slots_ref.at[0], r.returned, 0, r.total)
    gated_sums(r.gates_ref, r.total, r.routed_ref, 0, r.delta_ref)

    def finish_saves(tile):
        for copy in saves(0, tile):
            copy.wait()

    each_tile(finish_saves)
    for side in range(2):
        await_sent(r.leaving, r.arrived_ref, r.sems, 0, side, 1)
        await_sent(r.made, r.returned, r.sems, 1, side, -1)
    row_swap.wait_send()
    keep.wait()
    for copy in saved:
        copy.wait()
    if opens:
        keep_in.wait()
    if more:
        for copy in next_copies:
            copy.wait()
        gather.finish()
    sum_swap.wait_recv()
    sum_swap.wait_send()

    def add_other(rows):
        step = r.delta_ref[rows, :] + r.other[rows, :].astype(F32)
        if more:
            r.delta_ref[rows, :] = step
        else:
            values = r.x1_ref[rows, :] + step
            r.final_ref[rows, :] = values.astype(BF16)
            grad = (values - r.teacher_ref[rows, :].astype(F32)) * r.scale_ref[rows, :]
            r.grad_ref[rows, :] = grad
            r.sent_ref[rows, :] = grad.astype(BF16)

    each_chunk(add_other)


def in_vmem(count):
    return [pl.BlockSpec(memory_space=pltpu.VMEM)] * count


def anywhere(count):
    return [pl.BlockSpec(memory_space=pl.ANY)] * count


def blocks_of(model):
    return pltpu.VMEM((2, PLACES, CAP_PAD, model), BF16)


def run_layer(layer, arrays, in_hbm, expert_out, expert_in):
    layers, _, part, hidden = expert_in.shape
    model = part * SHARDS
    opens, more = layer == 0, layer + 1 < layers
    width = 4 * model + LANES
    hbm_inputs = dict(outs_hbm=expert_out)
    if not opens:
        hbm_inputs.update(in_hbm=in_hbm)
    if opens or more:
        hbm_inputs.update(ins_hbm=expert_in)
    rows_of_kind = lambda kind, columns=model: shape((ROWS, columns), kind)
    kept = dict(
        x_ref=rows_of_kind(F32),
        x1_ref=rows_of_kind(F32),
        proj_ref=rows_of_kind(BF16, 3 * model),
        log_ref=rows_of_kind(F32, LANES),
        att_ref=rows_of_kind(BF16),
        arrived_ref=shape((2, PLACES, CAP_PAD, model), BF16),
    )
    outputs = {}
    if opens:
        outputs.update(w_ref=shape((model, width), BF16), theirs_ref=shape((8, ROWS), jnp.int32))
    if more:
        outputs.update(next_w_ref=shape((model, width), BF16), delta_ref=rows_of_kind(F32))
    else:
        outputs.update(final_ref=rows_of_kind(BF16), grad_ref=rows_of_kind(F32), sent_ref=rows_of_kind(BF16))
    outputs.update(
        lanes_ref=rows_of_kind(jnp.int32, LANES),
        slots_ref=shape((2, ROWS, LANES), jnp.int32),
        turned_ref=shape((2, 8, ROWS), jnp.int32),
        chances_ref=rows_of_kind(F32, LANES),
        gates_ref=shape((2, ROWS, LANES), F32),
        routed_ref=shape((2, TOP * ROWS, model), BF16),
    )
    hbm_outputs = dict(
        act_hbm=shape((2 * HALF, hidden), BF16),
        slope_hbm=shape((2 * HALF, hidden), BF16),
        kept_hbm=shape((hidden, model), BF16),
    )
    if opens:
        hbm_outputs.update(kept_in_hbm=shape((model, hidden), BF16))
    if more:
        hbm_outputs.update(next_hbm=shape((model, hidden), BF16))
    scratch = dict(
        normed_ref=pltpu.VMEM((ROWS, model), BF16),
        twin_rows=pltpu.VMEM((ROWS, model), BF16),
        twin_lanes=pltpu.VMEM((ROWS, LANES), jnp.int32),
        leaving=blocks_of(model),
        made=blocks_of(model),
        returned=blocks_of(model),
        total=pltpu.VMEM((TOP * ROWS, model), F32),
        twin_sum=pltpu.VMEM((ROWS, model), BF16),
        other=pltpu.VMEM((ROWS, model), BF16),
        act_ref=pltpu.VMEM((2, TILE, hidden), BF16),
        slope_ref=pltpu.VMEM((2, TILE, hidden), BF16),
        in_ref=pltpu.VMEM((model, hidden), BF16),
        out_ref=pltpu.VMEM((hidden, model), BF16),
        sems=pltpu.SemaphoreType.DMA((2, 2, 2, PLACES)),
        twin_sems=pltpu.SemaphoreType.DMA((2, 2 * SLOTS)),
        load_sems=pltpu.SemaphoreType.DMA((3,)),
        save_sems=pltpu.SemaphoreType.DMA((2, 2)),
        out_sems=pltpu.SemaphoreType.DMA((2, SHARDS)),
        keep_sems=pltpu.SemaphoreType.DMA((len(kept),)),
        ready_ref=pltpu.VMEM((HALF, TOP * ROWS), BF16),
    )
    scratch.update({name: pltpu.VMEM(kind.shape, kind.dtype) for name, kind in kept.items()})
    far, flat, core, own = gather_sems()
    if opens:
        scratch.update(in_sems=pltpu.SemaphoreType.DMA((2, SHARDS)), pick_sems=pltpu.SemaphoreType.DMA((2, 1)))
        scratch.update(open_far=far, open_flat=flat, open_core=core, open_own=own)
    if more:
        scratch.update(stage_ref=pltpu.VMEM((part, hidden), BF16), next_in_sems=pltpu.SemaphoreType.DMA((2, SHARDS)))
        scratch.update(next_far=far, next_flat=flat, next_core=core, next_own=own)
    else:
        scratch.update(delta_ref=pltpu.VMEM((ROWS, model), F32))
    names = list(arrays) + list(hbm_inputs) + list(outputs) + list(hbm_outputs)
    split = len(names)

    def body(*refs):
        own, saved, rest = refs[:split], refs[split : split + len(kept)], refs[split + len(kept) :]
        layer_kernel(layer, more, names + list(scratch), list(kept), *own, *rest, *saved)

    results = pl.pallas_call(
        body,
        out_shape=list(outputs.values()) + list(hbm_outputs.values()) + list(kept.values()),
        in_specs=in_vmem(len(arrays)) + anywhere(len(hbm_inputs)),
        out_specs=in_vmem(len(outputs)) + anywhere(len(hbm_outputs) + len(kept)),
        scratch_shapes=list(scratch.values()),
        compiler_params=pltpu.CompilerParams(vmem_limit_bytes=LIMIT, collective_id=1 + layer, has_side_effects=True),
        name="layer",
    )(*arrays.values(), *hbm_inputs.values())
    return dict(zip(list(outputs) + list(hbm_outputs) + list(kept), results))


def unmix_kernel(
    carry, grad_ref, sent_ref, gates_ref, slots_ref, turned_ref, routed_hbm, arrived_hbm, act_hbm, slope_hbm, in_hbm, out_hbm, *refs,
):
    if carry:
        carried_hbm, *refs = refs
    sums_ref, grad_gates_ref, gin_hbm, gout_hbm, *refs = refs
    if carry:
        shared_hbm, *refs = refs
    twin_rows, leaving, came, made, returned, pairs, twin_sum, other, twin_gates, other_gates, *refs = refs
    pre_ref, slope_ref, act_ref, arrived_ref, in_ref, out_ref, *refs = refs
    routed_ref, ready_ref, gin_ref, gout_ref, *refs = refs
    sems, twin_sems, load_sems, slope_sems, act_sems, save_sems, *refs = refs
    if carry:
        stage_ref, share_sems = refs
    _, shard, _, _ = position()
    model, hidden = in_ref.shape
    RowSwap.clear(twin_rows)
    RowSwap.clear(other)
    if carry:
        stage = pltpu.make_async_copy(carried_hbm.at[shard], stage_ref, load_sems.at[3])
        stage.start()
    loads = [
        pltpu.make_async_copy(src, dst, load_sems.at[i])
        for i, (src, dst) in enumerate(((in_hbm, in_ref), (out_hbm, out_ref), (arrived_hbm, arrived_ref)))
    ]
    load_routed = pltpu.make_async_copy(routed_hbm, routed_ref, load_sems.at[4])
    load_routed.start()
    for load in loads:
        load.start()

    def slopes(side, tile):
        at = pl.ds((side * TILES + tile) * TILE, TILE)
        return pltpu.make_async_copy(slope_hbm.at[at, :], slope_ref.at[tile], slope_sems.at[tile])

    def acts(chunk):
        slot = chunk % 2
        return pltpu.make_async_copy(act_hbm.at[:, rows_of(chunk, WIDE)], act_ref.at[slot], act_sems.at[slot])

    for tile in range(TILES):
        slopes(0, tile).start()
    for chunk in range(2):
        acts(chunk).start()
    meet()
    row_swap = RowSwap(sent_ref, twin_rows, twin_sems, 0)
    row_swap.start()
    load_routed.wait()
    gate_grads(grad_ref, gates_ref, routed_ref, 0, pairs, grad_gates_ref)
    spread(lambda run: dispatch_pair_block(turned_ref.at[0], pairs, run), leaving, came, sems, 0)
    ready_dispatch(turned_ref.at[1], ready_ref, True)
    row_swap.wait_recv()
    gate_grads(twin_rows, gates_ref, routed_ref, 1, pairs, twin_gates)
    gates_copy = to_twin(twin_gates, other_gates, twin_sems, 2 * SLOTS)
    spread(lambda run: dot(ready_ref[rows_of(run, BLOCK), :], pairs[...]).astype(BF16), leaving, came, sems, 1)
    gates_copy.start()
    share_copies = []
    if carry:
        stage.wait()
        share_copies = share_blocks(lambda to: carried_hbm.at[to], lambda own: shared_hbm.at[own], share_sems, stage_ref)
        for copy in share_copies[:2]:
            copy.start()
    for load in loads:
        load.wait()

    def back_tile(side, tile):
        await_blocks(leaving, came, sems, 0, side, tile, TILE_PLACES, 1)
        slopes(side, tile).wait()
        rows = came[side, pl.ds(tile * TILE_PLACES, TILE_PLACES)].reshape(TILE, model)
        at = rows_of(side * TILES + tile, TILE)

        def chunk(i, carry):
            columns = rows_of(i, WIDE)
            grad_act = dot_nt(rows, out_ref[columns, :])
            pre_ref[at, columns] = (slope_ref[tile, :, columns].astype(F32) * grad_act).astype(BF16)
            return carry

        lax.fori_loop(0, hidden // WIDE, chunk, 0)
        if side == 0:
            slopes(1, tile).start()
        result = dot_nt(pre_ref[at, :], in_ref[...]).astype(BF16)
        made[side, pl.ds(tile * TILE_PLACES, TILE_PLACES)] = result.reshape(TILE_PLACES, CAP_PAD, model)
        start_blocks(made, returned, sems, 1, side, tile, TILE_PLACES, -1)

    for side in range(2):

        def step(tile, carry, side=side):
            back_tile(side, tile)
            return carry

        lax.fori_loop(0, TILES, step, 0)
    for copy in share_copies[2:]:
        copy.start()
    ready_collect(slots_ref.at[1], ready_ref, False)
    all_back(made, returned, sems, 1)
    collect_ready(ready_ref, returned, 1, sums_ref)
    twin_sum[...] = sums_ref[...].astype(BF16)
    sum_swap = RowSwap(twin_sum, other, twin_sems, SLOTS)
    sum_swap.start()
    chunks = hidden // WIDE

    def weigh(chunk, carry):
        columns = rows_of(chunk, WIDE)
        gin_ref[:, columns] = dot_tn(arrived_ref[...].reshape(2 * HALF, model), pre_ref[:, columns]).astype(BF16)
        acts(chunk).wait()
        gout_ref[columns, :] = dot_tn(act_ref[chunk % 2], came[...].reshape(2 * HALF, model)).astype(BF16)

        @pl.when(chunk + 2 < chunks)
        def _():
            acts(chunk + 2).start()

        return carry

    lax.fori_loop(0, chunks, weigh, 0)
    saved = [
        pltpu.make_async_copy(src, dst, save_sems.at[i])
        for i, (src, dst) in enumerate(((gin_ref, gin_hbm), (gout_ref, gout_hbm)))
    ]
    for copy in saved:
        copy.start()
    all_back(made, returned, sems, 0)
    collect_sums(slots_ref.at[0], returned, 0, sums_ref)
    for side in range(2):
        await_sent(leaving, came, sems, 0, side, 1)
        await_sent(made, returned, sems, 1, side, -1)
    row_swap.wait_send()
    gates_copy.wait()
    grad_gates_ref[...] += other_gates[...]
    for copy in saved:
        copy.wait()
    for copy in share_copies:
        copy.wait()
    sum_swap.wait_recv()
    sum_swap.wait_send()

    def body(rows):
        sums_ref[rows, :] += other[rows, :].astype(F32)

    each_chunk(body)


def run_unmix(grad, sent, state, weight_in, carried=()):
    model, hidden = weight_in.shape
    carry = len(carried) > 0
    outs = [shape((ROWS, model), F32), shape((8, ROWS), F32), shape((model, hidden), BF16), shape((hidden, model), BF16)]
    extra = []
    if carry:
        outs += [shape(carried[0].shape, BF16)]
        extra = [
            pltpu.VMEM(carried[0].shape[1:], BF16),
            pltpu.SemaphoreType.DMA((2, SHARDS)),
        ]
    inputs = [grad, sent, state.gates_ref, state.slots_ref, state.turned_ref]
    inputs += [state.routed_ref, state.arrived_ref, state.act_hbm, state.slope_hbm, weight_in, state.kept_hbm, *carried]
    return pl.pallas_call(
        functools.partial(unmix_kernel, carry),
        out_shape=outs,
        in_specs=in_vmem(5) + anywhere(len(inputs) - 5),
        out_specs=in_vmem(2) + anywhere(len(outs) - 2),
        scratch_shapes=[
            pltpu.VMEM((ROWS, model), BF16),
            blocks_of(model),
            blocks_of(model),
            blocks_of(model),
            blocks_of(model),
            pltpu.VMEM((TOP * ROWS, model), BF16),
            pltpu.VMEM((ROWS, model), BF16),
            pltpu.VMEM((ROWS, model), BF16),
            pltpu.VMEM((8, ROWS), F32),
            pltpu.VMEM((8, ROWS), F32),
            pltpu.VMEM((2 * HALF, hidden), BF16),
            pltpu.VMEM((2, TILE, hidden), BF16),
            pltpu.VMEM((2, 2 * HALF, WIDE), BF16),
            blocks_of(model),
            pltpu.VMEM((model, hidden), BF16),
            pltpu.VMEM((hidden, model), BF16),
            pltpu.VMEM((2, TOP * ROWS, model), BF16),
            pltpu.VMEM((HALF, TOP * ROWS), BF16),
            pltpu.VMEM((model, hidden), BF16),
            pltpu.VMEM((hidden, model), BF16),
            pltpu.SemaphoreType.DMA((2, 2, 2, PLACES)),
            pltpu.SemaphoreType.DMA((2, 2 * SLOTS + 1)),
            pltpu.SemaphoreType.DMA((5,)),
            pltpu.SemaphoreType.DMA((2,)),
            pltpu.SemaphoreType.DMA((2,)),
            pltpu.SemaphoreType.DMA((2,)),
        ]
        + extra,
        compiler_params=pltpu.CompilerParams(vmem_limit_bytes=LIMIT, collective_id=3 + int(carry), has_side_effects=True),
        name="unmix",
    )(*inputs)


def flips():
    group = lax.axis_index("expert")
    along = 2 - 4 * (group // 2 % 2)
    up = 4 - 8 * (group // 4)
    return [group + along, group + up, group + along + up]


def other_core():
    group = lax.axis_index("expert")
    return group + 1 - 2 * (group % 2)


def remote(src, dst, send_sem, recv_sem, device):
    return pltpu.make_async_remote_copy(
        src_ref=src, dst_ref=dst, send_sem=send_sem, recv_sem=recv_sem, device_id=device, device_id_type=MESH
    )


def meet_axes():
    group, shard = lax.axis_index("expert"), lax.axis_index("shard")
    barrier = pltpu.get_barrier_semaphore()
    devices = [(group, (shard + k) % SHARDS) for k in range(1, SHARDS)]
    devices += [(there, shard) for there in flips() + [other_core()]]
    for device in devices:
        pl.semaphore_signal(barrier, inc=1, device_id=device, device_id_type=MESH)
    pl.semaphore_wait(barrier, len(devices))


class Gather:
    def __init__(self, piece, full, far_sems, flat_sems, core_sems, own_sem):
        self.group, self.shard = lax.axis_index("expert"), lax.axis_index("shard")
        self.piece, self.full = piece, full
        self.far_sems, self.flat_sems, self.core_sems = far_sems, flat_sems, core_sems
        self.planes = [(self.shard + SHARDS - k) % SHARDS for k in range(SHARDS)]
        self.own = pltpu.make_async_copy(piece, self.rows(self.shard, self.group), own_sem)
        self.sent = []

    def rows(self, plane, there):
        size = self.piece.shape[0]
        span = self.full.shape[0] // SHARDS
        return self.full.at[pl.ds(pl.multiple_of(plane * span + there * size, size), size)]

    def go(self, copy):
        copy.start()
        self.sent.append(copy)

    def far(self, k):
        to = (self.group, (self.shard + k) % SHARDS)
        return remote(self.piece, self.rows(self.shard, self.group), self.far_sems.at[0, k], self.far_sems.at[1, k], to)

    def flat(self, at, p, k):
        return remote(at, at, self.flat_sems.at[0, p, k], self.flat_sems.at[1, p, k], (flips()[p], self.shard))

    def core(self, at, p, k):
        return remote(at, at, self.core_sems.at[0, p, k], self.core_sems.at[1, p, k], (other_core(), self.shard))

    def start(self):
        self.own.start()
        for k in (2, 1, 3):
            self.go(self.far(k))
        self.own.wait()

    def spread(self):
        for k in (0, 1, 3, 2):
            at = self.rows(self.planes[k], self.group)
            if k:
                self.far(k).wait_recv()
            for p in range(3):
                self.go(self.flat(at, p, k))
            self.go(self.core(at, 3, k))

    def pair(self):
        for k in (0, 1, 3, 2):
            for p, there in enumerate(flips()):
                at = self.rows(self.planes[k], there)
                self.flat(at, p, k).wait_recv()
                self.go(self.core(at, p, k))

    def finish(self):
        turn = 1 - 2 * (self.group % 2)
        for k in range(SHARDS):
            for p, there in enumerate(flips() + [self.group]):
                self.core(self.rows(self.planes[k], there + turn), p, k).wait_recv()
        for copy in self.sent:
            copy.wait_send()


def gather_sems():
    return [
        pltpu.SemaphoreType.DMA((2, SHARDS)),
        pltpu.SemaphoreType.DMA((2, 3, SHARDS)),
        pltpu.SemaphoreType.DMA((2, 4, SHARDS)),
        pltpu.SemaphoreType.DMA,
    ]


def finish_kernel(
    layers, *refs
):
    smalls, (carried_hbm, out_ref, shared_hbm, *refs) = refs[:layers], refs[layers:]
    core_ref, leave_ref, came_ref, far_ref, far_came_ref, piece_ref, stage_ref, sum_ref, *refs = refs
    core_sems, flat_sems, far_sems, back_sems, pair_sems, share_sems, stage_sem = refs
    group, shard = lax.axis_index("expert"), lax.axis_index("shard")
    turn = 1 - 2 * (group % 2)
    chip = group // 2
    size = piece_ref.shape[1]
    height = SHARDS * size
    stage = pltpu.make_async_copy(carried_hbm.at[shard], stage_ref, stage_sem)
    stage.start()
    meet_axes()
    pending = []

    def go(copy):
        copy.start()
        pending.append(copy)

    def part(layer, there):
        return smalls[layer].at[pl.ds(pl.multiple_of(there * height, height), height)]

    def core_copy(layer, at):
        chip_at = at // 2
        src = part(layer, chip_at * 2 + 1 - group % 2)
        return remote(src, core_ref.at[layer, chip_at], core_sems.at[0, layer, chip_at], core_sems.at[1, layer, chip_at], (other_core(), shard))

    def flat_copy(p):
        return remote(leave_ref.at[p], came_ref.at[p], flat_sems.at[0, p], flat_sems.at[1, p], (flips()[p], shard))

    order = flips() + [group]
    for there in order:
        for layer in range(layers):
            go(core_copy(layer, there))
    stage.wait()
    shares = share_blocks(lambda to: carried_hbm.at[to], lambda own: shared_hbm.at[own], share_sems, stage_ref)
    for copy in shares[:2]:
        copy.start()
    for p, there in enumerate(order[:3]):
        for layer in range(layers):
            core_copy(layer, there).wait_recv()
            leave_ref[p, layer] = (part(layer, there)[...].astype(F32) + core_ref[layer, there // 2].astype(F32)).astype(BF16)
        if p:
            go(flat_copy(p - 1))
    for layer in range(layers):
        core_copy(layer, group).wait_recv()
    go(flat_copy(2))
    for p in range(3):
        flat_copy(p).wait_recv()
    for layer in range(layers):
        total = part(layer, group)[...].astype(F32) + core_ref[layer, chip].astype(F32)
        for p in range(3):
            total = total + came_ref[p, layer].astype(F32)
        for plane in range(SHARDS):
            far_ref[plane, layer] = total[plane * size : (plane + 1) * size].astype(far_ref.dtype)
        sum_ref[layer] = total

    def far_copy(k):
        to = (shard + k) % SHARDS
        return remote(far_ref.at[to], far_came_ref.at[k], far_sems.at[0, k], far_sems.at[1, k], (group, to))

    for k in (2, 1, 3):
        go(far_copy(k))
    for copy in shares[2:]:
        copy.start()
    for k in (1, 3, 2):
        far_copy(k).wait_recv()
    for layer in range(layers):
        total = sum_ref[layer, pl.ds(pl.multiple_of(shard * size, size), size), :]
        for k in (1, 2, 3):
            total = total + far_came_ref[k, layer].astype(F32)
        piece_ref[layer] = total.astype(BF16)

    def place(there):
        return out_ref.at[:, pl.ds(pl.multiple_of(there * size, size), size)]

    place(group)[...] = piece_ref[...]

    def back_copy(p, at):
        return remote(piece_ref, at, back_sems.at[0, p], back_sems.at[1, p], (flips()[p], shard))

    def pair_copy(p, src, at):
        return remote(src, at, pair_sems.at[0, p], pair_sems.at[1, p], (other_core(), shard))

    for p in range(3):
        go(back_copy(p, place(group)))
    go(pair_copy(3, piece_ref, place(group)))
    for p, there in enumerate(flips()):
        back_copy(p, place(there)).wait_recv()
        go(pair_copy(p, place(there), place(there)))
    for p, there in enumerate(order):
        pair_copy(p, piece_ref, place(there + turn)).wait_recv()
    for copy in pending:
        copy.wait_send()
    for copy in shares:
        copy.wait()


def run_finish(smalls, carried):
    layers = len(smalls)
    groups = EXPERTS // SHARDS
    rows, width = smalls[0].shape
    span = rows // SHARDS
    size = span // groups
    chips = groups // 2
    height = SHARDS * size
    return pl.pallas_call(
        functools.partial(finish_kernel, layers),
        out_shape=[shape((layers, span, width), BF16), shape(carried.shape, BF16)],
        in_specs=in_vmem(layers) + anywhere(1),
        out_specs=in_vmem(1) + anywhere(1),
        scratch_shapes=[
            pltpu.VMEM((layers, chips, height, width), BF16),
            pltpu.VMEM((3, layers, height, width), BF16),
            pltpu.VMEM((3, layers, height, width), BF16),
            pltpu.VMEM((SHARDS, layers, size, width), BF16),
            pltpu.VMEM((SHARDS, layers, size, width), BF16),
            pltpu.VMEM((layers, size, width), BF16),
            pltpu.VMEM(carried.shape[1:], BF16),
            pltpu.VMEM((layers, height, width), F32),
            pltpu.SemaphoreType.DMA((2, layers, chips)),
            pltpu.SemaphoreType.DMA((2, 3)),
            pltpu.SemaphoreType.DMA((2, SHARDS)),
            pltpu.SemaphoreType.DMA((2, 3)),
            pltpu.SemaphoreType.DMA((2, 4)),
            pltpu.SemaphoreType.DMA((2, SHARDS)),
            pltpu.SemaphoreType.DMA,
        ],
        compiler_params=pltpu.CompilerParams(vmem_limit_bytes=48 << 20, collective_id=6, has_side_effects=True),
        name="finish",
    )(*smalls, carried)


def back_kernel(grad_in_ref, sums_ref, picks_ref, grad_gates_ref, chances_ref, x1_ref, x_ref, proj_ref, log_ref, att_ref, w_ref, grad_ref, sent_ref, parts_ref, normed_ref, gnormed_ref, gproj_ref, gatt_ref, back_ref, mid_ref, sums_a, sums_b, router_ref, small_ref):
    model = x_ref.shape[1]
    gain1, gain2, shift1, shift2 = weight_parts(w_ref, model)
    gnormed_ref[...] = sums_ref[...]
    norm_rows(x1_ref, gain2, shift2, normed_ref)
    router_pullback(grad_gates_ref, picks_ref, chances_ref, w_ref, normed_ref, gnormed_ref, router_ref)
    norm_pullback(x1_ref, gain2, gnormed_ref, grad_in_ref, mid_ref, sums_b)
    norm_rows(x_ref, gain1, shift1, normed_ref)
    attention_pullback(mid_ref, w_ref, proj_ref, log_ref, att_ref, normed_ref, small_ref, gproj_ref, gatt_ref, back_ref, gnormed_ref)
    norm_pullback(x_ref, gain1, gnormed_ref, mid_ref, grad_ref, sums_a)
    sent_ref[...] = grad_ref[...].astype(BF16)
    rows = lax.broadcasted_iota(jnp.int32, (LANES, model), 0)
    side = jnp.zeros((LANES, model), F32)
    for i, value in enumerate((sums_a[0:1, :], sums_b[0:1, :], sums_a[1:2, :], sums_b[1:2, :])):
        side = jnp.where(rows == EXPERTS + i, value, side)
    lane = lax.broadcasted_iota(jnp.int32, (model, LANES), 1)
    small_ref[:, 4 * model :] = jnp.where(lane < EXPERTS, router_ref[...], jnp.transpose(side))
    size = model // EXPERTS
    for at in range(EXPERTS):
        shard, group = at % SHARDS, at // SHARDS
        row = (shard * (EXPERTS // SHARDS) + group) * size
        parts_ref[at * size : (at + 1) * size, :] = small_ref[row : row + size, :].astype(BF16)


def shape(dims, kind):
    return jax.ShapeDtypeStruct(dims, kind)


def run_back(grad, sums, grad_gates, state):
    model = grad.shape[1]
    width = 4 * model + LANES
    inputs = [grad, sums, state.lanes_ref, grad_gates, state.chances_ref, state.x1_ref, state.x_ref]
    inputs += [state.proj_ref, state.log_ref, state.att_ref, state.w_ref]
    return pl.pallas_call(
        back_kernel,
        out_shape=[shape((ROWS, model), F32), shape((ROWS, model), BF16), shape((model, width), BF16)],
        in_specs=in_vmem(len(inputs)),
        out_specs=in_vmem(3),
        scratch_shapes=[
            pltpu.VMEM((ROWS, model), BF16),
            pltpu.VMEM((ROWS, model), F32),
            pltpu.VMEM((ROWS, 3 * model), BF16),
            pltpu.VMEM((ROWS, model), BF16),
            pltpu.VMEM((ROWS, model), BF16),
            pltpu.VMEM((ROWS, model), F32),
            pltpu.VMEM((2, model), F32),
            pltpu.VMEM((2, model), F32),
            pltpu.VMEM((model, LANES), F32),
            pltpu.VMEM((model, width), F32),
        ],
        compiler_params=pltpu.CompilerParams(vmem_limit_bytes=56 << 20),
        name="back",
    )(*inputs)


def output_kernel(layers, *refs):
    ins, outs = refs[:layers], refs[layers : 2 * layers]
    small_ref, grad_ref, count_ref = refs[2 * layers : 2 * layers + 3]
    in_ref, out_ref, qkv_ref, mix_ref, side_ref, input_ref = refs[2 * layers + 3 :]
    step = pl.program_id(0)
    model = grad_ref.shape[1]
    for layer in range(layers):

        @pl.when(step // SHARDS == layer)
        def _(layer=layer):
            in_ref[...] = ins[layer][...].astype(F32).reshape(in_ref.shape)
            out_ref[...] = outs[layer][...].astype(F32).reshape(out_ref.shape)

    @pl.when(step == 0)
    def _():
        qkv_ref[...] = small_ref[:, :, : 3 * model].astype(F32)
        mix_ref[...] = small_ref[:, :, 3 * model : 4 * model].astype(F32)
        side_ref[...] = small_ref[:, :, 4 * model :].astype(F32)
        for image in range(SLOTS):
            to, rows = image * SEQ, image * SEQ_PAD
            input_ref[to : to + SEQ, :] = grad_ref[rows : rows + SEQ, :] * count_ref[0]


def run_output(ins, outs, small, grad, counted):
    layers = len(ins)
    model = grad.shape[1]
    span = small.shape[1]

    def block(array, layer):
        at = lambda i: (jnp.clip(i - layer * SHARDS, 0, SHARDS - 1), 0, 0)
        return pl.BlockSpec((1,) + array.shape[1:], at)

    whole = lambda dims: pl.BlockSpec(dims, lambda i: (0,) * len(dims))
    filled = lambda array: pl.BlockSpec((1, 1) + array.shape[1:], lambda i: (i // SHARDS, i % SHARDS, 0, 0))
    small_shapes = [(layers, span, 3 * model), (layers, span, model), (layers, span, LANES), (SLOTS * SEQ, model)]
    return pl.pallas_call(
        functools.partial(output_kernel, layers),
        grid=(layers * SHARDS,),
        in_specs=[block(array, layer) for layer, array in enumerate(ins)]
        + [block(array, layer) for layer, array in enumerate(outs)]
        + [whole(small.shape), whole(grad.shape), pl.BlockSpec(memory_space=pltpu.SMEM)],
        out_specs=[filled(ins[0]), filled(outs[0])] + [whole(dims) for dims in small_shapes],
        out_shape=[shape((layers,) + ins[0].shape, F32), shape((layers,) + outs[0].shape, F32)]
        + [shape(dims, F32) for dims in small_shapes],
        compiler_params=pltpu.CompilerParams(vmem_limit_bytes=48 << 20),
        name="output",
    )(*ins, *outs, small, grad, counted)


def layer_norm(values, gain_row, shift_row):
    centred = values - jnp.mean(values, axis=-1, keepdims=True)
    spread = jnp.mean(centred * centred, axis=-1, keepdims=True)
    return centred * lax.rsqrt(spread + norm_eps) * gain_row + shift_row


def route_slots(picks_dev, capacity):
    flat_ids = picks_dev.reshape(-1)
    onehot = (flat_ids[:, None] == jnp.arange(EXPERTS, dtype=jnp.int32)[None, :]).astype(jnp.int32)
    before = jnp.cumsum(onehot, axis=0) - onehot
    ranking = jnp.sum(before * onehot, axis=1)
    slot_index = flat_ids * capacity + ranking
    routes_dev = flat_ids.shape[0]
    source = jnp.full((EXPERTS * capacity,), routes_dev, jnp.int32)
    source = source.at[slot_index].set(jnp.arange(routes_dev, dtype=jnp.int32))
    return (slot_index, source)


def attention_forward(current, qkv_full, out_full, gain_row, shift_row):
    model_width = current.shape[1]
    normed = layer_norm(current, gain_row, shift_row).astype(jnp.bfloat16)
    projected = jnp.dot(normed, qkv_full, preferred_element_type=jnp.float32).astype(jnp.bfloat16)
    split_parts = projected.reshape(SLOTS, SEQ, 3, HEADS, HEAD_DIM)
    scores = jnp.einsum(
        "ashd,athd->ahst",
        split_parts[:, :, 0],
        split_parts[:, :, 1],
        preferred_element_type=jnp.float32,
    ) * HEAD_DIM ** (-0.5)
    highest_score = jnp.max(scores, axis=-1, keepdims=True)
    exponent = jnp.exp(scores - highest_score)
    summed = jnp.sum(exponent, axis=-1, keepdims=True)
    weights = (exponent / summed).astype(jnp.bfloat16)
    log_total = highest_score + jnp.log(summed)
    attended = jnp.einsum(
        "ahst,athd->ashd", weights, split_parts[:, :, 2], preferred_element_type=jnp.float32
    )
    attended = attended.reshape(SLOTS * SEQ, model_width).astype(jnp.bfloat16)
    branch_out = jnp.dot(attended, out_full, preferred_element_type=jnp.float32)
    return (current + branch_out, (current, normed, projected, log_total, attended))


def attention_backward(grad_states, saved, qkv_full, out_full, gain_row, shift_row):
    current, normed, projected, log_total, attended = saved
    model_width = current.shape[1]
    grad_branch = grad_states.astype(jnp.bfloat16)
    grad_out = jnp.einsum("rd,re->de", attended, grad_branch, preferred_element_type=jnp.float32)
    grad_attended = jnp.einsum(
        "re,de->rd", grad_branch, out_full, preferred_element_type=jnp.float32
    ).astype(jnp.bfloat16)
    split_parts = projected.reshape(SLOTS, SEQ, 3, HEADS, HEAD_DIM)
    queries = split_parts[:, :, 0]
    keys_part = split_parts[:, :, 1]
    values_part = split_parts[:, :, 2]
    scaling = HEAD_DIM ** (-0.5)
    scores = (
        jnp.einsum("ashd,athd->ahst", queries, keys_part, preferred_element_type=jnp.float32)
        * scaling
    )
    chances = jnp.exp(scores - log_total)
    grad_heads = grad_attended.reshape(SLOTS, SEQ, HEADS, HEAD_DIM)
    grad_weights = jnp.einsum(
        "ashd,athd->ahst", grad_heads, values_part, preferred_element_type=jnp.float32
    )
    grad_values = jnp.einsum(
        "ahst,ashd->athd",
        chances.astype(jnp.bfloat16),
        grad_heads,
        preferred_element_type=jnp.float32,
    )
    centre_term = jnp.sum(grad_weights * chances, axis=-1, keepdims=True)
    grad_scores = (chances * (grad_weights - centre_term)).astype(jnp.bfloat16)
    grad_queries = (
        jnp.einsum("ahst,athd->ashd", grad_scores, keys_part, preferred_element_type=jnp.float32)
        * scaling
    )
    grad_keys = (
        jnp.einsum("ahst,ashd->athd", grad_scores, queries, preferred_element_type=jnp.float32)
        * scaling
    )
    grad_projected = jnp.stack([grad_queries, grad_keys, grad_values], axis=2)
    grad_projected = grad_projected.reshape(SLOTS * SEQ, 3 * model_width).astype(jnp.bfloat16)
    grad_qkv = jnp.einsum("rd,re->de", normed, grad_projected, preferred_element_type=jnp.float32)
    grad_normed = jnp.einsum(
        "re,de->rd", grad_projected, qkv_full, preferred_element_type=jnp.float32
    )
    _, norm_pullback = jax.vjp(layer_norm, current, gain_row, shift_row)
    grad_input, grad_gain, grad_shift = norm_pullback(grad_normed)
    return (grad_states + grad_input, grad_qkv, grad_out, grad_gain, grad_shift)


def mixture_forward(current, gain_row, shift_row, router_full, in_shard, out_shard, picks_layer):
    row_count, model_width = current.shape
    experts_all = router_full.shape[1]
    normed = layer_norm(current, gain_row, shift_row).astype(jnp.bfloat16)
    logits = jnp.dot(normed, router_full, preferred_element_type=jnp.float32)
    chances = jax.nn.softmax(logits, axis=-1)
    matches = picks_layer[:, :, None] == jnp.arange(experts_all, dtype=jnp.int32)[None, None, :]
    gate_values = jnp.sum(jnp.where(matches, chances[:, None, :], 0.0), axis=-1)
    slot_index, source = route_slots(picks_layer, CAP)
    filled = source < TOP * row_count
    route_clip = jnp.minimum(source, TOP * row_count - 1)
    taken_rows = route_clip // TOP
    outgoing = jnp.where(filled[:, None], normed[taken_rows], jnp.zeros((), jnp.bfloat16))
    outgoing = outgoing.reshape(experts_all, CAP, model_width)
    arrived = lax.all_to_all(outgoing, "expert", split_axis=0, concat_axis=1, tiled=True)
    in_full, out_full = (
        lax.all_gather(in_shard, "shard", axis=1, tiled=True),
        lax.all_gather(out_shard, "shard", axis=1, tiled=True),
    )
    hidden_pre = jnp.einsum("erd,edh->erh", arrived, in_full, preferred_element_type=jnp.float32)
    activated = jax.nn.gelu(hidden_pre).astype(jnp.bfloat16)
    produced = jnp.einsum(
        "erh,ehd->erd", activated, out_full, preferred_element_type=jnp.float32
    ).astype(jnp.bfloat16)
    returned = lax.all_to_all(produced, "expert", split_axis=1, concat_axis=0, tiled=True)
    routed = returned.reshape(experts_all * CAP, model_width)[slot_index].reshape(
        row_count, TOP, model_width
    )
    updated = current + jnp.sum(gate_values[:, :, None] * routed.astype(jnp.float32), axis=1)
    saved = (
        current,
        normed,
        chances,
        matches,
        gate_values,
        slot_index,
        filled,
        route_clip,
        arrived,
        routed,
        in_full,
        out_full,
    )
    return (updated, saved)


def mixture_backward(grad_states, saved, gain_row, shift_row, router_full, in_shard, out_shard):
    (current, normed, chances, matches, gate_values, slot_index, filled, route_clip, arrived, routed, _, _) = saved
    row_count, model_width = current.shape
    experts_all = chances.shape[1]
    grad_routed = (gate_values[:, :, None] * grad_states[:, None, :]).astype(jnp.bfloat16)
    grad_routed = grad_routed.reshape(TOP * row_count, model_width)
    grad_gates = jnp.sum(grad_states[:, None, :] * routed.astype(jnp.float32), axis=-1)
    grad_outgoing = jnp.where(filled[:, None], grad_routed[route_clip], jnp.zeros((), jnp.bfloat16))
    grad_outgoing = grad_outgoing.reshape(experts_all, CAP, model_width)
    grad_result = lax.all_to_all(grad_outgoing, "expert", split_axis=0, concat_axis=1, tiled=True)
    in_full, out_full = (
        lax.all_gather(in_shard, "shard", axis=1, tiled=True),
        lax.all_gather(out_shard, "shard", axis=1, tiled=True),
    )
    hidden_pre = jnp.einsum("erd,edh->erh", arrived, in_full, preferred_element_type=jnp.float32)
    activated, gelu_pullback = jax.vjp(jax.nn.gelu, hidden_pre)
    grad_out_experts = jnp.einsum(
        "erh,erd->ehd",
        activated.astype(jnp.bfloat16),
        grad_result,
        preferred_element_type=jnp.float32,
    )
    grad_activated = jnp.einsum(
        "erd,ehd->erh", grad_result, out_full, preferred_element_type=jnp.float32
    )
    grad_pre = gelu_pullback(grad_activated)[0].astype(jnp.bfloat16)
    grad_in_experts = jnp.einsum(
        "erd,erh->edh", arrived, grad_pre, preferred_element_type=jnp.float32
    )
    grad_arrived = jnp.einsum(
        "erh,edh->erd", grad_pre, in_full, preferred_element_type=jnp.float32
    ).astype(jnp.bfloat16)
    grad_returned = lax.all_to_all(grad_arrived, "expert", split_axis=1, concat_axis=0, tiled=True)
    grad_in_share, grad_out_share = (
        lax.psum_scatter(
            grad_in_experts.astype(jnp.bfloat16), "shard", scatter_dimension=1, tiled=True
        ).astype(jnp.float32),
        lax.psum_scatter(
            grad_out_experts.astype(jnp.bfloat16), "shard", scatter_dimension=1, tiled=True
        ).astype(jnp.float32),
    )
    grad_routes = grad_returned.reshape(experts_all * CAP, model_width)[slot_index]
    grad_normed = jnp.sum(
        grad_routes.reshape(row_count, TOP, model_width).astype(jnp.float32), axis=1
    )
    grad_chances = jnp.sum(jnp.where(matches, grad_gates[:, :, None], 0.0), axis=1)
    grad_logits = chances * (grad_chances - jnp.sum(grad_chances * chances, axis=-1, keepdims=True))
    grad_logits = grad_logits.astype(jnp.bfloat16)
    grad_router = jnp.einsum("rd,re->de", normed, grad_logits, preferred_element_type=jnp.float32)
    grad_normed = grad_normed + jnp.einsum(
        "re,de->rd", grad_logits, router_full, preferred_element_type=jnp.float32
    )
    _, norm_pullback = jax.vjp(layer_norm, current, gain_row, shift_row)
    grad_input, grad_gain, grad_shift = norm_pullback(grad_normed)
    return (
        grad_states + grad_input,
        grad_router,
        grad_gain,
        grad_shift,
        grad_in_share,
        grad_out_share,
    )


def shards(
    states,
    qkv_weight,
    out_weight,
    norm_gain,
    norm_bias,
    router_weight,
    expert_in,
    expert_out,
    chosen,
    image_count,
    teacher,
):
    qkv_full, out_full, gain_full, bias_full, router_full = (
        lax.all_gather(qkv_weight, "shard", axis=1, tiled=True),
        lax.all_gather(out_weight, "shard", axis=1, tiled=True),
        lax.all_gather(norm_gain, "shard", axis=1, tiled=True),
        lax.all_gather(norm_bias, "shard", axis=1, tiled=True),
        lax.all_gather(router_weight, "shard", axis=1, tiled=True),
    )
    gain_float = gain_full.astype(jnp.float32)
    bias_float = bias_full.astype(jnp.float32)
    layer_count = qkv_weight.shape[0]
    row_count, model_width = states.shape
    slot_image = jnp.arange(row_count, dtype=jnp.int32) // SEQ
    living = slot_image < image_count[0]
    counted = lax.psum(image_count[0].astype(jnp.float32) * SEQ, ("expert", "shard"))
    current = states.astype(jnp.float32)
    attention_kept = []
    mixture_kept = []
    for layer_index in range(layer_count):
        current, kept_attention = attention_forward(
            current,
            qkv_full[layer_index],
            out_full[layer_index],
            gain_float[layer_index, :, 0],
            bias_float[layer_index, :, 0],
        )
        current, kept_mixture = mixture_forward(
            current,
            gain_float[layer_index, :, 1],
            bias_float[layer_index, :, 1],
            router_full[layer_index],
            expert_in[layer_index],
            expert_out[layer_index],
            chosen[layer_index],
        )
        attention_kept.append(kept_attention)
        mixture_kept.append(kept_mixture)
    missed = current - teacher.astype(jnp.float32)
    grad_states = jnp.where(living[:, None], 2.0 * missed, 0.0) / counted
    qkv_list = [None] * layer_count
    out_list = [None] * layer_count
    gain_list = [None] * layer_count
    bias_list = [None] * layer_count
    router_list = [None] * layer_count
    in_list = [None] * layer_count
    experts_out_list = [None] * layer_count
    for layer_index in reversed(range(layer_count)):
        grad_states, grad_router, gain_second, shift_second, grad_in_share, grad_out_share = (
            mixture_backward(
                grad_states,
                mixture_kept[layer_index],
                gain_float[layer_index, :, 1],
                bias_float[layer_index, :, 1],
                router_full[layer_index],
                expert_in[layer_index],
                expert_out[layer_index],
            )
        )
        grad_states, grad_qkv, grad_out, gain_first, shift_first = attention_backward(
            grad_states,
            attention_kept[layer_index],
            qkv_full[layer_index],
            out_full[layer_index],
            gain_float[layer_index, :, 0],
            bias_float[layer_index, :, 0],
        )
        qkv_list[layer_index] = grad_qkv
        out_list[layer_index] = grad_out
        gain_list[layer_index] = jnp.stack([gain_first, gain_second], axis=-1)
        bias_list[layer_index] = jnp.stack([shift_first, shift_second], axis=-1)
        router_list[layer_index] = grad_router
        in_list[layer_index] = grad_in_share
        experts_out_list[layer_index] = grad_out_share
    mixer_grads = (
        jnp.stack(qkv_list),
        jnp.stack(out_list),
        jnp.stack(gain_list),
        jnp.stack(bias_list),
        jnp.stack(router_list),
    )
    summed = lax.psum(
        (mixer_grads[0], mixer_grads[1], mixer_grads[2], mixer_grads[3], mixer_grads[4]),
        ("expert", "shard"),
    )
    share_width = model_width // lax.axis_size("shard")
    start_index = lax.axis_index("shard") * share_width
    reduced = tuple(
        (lax.dynamic_slice_in_dim(member, start_index, share_width, 1) for member in summed)
    )
    return (
        current.astype(jnp.bfloat16),
        grad_states * counted,
        reduced[0],
        reduced[1],
        reduced[2],
        reduced[3],
        reduced[4],
        jnp.stack(in_list),
        jnp.stack(experts_out_list),
    )


def pad_rows(values, fill=0):
    width = values.shape[-1]
    images = values.reshape(SLOTS, SEQ, width)
    images = jnp.pad(images, ((0, 0), (0, SEQ_PAD - SEQ), (0, 0)), constant_values=fill)
    images = images.reshape(SLOTS * SEQ_PAD, width)
    return jnp.pad(images, ((0, ROWS - SLOTS * SEQ_PAD), (0, 0)), constant_values=fill)


def live_rows(values):
    images = values[: SLOTS * SEQ_PAD].reshape(SLOTS, SEQ_PAD, values.shape[-1])
    return images[:, :SEQ].reshape(SLOTS * SEQ, values.shape[-1])


def owners(
    states,
    qkv_weight,
    out_weight,
    norm_gain,
    norm_bias,
    router_weight,
    expert_in,
    expert_out,
    chosen,
    image_count,
    teacher,
):
    layers, share, _ = qkv_weight.shape
    model = states.shape[1]
    groups = lax.axis_size("expert")
    piece = share // groups
    spare = LANES - EXPERTS - 5
    marks = jnp.zeros((layers, share, 1 + spare), BF16)
    packed = jnp.concatenate([qkv_weight, out_weight, router_weight, norm_gain, norm_bias, marks], axis=2)
    packed = lax.dynamic_slice_in_dim(packed, lax.axis_index("expert") * piece, piece, 1)
    mark_at = 4 * model + EXPERTS + 4
    packed = packed.at[0, 0, mark_at].set(image_count[0].astype(BF16))
    picks = [pad_rows(chosen[layer], -1).T for layer in range(layers)]
    picks = jnp.concatenate(picks + [jnp.full((8 - TOP * layers, ROWS), -1, jnp.int32)])
    arrays = dict(states_ref=states, piece_ref=packed[0], picks_ref=picks)
    kept = []
    next_in = None
    for layer in range(layers):
        more = layer + 1 < layers
        if more:
            arrays.update(next_piece_ref=packed[layer + 1])
        made = run_layer(layer, arrays, next_in, expert_out, expert_in)
        state = types.SimpleNamespace(**arrays, **made)
        kept.append(state)
        if layer == 0:
            counted = jnp.sum(state.w_ref[:, mark_at].astype(F32)) * SEQ
            slot_image = jnp.arange(states.shape[0], dtype=jnp.int32) // SEQ
            living = slot_image < image_count[0]
            scale = pad_rows(jnp.where(living, 2.0 / counted, 0.0)[:, None])
        if more:
            next_in = state.next_hbm
            arrays = dict(
                below_ref=state.x1_ref,
                step_ref=state.delta_ref,
                w_ref=state.next_w_ref,
                picks_ref=picks,
                theirs_ref=kept[0].theirs_ref,
            )
        if layer + 2 == layers:
            arrays.update(teacher_ref=pad_rows(teacher), scale_ref=scale)
    grad, sent = state.grad_ref, state.sent_ref
    smalls, ins, outs = [None] * layers, [None] * layers, [None] * layers
    carried = ()
    for layer in reversed(range(layers)):
        state = kept[layer]
        own_in = kept[layer - 1].next_hbm if layer else state.kept_in_hbm
        sums, grad_gates, grad_in, grad_out, *shared = run_unmix(grad, sent, state, own_in, carried)
        if shared:
            (outs[layer + 1],) = shared
        blocks = lambda part: part.reshape(SHARDS, part.shape[0] // SHARDS, part.shape[1])
        carried = (blocks(grad_out),)
        ins[layer] = lax.all_to_all(blocks(grad_in), "shard", split_axis=0, concat_axis=0, tiled=True)
        grad, sent, smalls[layer] = run_back(grad, sums, grad_gates, state)
    small, outs[0] = run_finish(smalls, *carried)
    final = kept[-1].final_ref
    in_grad, out_grad, qkv, mixed, side, first_grad = run_output(ins, outs, small, grad, counted.reshape(1))
    return (
        live_rows(final),
        first_grad,
        qkv,
        mixed,
        side[:, :, EXPERTS : EXPERTS + 2],
        side[:, :, EXPERTS + 2 : EXPERTS + 4],
        side[:, :, :EXPERTS],
        in_grad,
        out_grad,
    )


def plan_of(mesh):
    return owners if owns(mesh) else shards


def owns(mesh):
    groups, shards_all = mesh.shape["expert"], mesh.shape["shard"]
    return shards_all == SHARDS and groups * shards_all == EXPERTS


def solution(mesh):
    in_specs = (
        P(("expert", "shard"), None),
        P(None, "shard", None),
        P(None, "shard", None),
        P(None, "shard", None),
        P(None, "shard", None),
        P(None, "shard", None),
        P(None, "expert", "shard", None),
        P(None, "expert", "shard", None),
        P(None, ("expert", "shard"), None),
        P(("expert", "shard")),
        P(("expert", "shard"), None),
    )
    out_specs = (
        P(("expert", "shard"), None),
        P(("expert", "shard"), None),
        P(None, "shard", None),
        P(None, "shard", None),
        P(None, "shard", None),
        P(None, "shard", None),
        P(None, "shard", None),
        P(None, "expert", "shard", None),
        P(None, "expert", "shard", None),
    )
    return jax.shard_map(plan_of(mesh), mesh=mesh, in_specs=in_specs, out_specs=out_specs, check_vma=False)
```

```python
import functools
import types
import jax
import jax.numpy as jnp
from jax import lax
from jax.experimental import pallas as pl
from jax.experimental.pallas import tpu as pltpu
from jax.sharding import PartitionSpec as P


HEADS = 8
HEAD_DIM = 64
EXPERTS = 32
TOP = 2
SEQ = 197
SLOTS = 3
CAP = 74
norm_eps = 1e-06

LANES = 128
SEQ_PAD = 208
ROWS = 640
CAP_PAD = 80
CHUNK = 64
SHARDS = 4
LIMIT = 62 << 20
F32 = jnp.float32
BF16 = jnp.bfloat16


def dot(a, b):
    return jnp.dot(a, b, preferred_element_type=F32)


def dot_nt(a, b):
    return lax.dot_general(a, b, (((1,), (1,)), ((), ())), preferred_element_type=F32)


def dot_tn(a, b):
    return lax.dot_general(a, b, (((0,), (0,)), ((), ())), preferred_element_type=F32)


def rows_of(step, size):
    return pl.ds(pl.multiple_of(step * size, size), size)


def each_chunk(body, size=CHUNK, total=ROWS):
    def step(i, carry):
        body(rows_of(i, size))
        return carry

    lax.fori_loop(0, total // size, step, 0)


def centre(values):
    centred = values - jnp.mean(values, axis=-1, keepdims=True)
    spread = jnp.mean(centred * centred, axis=-1, keepdims=True)
    return centred, lax.rsqrt(spread + norm_eps)


def norm_rows(x_ref, gain, shift, out_ref):
    def body(rows):
        centred, inverse = centre(x_ref[rows, :])
        out_ref[rows, :] = (centred * inverse * gain + shift).astype(BF16)

    each_chunk(body)


def norm_pullback(x_ref, gain, grad_ref, total_ref, out_ref, sums_ref):
    sums_ref[...] = jnp.zeros_like(sums_ref)

    def body(rows):
        centred, inverse = centre(x_ref[rows, :])
        unit = centred * inverse
        grad = grad_ref[rows, :]
        scaled = grad * gain
        first = jnp.mean(scaled, axis=-1, keepdims=True)
        second = jnp.mean(scaled * unit, axis=-1, keepdims=True)
        out_ref[rows, :] = total_ref[rows, :] + inverse * (scaled - first - unit * second)
        sums_ref[0:1, :] += jnp.sum(grad * unit, axis=0, keepdims=True)
        sums_ref[1:2, :] += jnp.sum(grad, axis=0, keepdims=True)

    each_chunk(body)


def weight_parts(w_ref, model):
    side = jnp.transpose(w_ref[:, 4 * model :].astype(F32))
    return [side[EXPERTS + i : EXPERTS + i + 1, :] for i in range(4)]


def attention_rows(x_ref, w_ref, gain, shift, x1_ref, proj_ref, log_ref, att_ref, normed_ref):
    model = x_ref.shape[1]
    norm_rows(x_ref, gain, shift, normed_ref)
    for part in range(3):
        columns = slice(part * model, (part + 1) * model)
        proj_ref[:, columns] = dot(normed_ref[...], w_ref[:, columns]).astype(BF16)
    att_ref[...] = jnp.zeros_like(att_ref)
    log_ref[...] = jnp.zeros_like(log_ref)
    low = lax.broadcasted_iota(jnp.int32, (SEQ_PAD, LANES), 1) < HEAD_DIM
    inside = lax.broadcasted_iota(jnp.int32, (SEQ_PAD, SEQ_PAD), 1) < SEQ
    lane = lax.broadcasted_iota(jnp.int32, (SEQ_PAD, LANES), 1)

    def image(i, carry):
        rows = rows_of(i, SEQ_PAD)
        logs = jnp.zeros((SEQ_PAD, LANES), F32)
        for pair in range(HEADS // 2):
            at = pair * LANES
            queries = proj_ref[rows, at : at + LANES]
            keys = proj_ref[rows, model + at : model + at + LANES]
            values = proj_ref[rows, 2 * model + at : 2 * model + at + LANES]
            results = []
            for side in range(2):
                mine = low if side == 0 else jnp.logical_not(low)
                masked = jnp.where(mine, queries, jnp.zeros_like(queries))
                scores = dot_nt(masked, keys) * HEAD_DIM ** (-0.5)
                scores = jnp.where(inside, scores, -1e30)
                highest = jnp.max(scores, axis=-1, keepdims=True)
                exponent = jnp.exp(scores - highest)
                summed = jnp.sum(exponent, axis=-1, keepdims=True)
                weights = (exponent / summed).astype(BF16)
                logs = jnp.where(lane == 2 * pair + side, highest + jnp.log(summed), logs)
                results.append(dot(weights, values))
            att_ref[rows, at : at + LANES] = jnp.where(low, results[0], results[1]).astype(BF16)
        log_ref[rows, :] = logs
        return carry

    lax.fori_loop(0, SLOTS, image, 0)
    x1_ref[...] = x_ref[...] + dot(att_ref[...], w_ref[:, 3 * model : 4 * model])


def route_rows(picks, slots_ref, turned_ref):
    lane = lax.broadcasted_iota(jnp.int32, (ROWS, LANES), 1)
    firsts, seconds = picks[:, 0:1], picks[:, 1:2]
    place_first, place_second = picks[:, 2:3], picks[:, 3:4]
    match_first, match_second = lane == firsts, lane == seconds
    either = jnp.where(match_first | match_second, 1.0, 0.0).astype(BF16)
    down = lax.broadcasted_iota(jnp.int32, (ROWS, ROWS), 0)
    across = lax.broadcasted_iota(jnp.int32, (ROWS, ROWS), 1)
    before = dot(jnp.where(across < down, 1.0, 0.0).astype(BF16), either)
    rank_first = jnp.sum(jnp.where(match_first, before, 0.0), axis=-1, keepdims=True)
    rank_second = jnp.sum(jnp.where(match_second, before, 0.0), axis=-1, keepdims=True)
    slot_first = jnp.where(place_first < 0, -1.0, place_first.astype(F32) * CAP_PAD + rank_first)
    slot_second = jnp.where(place_second < 0, -1.0, place_second.astype(F32) * CAP_PAD + rank_second)
    both = jnp.where(lane == 0, slot_first, jnp.where(lane == 1, slot_second, -1.0))
    slots_ref[...] = both.astype(jnp.int32)
    turned_ref[...] = jnp.transpose(both)[0:8, :].astype(jnp.int32)


def gate_rows(normed_ref, router_ref, picks, chances_ref, gates_ref):
    lane = lax.broadcasted_iota(jnp.int32, (ROWS, LANES), 1)
    logits = dot(normed_ref[...], router_ref[...])
    logits = jnp.where(lane < EXPERTS, logits, -1e30)
    exponent = jnp.exp(logits - jnp.max(logits, axis=-1, keepdims=True))
    chances = exponent / jnp.sum(exponent, axis=-1, keepdims=True)
    if chances_ref is not None:
        chances_ref[...] = chances
    gate_first = jnp.sum(jnp.where(lane == picks[:, 0:1], chances, 0.0), axis=-1, keepdims=True)
    gate_second = jnp.sum(jnp.where(lane == picks[:, 1:2], chances, 0.0), axis=-1, keepdims=True)
    gates_ref[...] = jnp.where(lane == 0, gate_first, jnp.where(lane == 1, gate_second, 0.0))


PLACES = EXPERTS // 2
GROUP = 4
BLOCK = GROUP * CAP_PAD
HALF = PLACES * CAP_PAD


def pick_block(turned_ref, group):
    slot = lax.broadcasted_iota(jnp.int32, (BLOCK, ROWS), 0) + group * BLOCK
    return slot == turned_ref[0:1, :], slot == turned_ref[1:2, :]


def as_weights(mask):
    return jnp.where(mask, 1.0, 0.0).astype(BF16)


def dispatch_block(turned_ref, rows_ref, group):
    first, second = pick_block(turned_ref, group)
    return dot(as_weights(first | second), rows_ref[...]).astype(BF16)


def dispatch_pair_block(turned_ref, pairs_ref, group):
    first, second = pick_block(turned_ref, group)
    both = jnp.concatenate([as_weights(first), as_weights(second)], axis=1)
    return dot(both, pairs_ref[...]).astype(BF16)


def ready_dispatch(turned_ref, ready_ref, pairs):
    def step(run, carry):
        first, second = pick_block(turned_ref, run)
        rows = rows_of(run, BLOCK)
        if pairs:
            ready_ref[rows, :ROWS] = as_weights(first)
            ready_ref[rows, ROWS:] = as_weights(second)
        else:
            ready_ref[rows, :ROWS] = as_weights(first | second)
        return carry

    lax.fori_loop(0, PLACES // GROUP, step, 0)


def ready_collect(slots_ref, ready_ref, pairs):
    def body(rows):
        slot = lax.broadcasted_iota(jnp.int32, (CHUNK, HALF), 1)
        slots = slots_ref[rows, :]
        first, second = slot == slots[:, 0:1], slot == slots[:, 1:2]
        if pairs:
            ready_ref[rows, :] = as_weights(first)
            ready_ref[later_rows(rows), :] = as_weights(second)
        else:
            ready_ref[rows, :] = as_weights(first | second)

    each_chunk(body)


def collect_ready(ready_ref, found_ref, side, total_ref):
    def step(run, carry):
        rows = rows_of(run, BLOCK)
        total_ref[rows, :] = dot(ready_ref[rows, :], found_ref[side].reshape(HALF, found_ref.shape[-1]))
        return carry

    lax.fori_loop(0, total_ref.shape[0] // BLOCK, step, 0)


def rows_at(ref, lead, group):
    block = ref[(*lead, pl.ds(group * GROUP, GROUP))]
    return block.reshape(BLOCK, block.shape[-1])


def collect_pairs(slots_ref, found_ref, side, total_ref):
    total_ref[...] = jnp.zeros_like(total_ref)

    def step(group, carry):
        slot = lax.broadcasted_iota(jnp.int32, (ROWS, BLOCK), 1) + group * BLOCK
        rows = rows_at(found_ref, (side,), group)
        for which in range(TOP):
            part = dot(as_weights(slot == slots_ref[:, which : which + 1]), rows)
            total_ref[which * ROWS : (which + 1) * ROWS, :] += part
        return carry

    lax.fori_loop(0, PLACES // GROUP, step, 0)


def collect_sums(slots_ref, found_ref, side, total_ref):
    total_ref[...] = jnp.zeros_like(total_ref)

    def step(group, carry):
        slot = lax.broadcasted_iota(jnp.int32, (ROWS, BLOCK), 1) + group * BLOCK
        chosen = (slot == slots_ref[:, 0:1]) | (slot == slots_ref[:, 1:2])
        total_ref[...] += dot(as_weights(chosen), rows_at(found_ref, (side,), group))
        return carry

    lax.fori_loop(0, PLACES // GROUP, step, 0)


def later_rows(rows):
    return pl.ds(pl.multiple_of(rows.start + ROWS, CHUNK), CHUNK)


def gated_sums(gates_ref, total_ref, routed_ref, side, out_ref):
    def body(rows):
        later = later_rows(rows)
        first, second = total_ref[rows, :], total_ref[later, :]
        gates = gates_ref[side, rows, :]
        out_ref[rows, :] = (gates[:, 0:1] * first + gates[:, 1:2] * second).astype(out_ref.dtype)
        routed_ref[side, rows, :] = first.astype(BF16)
        routed_ref[side, later, :] = second.astype(BF16)

    each_chunk(body)


def gate_grads(grad_ref, gates_ref, routed_ref, side, pairs_ref, grad_gates_ref):
    lane = lax.broadcasted_iota(jnp.int32, (LANES, LANES), 1)

    def body(i, carry):
        rows = rows_of(i, LANES)
        later = pl.ds(pl.multiple_of(i * LANES + ROWS, LANES), LANES)
        grad = grad_ref[rows, :].astype(F32)
        gates = gates_ref[side, rows, :]
        pairs_ref[rows, :] = (gates[:, 0:1] * grad).astype(BF16)
        pairs_ref[later, :] = (gates[:, 1:2] * grad).astype(BF16)
        first = jnp.sum(grad * routed_ref[side, rows, :].astype(F32), axis=-1, keepdims=True)
        second = jnp.sum(grad * routed_ref[side, later, :].astype(F32), axis=-1, keepdims=True)
        both = jnp.where(lane == 0, first, jnp.where(lane == 1, second, 0.0))
        grad_gates_ref[:, rows] = jnp.transpose(both)[0:8, :]
        return carry

    lax.fori_loop(0, ROWS // LANES, body, 0)


def attention_pullback(grad_ref, w_ref, proj_ref, log_ref, att_ref, normed_ref, small_ref, gproj_ref, gatt_ref, back_ref, gnormed_ref):
    model = grad_ref.shape[1]

    def body(rows):
        back_ref[rows, :] = grad_ref[rows, :].astype(BF16)

    each_chunk(body)
    small_ref[:, 3 * model : 4 * model] = dot_tn(att_ref[...], back_ref[...])
    gatt_ref[...] = dot_nt(back_ref[...], w_ref[:, 3 * model : 4 * model]).astype(BF16)
    gproj_ref[SLOTS * SEQ_PAD :, :] = jnp.zeros((ROWS - SLOTS * SEQ_PAD, 3 * model), BF16)
    low = lax.broadcasted_iota(jnp.int32, (SEQ_PAD, LANES), 1) < HEAD_DIM
    inside = lax.broadcasted_iota(jnp.int32, (SEQ_PAD, SEQ_PAD), 1) < SEQ
    scaling = HEAD_DIM ** (-0.5)

    def image(i, carry):
        rows = rows_of(i, SEQ_PAD)
        for pair in range(HEADS // 2):
            at = pair * LANES
            queries = proj_ref[rows, at : at + LANES]
            keys = proj_ref[rows, model + at : model + at + LANES]
            values = proj_ref[rows, 2 * model + at : 2 * model + at + LANES]
            grad_heads = gatt_ref[rows, at : at + LANES]
            parts = []
            for side in range(2):
                mine = low if side == 0 else jnp.logical_not(low)
                zero = jnp.zeros_like(queries)
                head = 2 * pair + side
                scores = dot_nt(jnp.where(mine, queries, zero), keys) * scaling
                chances = jnp.where(inside, jnp.exp(scores - log_ref[rows, head : head + 1]), 0.0)
                grad_weights = dot_nt(jnp.where(mine, grad_heads, zero), values)
                centre_term = jnp.sum(grad_weights * chances, axis=-1, keepdims=True)
                grad_scores = (chances * (grad_weights - centre_term)).astype(BF16)
                parts.append(
                    (
                        dot(grad_scores, keys) * scaling,
                        dot_tn(grad_scores, queries) * scaling,
                        dot_tn(chances.astype(BF16), grad_heads),
                    )
                )
            for which in range(3):
                to = which * model + at
                gproj_ref[rows, to : to + LANES] = jnp.where(low, parts[0][which], parts[1][which]).astype(BF16)
        return carry

    lax.fori_loop(0, SLOTS, image, 0)
    for part in range(3):
        columns = slice(part * model, (part + 1) * model)
        small_ref[:, columns] = dot_tn(normed_ref[...], gproj_ref[:, columns])
    gnormed_ref[...] = dot_nt(gproj_ref[...], w_ref[:, : 3 * model])


def router_pullback(grad_gates_ref, picks_ref, chances_ref, w_ref, normed_ref, gnormed_ref, router_ref):
    model = normed_ref.shape[1]
    lane = lax.broadcasted_iota(jnp.int32, (ROWS, LANES), 1)
    picks, chances = picks_ref[...], chances_ref[...]
    turned = jnp.concatenate([grad_gates_ref[...], jnp.zeros((LANES - 8, ROWS), F32)], axis=0)
    grads = jnp.transpose(turned)
    spread = jnp.where(lane == picks[:, 0:1], grads[:, 0:1], 0.0) + jnp.where(lane == picks[:, 1:2], grads[:, 1:2], 0.0)
    logits = chances * (spread - jnp.sum(spread * chances, axis=-1, keepdims=True))
    logits = logits.astype(BF16)
    router_ref[...] = dot_tn(normed_ref[...], logits)
    gnormed_ref[...] += dot_nt(logits, w_ref[:, 4 * model :])


MESH = pl.DeviceIdType.MESH


def position():
    group, shard = lax.axis_index("expert"), lax.axis_index("shard")
    low = shard % 2
    return group, shard, low, group * 2 + low


def place_id(step):
    _, shard, low, me = position()
    there = (me + step + PLACES) % PLACES
    return (there // 2, shard - low + there % 2)


def twin_id():
    group, shard, _, _ = position()
    return (group, (shard + 2) % SHARDS)


def meet():
    barrier = pltpu.get_barrier_semaphore()
    for k in range(1, PLACES):
        pl.semaphore_signal(barrier, inc=1, device_id=place_id(k), device_id_type=MESH)
    group, shard, low, _ = position()
    for k in range(2):
        there = (shard - low + SHARDS // 2 + k) % SHARDS
        pl.semaphore_signal(barrier, inc=1, device_id=(group, there), device_id_type=MESH)
    pl.semaphore_wait(barrier, PLACES + 1)


SENT = 200


def to_twin(src, dst, sems, at):
    return pltpu.make_async_remote_copy(
        src_ref=src, dst_ref=dst, send_sem=sems.at[0, at], recv_sem=sems.at[1, at], device_id=twin_id(), device_id_type=MESH
    )


class RowSwap:
    def __init__(self, src, dst, sems, at):
        self.dst = dst
        self.copies = []
        for image in range(SLOTS):
            rows = pl.ds(image * SEQ_PAD, SENT)
            self.copies.append(to_twin(src.at[rows], dst.at[rows], sems, at + image))

    @staticmethod
    def clear(dst):
        for image in range(SLOTS):
            stop = (image + 1) * SEQ_PAD
            start = stop - (SEQ_PAD - SENT)
            stop = ROWS if image == SLOTS - 1 else stop
            dst[start:stop, :] = jnp.zeros((stop - start, dst.shape[1]), dst.dtype)

    def start(self):
        for copy in self.copies:
            copy.start()

    def wait_recv(self):
        for copy in self.copies:
            copy.wait_recv()

    def wait_send(self):
        for copy in self.copies:
            copy.wait_send()


def shard_rows(ref, shard):
    rows = ref.shape[0] // SHARDS
    return pl.ds(pl.multiple_of(shard * rows, rows), rows)


def share_blocks(source, target, sems, own_source=None):
    group, shard, _, _ = position()
    copies = [pltpu.make_async_copy(source(shard) if own_source is None else own_source, target(shard), sems.at[1, 0])]
    for k in (2, 1, 3):
        to = (shard + k) % SHARDS
        copies.append(
            pltpu.make_async_remote_copy(
                src_ref=source(to),
                dst_ref=target(shard),
                send_sem=sems.at[0, k],
                recv_sem=sems.at[1, k],
                device_id=(group, to),
                device_id_type=MESH,
            )
        )
    return copies


def stay_copy(src, dst, sems, lane, side):
    return pltpu.make_async_copy(src.at[side, 0], dst.at[side, 0], sems.at[lane, 1, side, 0])


def block_copy(src, dst, sems, lane, side, k, sign):
    return pltpu.make_async_remote_copy(
        src_ref=src.at[side, k],
        dst_ref=dst.at[side, k],
        send_sem=sems.at[lane, 0, side, k],
        recv_sem=sems.at[lane, 1, side, k],
        device_id=place_id(sign * k),
        device_id_type=MESH,
    )


def start_blocks(src, dst, sems, lane, side, run, count, sign):
    first = run * count

    @pl.when(run == 0)
    def _():
        stay_copy(src, dst, sems, lane, side).start()

    @pl.when(run != 0)
    def _():
        block_copy(src, dst, sems, lane, side, first, sign).start()

    for j in range(1, count):
        block_copy(src, dst, sems, lane, side, first + j, sign).start()


def await_blocks(src, dst, sems, lane, side, run, count, sign):
    first = run * count

    @pl.when(run == 0)
    def _():
        stay_copy(src, dst, sems, lane, side).wait()

    @pl.when(run != 0)
    def _():
        block_copy(src, dst, sems, lane, side, first, sign).wait_recv()

    for j in range(1, count):
        block_copy(src, dst, sems, lane, side, first + j, sign).wait_recv()


def await_sent(src, dst, sems, lane, side, sign):
    def step(k, carry):
        block_copy(src, dst, sems, lane, side, k, sign).wait_send()
        return carry

    lax.fori_loop(1, PLACES, step, 0)


def spread(make_block, src, dst, sems, side):
    runs = PLACES // GROUP

    def step(run, carry):
        src[side, pl.ds(run * GROUP, GROUP)] = make_block(run).reshape(GROUP, CAP_PAD, src.shape[-1])

        @pl.when(run > 0)
        def _():
            start_blocks(src, dst, sems, 0, side, run - 1, GROUP, 1)

        return carry

    lax.fori_loop(0, runs, step, 0)
    start_blocks(src, dst, sems, 0, side, runs - 1, GROUP, 1)


def all_back(src, dst, sems, side):
    for run in range(TILES):
        await_blocks(src, dst, sems, 1, side, run, TILE_PLACES, -1)


def pick_lanes(rows_ref, layer):
    _, shard, _, me = position()
    turned = jnp.transpose(jnp.concatenate([rows_ref[...].astype(F32), jnp.zeros((LANES - 8, ROWS), F32)], axis=0))
    lane = lax.broadcasted_iota(jnp.int32, (ROWS, LANES), 1)
    lanes = jnp.full((ROWS, LANES), -1, jnp.int32)
    for which in range(TOP):
        at = TOP * layer + which
        expert = turned[:, at : at + 1].astype(jnp.int32)
        side = expert & (SHARDS - 1)
        place = ((expert >> 2) * 2 + (side & 1) + (PLACES - me)) & (PLACES - 1)
        place = jnp.where((expert >= 0) & ((side >> 1) == shard // 2), place, -1)
        lanes = jnp.where(lane == which, expert, jnp.where(lane == TOP + which, place, lanes))
    return lanes


TILE_PLACES = 8
TILE = TILE_PLACES * CAP_PAD
TILES = PLACES // TILE_PLACES
WIDE = 512
ROOT = 0.7978845608028654
CUBE = 0.044715


class Refs:
    def __init__(self, names, refs):
        self.__dict__.update(zip(names, refs))


def layer_kernel(layer, more, names, kept_names, *refs):
    r = Refs(names, refs)
    h = Refs(kept_names, refs[len(names) :])
    _, shard, _, _ = position()
    opens = layer == 0
    saved = []

    def save(ref, kept, at):
        copy = pltpu.make_async_copy(ref, kept, r.keep_sems.at[at])
        copy.start()
        saved.append(copy)

    model = r.x1_ref.shape[1]
    RowSwap.clear(r.twin_rows)
    RowSwap.clear(r.other)
    r.normed_ref[SLOTS * SEQ_PAD :, :] = jnp.zeros((ROWS - SLOTS * SEQ_PAD, model), BF16)
    if more:
        stage = pltpu.make_async_copy(r.ins_hbm.at[layer + 1, shard], r.stage_ref, r.load_sems.at[1])
        stage.start()
    out_copies = share_blocks(
        lambda to: r.outs_hbm.at[layer, to], lambda own: r.out_ref.at[shard_rows(r.out_ref, own)], r.out_sems
    )
    meet()
    if opens:
        gather = Gather(r.piece_ref, r.w_ref, r.open_far, r.open_flat, r.open_core, r.open_own)
        gather.start()
        picks_copy = to_twin(r.picks_ref, r.theirs_ref, r.pick_sems, 0)
        picks_copy.start()
        in_copies = share_blocks(
            lambda to: r.ins_hbm.at[layer, to], lambda own: r.in_ref.at[shard_rows(r.in_ref, own)], r.in_sems
        )
        for copy in in_copies:
            copy.start()
        states = r.states_ref[...].astype(F32)
        r.x_ref[...] = jnp.zeros_like(r.x_ref)
        for image in range(SLOTS):
            r.x_ref[image * SEQ_PAD : image * SEQ_PAD + SEQ, :] = states[image * SEQ : (image + 1) * SEQ]
        gather.spread()
        gather.pair()
        gather.finish()
        picks_copy.wait()
        r.marks_ref[...] = jnp.sum(r.w_ref[:, 4 * model :].astype(F32), axis=0, keepdims=True)
    else:
        load = pltpu.make_async_copy(r.in_hbm, r.in_ref, r.load_sems.at[0])
        load.start()
        for copy in out_copies[:2]:
            copy.start()

        def body(rows):
            r.x_ref[rows, :] = r.below_ref[rows, :] + r.step_ref[rows, :]

        each_chunk(body)
    gain1, gain2, shift1, shift2 = weight_parts(r.w_ref, model)
    attention_rows(r.x_ref, r.w_ref, gain1, shift1, r.x1_ref, r.proj_ref, r.log_ref, r.att_ref, r.normed_ref)
    norm_rows(r.x1_ref, gain2, shift2, r.normed_ref)
    row_swap = RowSwap(r.normed_ref, r.twin_rows, r.twin_sems, 0)
    row_swap.start()
    for at, (ref, kept) in enumerate(
        ((r.x_ref, h.x_ref), (r.x1_ref, h.x1_ref), (r.proj_ref, h.proj_ref), (r.log_ref, h.log_ref), (r.att_ref, h.att_ref))
    ):
        save(ref, kept, at)
    if more:
        gather = Gather(r.next_piece_ref, r.next_w_ref, r.next_far, r.next_flat, r.next_core, r.next_own)
        gather.start()
        stage.wait()
        next_copies = share_blocks(
            lambda to: r.ins_hbm.at[layer + 1, to],
            lambda own: r.next_hbm.at[shard_rows(r.next_hbm, own)],
            r.next_in_sems,
            r.stage_ref,
        )
    router_ref = r.w_ref.at[:, 4 * model :]
    r.lanes_ref[...] = pick_lanes(r.picks_ref, layer)
    route_rows(r.lanes_ref[...], r.slots_ref.at[0], r.turned_ref.at[0])
    spread(lambda run: dispatch_block(r.turned_ref.at[0], r.normed_ref, run), r.leaving, r.arrived_ref, r.sems, 0)
    for copy in out_copies if opens else out_copies[2:]:
        copy.start()
    gate_rows(r.normed_ref, router_ref, r.lanes_ref[...], r.chances_ref, r.gates_ref.at[0])
    r.twin_lanes[...] = pick_lanes(r.theirs_ref, layer)
    route_rows(r.twin_lanes[...], r.slots_ref.at[1], r.turned_ref.at[1])
    ready_dispatch(r.turned_ref.at[1], r.ready_ref, False)
    row_swap.wait_recv()

    def twin_block(run):
        return dot(r.ready_ref[rows_of(run, BLOCK), :ROWS], r.twin_rows[...]).astype(BF16)

    spread(twin_block, r.leaving, r.arrived_ref, r.sems, 1)
    if more:
        gather.spread()
        for copy in next_copies:
            copy.start()
    gate_rows(r.twin_rows, router_ref, r.twin_lanes[...], None, r.gates_ref.at[1])

    def saves(side, tile):
        to = pl.ds((side * TILES + tile) * TILE, TILE)
        return [
            pltpu.make_async_copy(r.act_ref.at[tile], r.act_hbm.at[to, :], r.save_sems.at[0, tile]),
            pltpu.make_async_copy(r.slope_ref.at[tile], r.slope_hbm.at[to, :], r.save_sems.at[1, tile]),
        ]

    def inner(side, tile):
        await_blocks(r.leaving, r.arrived_ref, r.sems, 0, side, tile, TILE_PLACES, 1)
        rows = r.arrived_ref[side, pl.ds(tile * TILE_PLACES, TILE_PLACES)].reshape(TILE, model)

        def chunk(i, carry):
            columns = rows_of(i, WIDE)
            pre = dot(rows, r.in_ref[:, columns])
            square = pre * pre
            bend = jnp.tanh(pre * (ROOT + ROOT * CUBE * square))
            half = 0.5 + 0.5 * bend
            act = (pre * half).astype(BF16)
            slope = half + (0.5 * pre) * (1.0 - bend * bend) * (ROOT + 3.0 * ROOT * CUBE * square)
            r.act_ref[tile, :, columns] = act
            r.slope_ref[tile, :, columns] = slope.astype(BF16)
            return carry

        lax.fori_loop(0, r.in_ref.shape[1] // WIDE, chunk, 0)

    def outer(side, tile):
        result = dot(r.act_ref[tile], r.out_ref[...]).astype(BF16)
        r.made[side, pl.ds(tile * TILE_PLACES, TILE_PLACES)] = result.reshape(TILE_PLACES, CAP_PAD, model)
        for save in saves(side, tile):
            save.start()
        start_blocks(r.made, r.returned, r.sems, 1, side, tile, TILE_PLACES, -1)

    def each_tile(body):
        def step(tile, carry):
            body(tile)
            return carry

        lax.fori_loop(0, TILES, step, 0)

    if opens:
        for copy in in_copies:
            copy.wait()
        keep_in = pltpu.make_async_copy(r.in_ref, r.kept_in_hbm, r.load_sems.at[0])
        keep_in.start()
    else:
        load.wait()
    each_tile(lambda tile: inner(1, tile))
    for copy in out_copies:
        copy.wait()
    keep = pltpu.make_async_copy(r.out_ref, r.kept_hbm, r.load_sems.at[2])
    keep.start()
    each_tile(lambda tile: outer(1, tile))

    def own_tile(tile):
        for copy in saves(1, tile):
            copy.wait()
        inner(0, tile)
        outer(0, tile)

    own_tile(0)
    ready_collect(r.slots_ref.at[1], r.ready_ref, True)
    all_back(r.made, r.returned, r.sems, 1)
    collect_ready(r.ready_ref, r.returned, 1, r.total)
    gated_sums(r.gates_ref, r.total, r.routed_ref, 1, r.twin_sum)
    sum_swap = RowSwap(r.twin_sum, r.other, r.twin_sems, SLOTS)
    sum_swap.start()
    own_tile(1)
    save(r.arrived_ref, h.arrived_ref, 5)
    if more:
        gather.pair()
    all_back(r.made, r.returned, r.sems, 0)
    collect_pairs(r.slots_ref.at[0], r.returned, 0, r.total)
    gated_sums(r.gates_ref, r.total, r.routed_ref, 0, r.delta_ref)

    def finish_saves(tile):
        for copy in saves(0, tile):
            copy.wait()

    each_tile(finish_saves)
    for side in range(2):
        await_sent(r.leaving, r.arrived_ref, r.sems, 0, side, 1)
        await_sent(r.made, r.returned, r.sems, 1, side, -1)
    row_swap.wait_send()
    keep.wait()
    for copy in saved:
        copy.wait()
    if opens:
        keep_in.wait()
    if more:
        for copy in next_copies:
            copy.wait()
        gather.finish()
    sum_swap.wait_recv()
    sum_swap.wait_send()

    if not more:
        counted = r.marks_ref[:, EXPERTS + 4 : EXPERTS + 5] * float(SEQ)

    def add_other(rows):
        step = r.delta_ref[rows, :] + r.other[rows, :].astype(F32)
        if more:
            r.delta_ref[rows, :] = step
        else:
            values = r.x1_ref[rows, :] + step
            r.final_ref[rows, :] = values.astype(BF16)
            grad = (values - r.teacher_ref[rows, :].astype(F32)) * (r.twice_ref[rows, :] / counted)
            r.grad_ref[rows, :] = grad
            r.sent_ref[rows, :] = grad.astype(BF16)

    each_chunk(add_other)


def in_vmem(count):
    return [pl.BlockSpec(memory_space=pltpu.VMEM)] * count


def anywhere(count):
    return [pl.BlockSpec(memory_space=pl.ANY)] * count


def blocks_of(model):
    return pltpu.VMEM((2, PLACES, CAP_PAD, model), BF16)


def run_layer(layer, arrays, in_hbm, expert_out, expert_in):
    layers, _, part, hidden = expert_in.shape
    model = part * SHARDS
    opens, more = layer == 0, layer + 1 < layers
    width = 4 * model + LANES
    hbm_inputs = dict(outs_hbm=expert_out)
    if not opens:
        hbm_inputs.update(in_hbm=in_hbm)
    if opens or more:
        hbm_inputs.update(ins_hbm=expert_in)
    rows_of_kind = lambda kind, columns=model: shape((ROWS, columns), kind)
    kept = dict(
        x_ref=rows_of_kind(F32),
        x1_ref=rows_of_kind(F32),
        proj_ref=rows_of_kind(BF16, 3 * model),
        log_ref=rows_of_kind(F32, LANES),
        att_ref=rows_of_kind(BF16),
        arrived_ref=shape((2, PLACES, CAP_PAD, model), BF16),
    )
    outputs = {}
    if opens:
        outputs.update(w_ref=shape((model, width), BF16), theirs_ref=shape((8, ROWS), jnp.int32))
        outputs.update(marks_ref=shape((1, LANES), F32))
    if more:
        outputs.update(next_w_ref=shape((model, width), BF16), delta_ref=rows_of_kind(F32))
    else:
        outputs.update(final_ref=rows_of_kind(BF16), grad_ref=rows_of_kind(F32), sent_ref=rows_of_kind(BF16))
    outputs.update(
        lanes_ref=rows_of_kind(jnp.int32, LANES),
        slots_ref=shape((2, ROWS, LANES), jnp.int32),
        turned_ref=shape((2, 8, ROWS), jnp.int32),
        chances_ref=rows_of_kind(F32, LANES),
        gates_ref=shape((2, ROWS, LANES), F32),
        routed_ref=shape((2, TOP * ROWS, model), BF16),
    )
    hbm_outputs = dict(
        act_hbm=shape((2 * HALF, hidden), BF16),
        slope_hbm=shape((2 * HALF, hidden), BF16),
        kept_hbm=shape((hidden, model), BF16),
    )
    if opens:
        hbm_outputs.update(kept_in_hbm=shape((model, hidden), BF16))
    if more:
        hbm_outputs.update(next_hbm=shape((model, hidden), BF16))
    scratch = dict(
        normed_ref=pltpu.VMEM((ROWS, model), BF16),
        twin_rows=pltpu.VMEM((ROWS, model), BF16),
        twin_lanes=pltpu.VMEM((ROWS, LANES), jnp.int32),
        leaving=blocks_of(model),
        made=blocks_of(model),
        returned=blocks_of(model),
        total=pltpu.VMEM((TOP * ROWS, model), F32),
        twin_sum=pltpu.VMEM((ROWS, model), BF16),
        other=pltpu.VMEM((ROWS, model), BF16),
        act_ref=pltpu.VMEM((2, TILE, hidden), BF16),
        slope_ref=pltpu.VMEM((2, TILE, hidden), BF16),
        in_ref=pltpu.VMEM((model, hidden), BF16),
        out_ref=pltpu.VMEM((hidden, model), BF16),
        sems=pltpu.SemaphoreType.DMA((2, 2, 2, PLACES)),
        twin_sems=pltpu.SemaphoreType.DMA((2, 2 * SLOTS)),
        load_sems=pltpu.SemaphoreType.DMA((3,)),
        save_sems=pltpu.SemaphoreType.DMA((2, 2)),
        out_sems=pltpu.SemaphoreType.DMA((2, SHARDS)),
        keep_sems=pltpu.SemaphoreType.DMA((len(kept),)),
        ready_ref=pltpu.VMEM((HALF, TOP * ROWS), BF16),
    )
    scratch.update({name: pltpu.VMEM(kind.shape, kind.dtype) for name, kind in kept.items()})
    far, flat, core, own = gather_sems()
    if opens:
        scratch.update(in_sems=pltpu.SemaphoreType.DMA((2, SHARDS)), pick_sems=pltpu.SemaphoreType.DMA((2, 1)))
        scratch.update(open_far=far, open_flat=flat, open_core=core, open_own=own)
    if more:
        scratch.update(stage_ref=pltpu.VMEM((part, hidden), BF16), next_in_sems=pltpu.SemaphoreType.DMA((2, SHARDS)))
        scratch.update(next_far=far, next_flat=flat, next_core=core, next_own=own)
    else:
        scratch.update(delta_ref=pltpu.VMEM((ROWS, model), F32))
    names = list(arrays) + list(hbm_inputs) + list(outputs) + list(hbm_outputs)
    split = len(names)

    def body(*refs):
        own, saved, rest = refs[:split], refs[split : split + len(kept)], refs[split + len(kept) :]
        layer_kernel(layer, more, names + list(scratch), list(kept), *own, *rest, *saved)

    results = pl.pallas_call(
        body,
        out_shape=list(outputs.values()) + list(hbm_outputs.values()) + list(kept.values()),
        in_specs=in_vmem(len(arrays)) + anywhere(len(hbm_inputs)),
        out_specs=in_vmem(len(outputs)) + anywhere(len(hbm_outputs) + len(kept)),
        scratch_shapes=list(scratch.values()),
        compiler_params=pltpu.CompilerParams(vmem_limit_bytes=LIMIT, collective_id=1 + layer, has_side_effects=True),
        name="layer",
    )(*arrays.values(), *hbm_inputs.values())
    return dict(zip(list(outputs) + list(hbm_outputs) + list(kept), results))


def unmix_kernel(
    carry, grad_ref, sent_ref, gates_ref, slots_ref, turned_ref, routed_hbm, arrived_hbm, act_hbm, slope_hbm, in_hbm, out_hbm, *refs,
):
    if carry:
        carried_hbm, *refs = refs
    sums_ref, grad_gates_ref, gin_hbm, gout_hbm, *refs = refs
    if carry:
        shared_hbm, *refs = refs
    twin_rows, leaving, came, made, returned, pairs, twin_sum, other, twin_gates, other_gates, *refs = refs
    pre_ref, slope_ref, act_ref, arrived_ref, in_ref, out_ref, *refs = refs
    routed_ref, ready_ref, gin_ref, gout_ref, *refs = refs
    sems, twin_sems, load_sems, slope_sems, act_sems, save_sems, *refs = refs
    if carry:
        stage_ref, share_sems = refs
    _, shard, _, _ = position()
    model, hidden = in_ref.shape
    RowSwap.clear(twin_rows)
    RowSwap.clear(other)
    if carry:
        stage = pltpu.make_async_copy(carried_hbm.at[shard], stage_ref, load_sems.at[3])
        stage.start()
    loads = [
        pltpu.make_async_copy(src, dst, load_sems.at[i])
        for i, (src, dst) in enumerate(((in_hbm, in_ref), (out_hbm, out_ref), (arrived_hbm, arrived_ref)))
    ]
    load_routed = pltpu.make_async_copy(routed_hbm, routed_ref, load_sems.at[4])
    load_routed.start()
    for load in loads:
        load.start()

    def slopes(side, tile):
        at = pl.ds((side * TILES + tile) * TILE, TILE)
        return pltpu.make_async_copy(slope_hbm.at[at, :], slope_ref.at[tile], slope_sems.at[tile])

    def acts(chunk):
        slot = chunk % 2
        return pltpu.make_async_copy(act_hbm.at[:, rows_of(chunk, WIDE)], act_ref.at[slot], act_sems.at[slot])

    for tile in range(TILES):
        slopes(0, tile).start()
    for chunk in range(2):
        acts(chunk).start()
    meet()
    row_swap = RowSwap(sent_ref, twin_rows, twin_sems, 0)
    row_swap.start()
    load_routed.wait()
    gate_grads(grad_ref, gates_ref, routed_ref, 0, pairs, grad_gates_ref)
    spread(lambda run: dispatch_pair_block(turned_ref.at[0], pairs, run), leaving, came, sems, 0)
    ready_dispatch(turned_ref.at[1], ready_ref, True)
    row_swap.wait_recv()
    gate_grads(twin_rows, gates_ref, routed_ref, 1, pairs, twin_gates)
    gates_copy = to_twin(twin_gates, other_gates, twin_sems, 2 * SLOTS)
    spread(lambda run: dot(ready_ref[rows_of(run, BLOCK), :], pairs[...]).astype(BF16), leaving, came, sems, 1)
    gates_copy.start()
    share_copies = []
    if carry:
        stage.wait()
        share_copies = share_blocks(lambda to: carried_hbm.at[to], lambda own: shared_hbm.at[own], share_sems, stage_ref)
        for copy in share_copies[:2]:
            copy.start()
    for load in loads:
        load.wait()

    def back_tile(side, tile):
        await_blocks(leaving, came, sems, 0, side, tile, TILE_PLACES, 1)
        slopes(side, tile).wait()
        rows = came[side, pl.ds(tile * TILE_PLACES, TILE_PLACES)].reshape(TILE, model)
        at = rows_of(side * TILES + tile, TILE)

        def chunk(i, carry):
            columns = rows_of(i, WIDE)
            grad_act = dot_nt(rows, out_ref[columns, :])
            pre_ref[at, columns] = (slope_ref[tile, :, columns].astype(F32) * grad_act).astype(BF16)
            return carry

        lax.fori_loop(0, hidden // WIDE, chunk, 0)
        if side == 0:
            slopes(1, tile).start()
        result = dot_nt(pre_ref[at, :], in_ref[...]).astype(BF16)
        made[side, pl.ds(tile * TILE_PLACES, TILE_PLACES)] = result.reshape(TILE_PLACES, CAP_PAD, model)
        start_blocks(made, returned, sems, 1, side, tile, TILE_PLACES, -1)

    for side in range(2):

        def step(tile, carry, side=side):
            back_tile(side, tile)
            return carry

        lax.fori_loop(0, TILES, step, 0)
    for copy in share_copies[2:]:
        copy.start()
    ready_collect(slots_ref.at[1], ready_ref, False)
    all_back(made, returned, sems, 1)
    collect_ready(ready_ref, returned, 1, sums_ref)
    twin_sum[...] = sums_ref[...].astype(BF16)
    sum_swap = RowSwap(twin_sum, other, twin_sems, SLOTS)
    sum_swap.start()
    chunks = hidden // WIDE

    def weigh(chunk, carry):
        columns = rows_of(chunk, WIDE)
        gin_ref[:, columns] = dot_tn(arrived_ref[...].reshape(2 * HALF, model), pre_ref[:, columns]).astype(BF16)
        acts(chunk).wait()
        gout_ref[columns, :] = dot_tn(act_ref[chunk % 2], came[...].reshape(2 * HALF, model)).astype(BF16)

        @pl.when(chunk + 2 < chunks)
        def _():
            acts(chunk + 2).start()

        return carry

    lax.fori_loop(0, chunks, weigh, 0)
    saved = [
        pltpu.make_async_copy(src, dst, save_sems.at[i])
        for i, (src, dst) in enumerate(((gin_ref, gin_hbm), (gout_ref, gout_hbm)))
    ]
    for copy in saved:
        copy.start()
    all_back(made, returned, sems, 0)
    collect_sums(slots_ref.at[0], returned, 0, sums_ref)
    for side in range(2):
        await_sent(leaving, came, sems, 0, side, 1)
        await_sent(made, returned, sems, 1, side, -1)
    row_swap.wait_send()
    gates_copy.wait()
    grad_gates_ref[...] += other_gates[...]
    for copy in saved:
        copy.wait()
    for copy in share_copies:
        copy.wait()
    sum_swap.wait_recv()
    sum_swap.wait_send()

    def body(rows):
        sums_ref[rows, :] += other[rows, :].astype(F32)

    each_chunk(body)


def run_unmix(grad, sent, state, weight_in, carried=()):
    model, hidden = weight_in.shape
    carry = len(carried) > 0
    outs = [shape((ROWS, model), F32), shape((8, ROWS), F32), shape((model, hidden), BF16), shape((hidden, model), BF16)]
    extra = []
    if carry:
        outs += [shape(carried[0].shape, BF16)]
        extra = [
            pltpu.VMEM(carried[0].shape[1:], BF16),
            pltpu.SemaphoreType.DMA((2, SHARDS)),
        ]
    inputs = [grad, sent, state.gates_ref, state.slots_ref, state.turned_ref]
    inputs += [state.routed_ref, state.arrived_ref, state.act_hbm, state.slope_hbm, weight_in, state.kept_hbm, *carried]
    return pl.pallas_call(
        functools.partial(unmix_kernel, carry),
        out_shape=outs,
        in_specs=in_vmem(5) + anywhere(len(inputs) - 5),
        out_specs=in_vmem(2) + anywhere(len(outs) - 2),
        scratch_shapes=[
            pltpu.VMEM((ROWS, model), BF16),
            blocks_of(model),
            blocks_of(model),
            blocks_of(model),
            blocks_of(model),
            pltpu.VMEM((TOP * ROWS, model), BF16),
            pltpu.VMEM((ROWS, model), BF16),
            pltpu.VMEM((ROWS, model), BF16),
            pltpu.VMEM((8, ROWS), F32),
            pltpu.VMEM((8, ROWS), F32),
            pltpu.VMEM((2 * HALF, hidden), BF16),
            pltpu.VMEM((2, TILE, hidden), BF16),
            pltpu.VMEM((2, 2 * HALF, WIDE), BF16),
            blocks_of(model),
            pltpu.VMEM((model, hidden), BF16),
            pltpu.VMEM((hidden, model), BF16),
            pltpu.VMEM((2, TOP * ROWS, model), BF16),
            pltpu.VMEM((HALF, TOP * ROWS), BF16),
            pltpu.VMEM((model, hidden), BF16),
            pltpu.VMEM((hidden, model), BF16),
            pltpu.SemaphoreType.DMA((2, 2, 2, PLACES)),
            pltpu.SemaphoreType.DMA((2, 2 * SLOTS + 1)),
            pltpu.SemaphoreType.DMA((5,)),
            pltpu.SemaphoreType.DMA((2,)),
            pltpu.SemaphoreType.DMA((2,)),
            pltpu.SemaphoreType.DMA((2,)),
        ]
        + extra,
        compiler_params=pltpu.CompilerParams(vmem_limit_bytes=LIMIT, collective_id=3 + int(carry), has_side_effects=True),
        name="unmix",
    )(*inputs)


def flips():
    group = lax.axis_index("expert")
    along = 2 - 4 * (group // 2 % 2)
    up = 4 - 8 * (group // 4)
    return [group + along, group + up, group + along + up]


def other_core():
    group = lax.axis_index("expert")
    return group + 1 - 2 * (group % 2)


def remote(src, dst, send_sem, recv_sem, device):
    return pltpu.make_async_remote_copy(
        src_ref=src, dst_ref=dst, send_sem=send_sem, recv_sem=recv_sem, device_id=device, device_id_type=MESH
    )


def meet_axes():
    group, shard = lax.axis_index("expert"), lax.axis_index("shard")
    barrier = pltpu.get_barrier_semaphore()
    devices = [(group, (shard + k) % SHARDS) for k in range(1, SHARDS)]
    devices += [(there, shard) for there in flips() + [other_core()]]
    for device in devices:
        pl.semaphore_signal(barrier, inc=1, device_id=device, device_id_type=MESH)
    pl.semaphore_wait(barrier, len(devices))


class Gather:
    def __init__(self, piece, full, far_sems, flat_sems, core_sems, own_sem):
        self.group, self.shard = lax.axis_index("expert"), lax.axis_index("shard")
        self.piece, self.full = piece, full
        self.far_sems, self.flat_sems, self.core_sems = far_sems, flat_sems, core_sems
        self.planes = [(self.shard + SHARDS - k) % SHARDS for k in range(SHARDS)]
        self.own = pltpu.make_async_copy(piece, self.rows(self.shard, self.group), own_sem)
        self.sent = []

    def rows(self, plane, there):
        size = self.piece.shape[0]
        span = self.full.shape[0] // SHARDS
        return self.full.at[pl.ds(pl.multiple_of(plane * span + there * size, size), size)]

    def go(self, copy):
        copy.start()
        self.sent.append(copy)

    def far(self, k):
        to = (self.group, (self.shard + k) % SHARDS)
        return remote(self.piece, self.rows(self.shard, self.group), self.far_sems.at[0, k], self.far_sems.at[1, k], to)

    def flat(self, at, p, k):
        return remote(at, at, self.flat_sems.at[0, p, k], self.flat_sems.at[1, p, k], (flips()[p], self.shard))

    def core(self, at, p, k):
        return remote(at, at, self.core_sems.at[0, p, k], self.core_sems.at[1, p, k], (other_core(), self.shard))

    def start(self):
        self.own.start()
        for k in (2, 1, 3):
            self.go(self.far(k))
        self.own.wait()

    def spread(self):
        for k in (0, 1, 3, 2):
            at = self.rows(self.planes[k], self.group)
            if k:
                self.far(k).wait_recv()
            for p in range(3):
                self.go(self.flat(at, p, k))
            self.go(self.core(at, 3, k))

    def pair(self):
        for k in (0, 1, 3, 2):
            for p, there in enumerate(flips()):
                at = self.rows(self.planes[k], there)
                self.flat(at, p, k).wait_recv()
                self.go(self.core(at, p, k))

    def finish(self):
        turn = 1 - 2 * (self.group % 2)
        for k in range(SHARDS):
            for p, there in enumerate(flips() + [self.group]):
                self.core(self.rows(self.planes[k], there + turn), p, k).wait_recv()
        for copy in self.sent:
            copy.wait_send()


def gather_sems():
    return [
        pltpu.SemaphoreType.DMA((2, SHARDS)),
        pltpu.SemaphoreType.DMA((2, 3, SHARDS)),
        pltpu.SemaphoreType.DMA((2, 4, SHARDS)),
        pltpu.SemaphoreType.DMA,
    ]


def finish_kernel(
    layers, *refs
):
    smalls, (carried_hbm, out_ref, shared_hbm, *refs) = refs[:layers], refs[layers:]
    core_ref, leave_ref, came_ref, far_ref, far_came_ref, piece_ref, stage_ref, sum_ref, *refs = refs
    core_sems, flat_sems, far_sems, back_sems, pair_sems, share_sems, stage_sem = refs
    group, shard = lax.axis_index("expert"), lax.axis_index("shard")
    turn = 1 - 2 * (group % 2)
    chip = group // 2
    size = piece_ref.shape[1]
    height = SHARDS * size
    stage = pltpu.make_async_copy(carried_hbm.at[shard], stage_ref, stage_sem)
    stage.start()
    meet_axes()
    pending = []

    def go(copy):
        copy.start()
        pending.append(copy)

    def part(layer, there):
        return smalls[layer].at[pl.ds(pl.multiple_of(there * height, height), height)]

    def core_copy(layer, at):
        chip_at = at // 2
        src = part(layer, chip_at * 2 + 1 - group % 2)
        return remote(src, core_ref.at[layer, chip_at], core_sems.at[0, layer, chip_at], core_sems.at[1, layer, chip_at], (other_core(), shard))

    def flat_copy(p):
        return remote(leave_ref.at[p], came_ref.at[p], flat_sems.at[0, p], flat_sems.at[1, p], (flips()[p], shard))

    order = flips() + [group]
    for there in order:
        for layer in range(layers):
            go(core_copy(layer, there))
    stage.wait()
    shares = share_blocks(lambda to: carried_hbm.at[to], lambda own: shared_hbm.at[own], share_sems, stage_ref)
    for copy in shares[:2]:
        copy.start()
    for p, there in enumerate(order[:3]):
        for layer in range(layers):
            core_copy(layer, there).wait_recv()
            leave_ref[p, layer] = (part(layer, there)[...].astype(F32) + core_ref[layer, there // 2].astype(F32)).astype(BF16)
        if p:
            go(flat_copy(p - 1))
    for layer in range(layers):
        core_copy(layer, group).wait_recv()
    go(flat_copy(2))
    for p in range(3):
        flat_copy(p).wait_recv()
    for layer in range(layers):
        total = part(layer, group)[...].astype(F32) + core_ref[layer, chip].astype(F32)
        for p in range(3):
            total = total + came_ref[p, layer].astype(F32)
        for plane in range(SHARDS):
            far_ref[plane, layer] = total[plane * size : (plane + 1) * size].astype(far_ref.dtype)
        sum_ref[layer] = total

    def far_copy(k):
        to = (shard + k) % SHARDS
        return remote(far_ref.at[to], far_came_ref.at[k], far_sems.at[0, k], far_sems.at[1, k], (group, to))

    for k in (2, 1, 3):
        go(far_copy(k))
    for copy in shares[2:]:
        copy.start()
    for k in (1, 3, 2):
        far_copy(k).wait_recv()
    for layer in range(layers):
        total = sum_ref[layer, pl.ds(pl.multiple_of(shard * size, size), size), :]
        for k in (1, 2, 3):
            total = total + far_came_ref[k, layer].astype(F32)
        piece_ref[layer] = total.astype(BF16)

    def place(there):
        return out_ref.at[:, pl.ds(pl.multiple_of(there * size, size), size)]

    place(group)[...] = piece_ref[...]

    def back_copy(p, at):
        return remote(piece_ref, at, back_sems.at[0, p], back_sems.at[1, p], (flips()[p], shard))

    def pair_copy(p, src, at):
        return remote(src, at, pair_sems.at[0, p], pair_sems.at[1, p], (other_core(), shard))

    for p in range(3):
        go(back_copy(p, place(group)))
    go(pair_copy(3, piece_ref, place(group)))
    for p, there in enumerate(flips()):
        back_copy(p, place(there)).wait_recv()
        go(pair_copy(p, place(there), place(there)))
    for p, there in enumerate(order):
        pair_copy(p, piece_ref, place(there + turn)).wait_recv()
    for copy in pending:
        copy.wait_send()
    for copy in shares:
        copy.wait()


def run_finish(smalls, carried):
    layers = len(smalls)
    groups = EXPERTS // SHARDS
    rows, width = smalls[0].shape
    span = rows // SHARDS
    size = span // groups
    chips = groups // 2
    height = SHARDS * size
    return pl.pallas_call(
        functools.partial(finish_kernel, layers),
        out_shape=[shape((layers, span, width), BF16), shape(carried.shape, BF16)],
        in_specs=in_vmem(layers) + anywhere(1),
        out_specs=in_vmem(1) + anywhere(1),
        scratch_shapes=[
            pltpu.VMEM((layers, chips, height, width), BF16),
            pltpu.VMEM((3, layers, height, width), BF16),
            pltpu.VMEM((3, layers, height, width), BF16),
            pltpu.VMEM((SHARDS, layers, size, width), BF16),
            pltpu.VMEM((SHARDS, layers, size, width), BF16),
            pltpu.VMEM((layers, size, width), BF16),
            pltpu.VMEM(carried.shape[1:], BF16),
            pltpu.VMEM((layers, height, width), F32),
            pltpu.SemaphoreType.DMA((2, layers, chips)),
            pltpu.SemaphoreType.DMA((2, 3)),
            pltpu.SemaphoreType.DMA((2, SHARDS)),
            pltpu.SemaphoreType.DMA((2, 3)),
            pltpu.SemaphoreType.DMA((2, 4)),
            pltpu.SemaphoreType.DMA((2, SHARDS)),
            pltpu.SemaphoreType.DMA,
        ],
        compiler_params=pltpu.CompilerParams(vmem_limit_bytes=48 << 20, collective_id=6, has_side_effects=True),
        name="finish",
    )(*smalls, carried)


def back_kernel(grad_in_ref, sums_ref, picks_ref, grad_gates_ref, chances_ref, x1_ref, x_ref, proj_ref, log_ref, att_ref, w_ref, grad_ref, sent_ref, parts_ref, normed_ref, gnormed_ref, gproj_ref, gatt_ref, back_ref, mid_ref, sums_a, sums_b, router_ref, small_ref):
    model = x_ref.shape[1]
    gain1, gain2, shift1, shift2 = weight_parts(w_ref, model)
    gnormed_ref[...] = sums_ref[...]
    norm_rows(x1_ref, gain2, shift2, normed_ref)
    router_pullback(grad_gates_ref, picks_ref, chances_ref, w_ref, normed_ref, gnormed_ref, router_ref)
    norm_pullback(x1_ref, gain2, gnormed_ref, grad_in_ref, mid_ref, sums_b)
    norm_rows(x_ref, gain1, shift1, normed_ref)
    attention_pullback(mid_ref, w_ref, proj_ref, log_ref, att_ref, normed_ref, small_ref, gproj_ref, gatt_ref, back_ref, gnormed_ref)
    norm_pullback(x_ref, gain1, gnormed_ref, mid_ref, grad_ref, sums_a)
    sent_ref[...] = grad_ref[...].astype(BF16)
    rows = lax.broadcasted_iota(jnp.int32, (LANES, model), 0)
    side = jnp.zeros((LANES, model), F32)
    for i, value in enumerate((sums_a[0:1, :], sums_b[0:1, :], sums_a[1:2, :], sums_b[1:2, :])):
        side = jnp.where(rows == EXPERTS + i, value, side)
    lane = lax.broadcasted_iota(jnp.int32, (model, LANES), 1)
    small_ref[:, 4 * model :] = jnp.where(lane < EXPERTS, router_ref[...], jnp.transpose(side))
    size = model // EXPERTS
    for at in range(EXPERTS):
        shard, group = at % SHARDS, at // SHARDS
        row = (shard * (EXPERTS // SHARDS) + group) * size
        parts_ref[at * size : (at + 1) * size, :] = small_ref[row : row + size, :].astype(BF16)


def shape(dims, kind):
    return jax.ShapeDtypeStruct(dims, kind)


def run_back(grad, sums, grad_gates, state):
    model = grad.shape[1]
    width = 4 * model + LANES
    inputs = [grad, sums, state.lanes_ref, grad_gates, state.chances_ref, state.x1_ref, state.x_ref]
    inputs += [state.proj_ref, state.log_ref, state.att_ref, state.w_ref]
    return pl.pallas_call(
        back_kernel,
        out_shape=[shape((ROWS, model), F32), shape((ROWS, model), BF16), shape((model, width), BF16)],
        in_specs=in_vmem(len(inputs)),
        out_specs=in_vmem(3),
        scratch_shapes=[
            pltpu.VMEM((ROWS, model), BF16),
            pltpu.VMEM((ROWS, model), F32),
            pltpu.VMEM((ROWS, 3 * model), BF16),
            pltpu.VMEM((ROWS, model), BF16),
            pltpu.VMEM((ROWS, model), BF16),
            pltpu.VMEM((ROWS, model), F32),
            pltpu.VMEM((2, model), F32),
            pltpu.VMEM((2, model), F32),
            pltpu.VMEM((model, LANES), F32),
            pltpu.VMEM((model, width), F32),
        ],
        compiler_params=pltpu.CompilerParams(vmem_limit_bytes=56 << 20),
        name="back",
    )(*inputs)


def output_kernel(layers, *refs):
    ins, outs = refs[:layers], refs[layers : 2 * layers]
    small_ref, grad_ref, count_ref = refs[2 * layers : 2 * layers + 3]
    in_ref, out_ref, qkv_ref, mix_ref, side_ref, input_ref = refs[2 * layers + 3 :]
    step = pl.program_id(0)
    model = grad_ref.shape[1]
    for layer in range(layers):

        @pl.when(step // SHARDS == layer)
        def _(layer=layer):
            in_ref[...] = ins[layer][...].astype(F32).reshape(in_ref.shape)
            out_ref[...] = outs[layer][...].astype(F32).reshape(out_ref.shape)

    @pl.when(step == 0)
    def _():
        qkv_ref[...] = small_ref[:, :, : 3 * model].astype(F32)
        mix_ref[...] = small_ref[:, :, 3 * model : 4 * model].astype(F32)
        side_ref[...] = small_ref[:, :, 4 * model :].astype(F32)
        for image in range(SLOTS):
            to, rows = image * SEQ, image * SEQ_PAD
            input_ref[to : to + SEQ, :] = grad_ref[rows : rows + SEQ, :] * count_ref[0]


def run_output(ins, outs, small, grad, counted):
    layers = len(ins)
    model = grad.shape[1]
    span = small.shape[1]

    def block(array, layer):
        at = lambda i: (jnp.clip(i - layer * SHARDS, 0, SHARDS - 1), 0, 0)
        return pl.BlockSpec((1,) + array.shape[1:], at)

    whole = lambda dims: pl.BlockSpec(dims, lambda i: (0,) * len(dims))
    filled = lambda array: pl.BlockSpec((1, 1) + array.shape[1:], lambda i: (i // SHARDS, i % SHARDS, 0, 0))
    small_shapes = [(layers, span, 3 * model), (layers, span, model), (layers, span, LANES), (SLOTS * SEQ, model)]
    return pl.pallas_call(
        functools.partial(output_kernel, layers),
        grid=(layers * SHARDS,),
        in_specs=[block(array, layer) for layer, array in enumerate(ins)]
        + [block(array, layer) for layer, array in enumerate(outs)]
        + [whole(small.shape), whole(grad.shape), pl.BlockSpec(memory_space=pltpu.SMEM)],
        out_specs=[filled(ins[0]), filled(outs[0])] + [whole(dims) for dims in small_shapes],
        out_shape=[shape((layers,) + ins[0].shape, F32), shape((layers,) + outs[0].shape, F32)]
        + [shape(dims, F32) for dims in small_shapes],
        compiler_params=pltpu.CompilerParams(vmem_limit_bytes=48 << 20),
        name="output",
    )(*ins, *outs, small, grad, counted)


def layer_norm(values, gain_row, shift_row):
    centred = values - jnp.mean(values, axis=-1, keepdims=True)
    spread = jnp.mean(centred * centred, axis=-1, keepdims=True)
    return centred * lax.rsqrt(spread + norm_eps) * gain_row + shift_row


def route_slots(picks_dev, capacity):
    flat_ids = picks_dev.reshape(-1)
    onehot = (flat_ids[:, None] == jnp.arange(EXPERTS, dtype=jnp.int32)[None, :]).astype(jnp.int32)
    before = jnp.cumsum(onehot, axis=0) - onehot
    ranking = jnp.sum(before * onehot, axis=1)
    slot_index = flat_ids * capacity + ranking
    routes_dev = flat_ids.shape[0]
    source = jnp.full((EXPERTS * capacity,), routes_dev, jnp.int32)
    source = source.at[slot_index].set(jnp.arange(routes_dev, dtype=jnp.int32))
    return (slot_index, source)


def attention_forward(current, qkv_full, out_full, gain_row, shift_row):
    model_width = current.shape[1]
    normed = layer_norm(current, gain_row, shift_row).astype(jnp.bfloat16)
    projected = jnp.dot(normed, qkv_full, preferred_element_type=jnp.float32).astype(jnp.bfloat16)
    split_parts = projected.reshape(SLOTS, SEQ, 3, HEADS, HEAD_DIM)
    scores = jnp.einsum(
        "ashd,athd->ahst",
        split_parts[:, :, 0],
        split_parts[:, :, 1],
        preferred_element_type=jnp.float32,
    ) * HEAD_DIM ** (-0.5)
    highest_score = jnp.max(scores, axis=-1, keepdims=True)
    exponent = jnp.exp(scores - highest_score)
    summed = jnp.sum(exponent, axis=-1, keepdims=True)
    weights = (exponent / summed).astype(jnp.bfloat16)
    log_total = highest_score + jnp.log(summed)
    attended = jnp.einsum(
        "ahst,athd->ashd", weights, split_parts[:, :, 2], preferred_element_type=jnp.float32
    )
    attended = attended.reshape(SLOTS * SEQ, model_width).astype(jnp.bfloat16)
    branch_out = jnp.dot(attended, out_full, preferred_element_type=jnp.float32)
    return (current + branch_out, (current, normed, projected, log_total, attended))


def attention_backward(grad_states, saved, qkv_full, out_full, gain_row, shift_row):
    current, normed, projected, log_total, attended = saved
    model_width = current.shape[1]
    grad_branch = grad_states.astype(jnp.bfloat16)
    grad_out = jnp.einsum("rd,re->de", attended, grad_branch, preferred_element_type=jnp.float32)
    grad_attended = jnp.einsum(
        "re,de->rd", grad_branch, out_full, preferred_element_type=jnp.float32
    ).astype(jnp.bfloat16)
    split_parts = projected.reshape(SLOTS, SEQ, 3, HEADS, HEAD_DIM)
    queries = split_parts[:, :, 0]
    keys_part = split_parts[:, :, 1]
    values_part = split_parts[:, :, 2]
    scaling = HEAD_DIM ** (-0.5)
    scores = (
        jnp.einsum("ashd,athd->ahst", queries, keys_part, preferred_element_type=jnp.float32)
        * scaling
    )
    chances = jnp.exp(scores - log_total)
    grad_heads = grad_attended.reshape(SLOTS, SEQ, HEADS, HEAD_DIM)
    grad_weights = jnp.einsum(
        "ashd,athd->ahst", grad_heads, values_part, preferred_element_type=jnp.float32
    )
    grad_values = jnp.einsum(
        "ahst,ashd->athd",
        chances.astype(jnp.bfloat16),
        grad_heads,
        preferred_element_type=jnp.float32,
    )
    centre_term = jnp.sum(grad_weights * chances, axis=-1, keepdims=True)
    grad_scores = (chances * (grad_weights - centre_term)).astype(jnp.bfloat16)
    grad_queries = (
        jnp.einsum("ahst,athd->ashd", grad_scores, keys_part, preferred_element_type=jnp.float32)
        * scaling
    )
    grad_keys = (
        jnp.einsum("ahst,ashd->athd", grad_scores, queries, preferred_element_type=jnp.float32)
        * scaling
    )
    grad_projected = jnp.stack([grad_queries, grad_keys, grad_values], axis=2)
    grad_projected = grad_projected.reshape(SLOTS * SEQ, 3 * model_width).astype(jnp.bfloat16)
    grad_qkv = jnp.einsum("rd,re->de", normed, grad_projected, preferred_element_type=jnp.float32)
    grad_normed = jnp.einsum(
        "re,de->rd", grad_projected, qkv_full, preferred_element_type=jnp.float32
    )
    _, norm_pullback = jax.vjp(layer_norm, current, gain_row, shift_row)
    grad_input, grad_gain, grad_shift = norm_pullback(grad_normed)
    return (grad_states + grad_input, grad_qkv, grad_out, grad_gain, grad_shift)


def mixture_forward(current, gain_row, shift_row, router_full, in_shard, out_shard, picks_layer):
    row_count, model_width = current.shape
    experts_all = router_full.shape[1]
    normed = layer_norm(current, gain_row, shift_row).astype(jnp.bfloat16)
    logits = jnp.dot(normed, router_full, preferred_element_type=jnp.float32)
    chances = jax.nn.softmax(logits, axis=-1)
    matches = picks_layer[:, :, None] == jnp.arange(experts_all, dtype=jnp.int32)[None, None, :]
    gate_values = jnp.sum(jnp.where(matches, chances[:, None, :], 0.0), axis=-1)
    slot_index, source = route_slots(picks_layer, CAP)
    filled = source < TOP * row_count
    route_clip = jnp.minimum(source, TOP * row_count - 1)
    taken_rows = route_clip // TOP
    outgoing = jnp.where(filled[:, None], normed[taken_rows], jnp.zeros((), jnp.bfloat16))
    outgoing = outgoing.reshape(experts_all, CAP, model_width)
    arrived = lax.all_to_all(outgoing, "expert", split_axis=0, concat_axis=1, tiled=True)
    in_full, out_full = (
        lax.all_gather(in_shard, "shard", axis=1, tiled=True),
        lax.all_gather(out_shard, "shard", axis=1, tiled=True),
    )
    hidden_pre = jnp.einsum("erd,edh->erh", arrived, in_full, preferred_element_type=jnp.float32)
    activated = jax.nn.gelu(hidden_pre).astype(jnp.bfloat16)
    produced = jnp.einsum(
        "erh,ehd->erd", activated, out_full, preferred_element_type=jnp.float32
    ).astype(jnp.bfloat16)
    returned = lax.all_to_all(produced, "expert", split_axis=1, concat_axis=0, tiled=True)
    routed = returned.reshape(experts_all * CAP, model_width)[slot_index].reshape(
        row_count, TOP, model_width
    )
    updated = current + jnp.sum(gate_values[:, :, None] * routed.astype(jnp.float32), axis=1)
    saved = (
        current,
        normed,
        chances,
        matches,
        gate_values,
        slot_index,
        filled,
        route_clip,
        arrived,
        routed,
        in_full,
        out_full,
    )
    return (updated, saved)


def mixture_backward(grad_states, saved, gain_row, shift_row, router_full, in_shard, out_shard):
    (current, normed, chances, matches, gate_values, slot_index, filled, route_clip, arrived, routed, _, _) = saved
    row_count, model_width = current.shape
    experts_all = chances.shape[1]
    grad_routed = (gate_values[:, :, None] * grad_states[:, None, :]).astype(jnp.bfloat16)
    grad_routed = grad_routed.reshape(TOP * row_count, model_width)
    grad_gates = jnp.sum(grad_states[:, None, :] * routed.astype(jnp.float32), axis=-1)
    grad_outgoing = jnp.where(filled[:, None], grad_routed[route_clip], jnp.zeros((), jnp.bfloat16))
    grad_outgoing = grad_outgoing.reshape(experts_all, CAP, model_width)
    grad_result = lax.all_to_all(grad_outgoing, "expert", split_axis=0, concat_axis=1, tiled=True)
    in_full, out_full = (
        lax.all_gather(in_shard, "shard", axis=1, tiled=True),
        lax.all_gather(out_shard, "shard", axis=1, tiled=True),
    )
    hidden_pre = jnp.einsum("erd,edh->erh", arrived, in_full, preferred_element_type=jnp.float32)
    activated, gelu_pullback = jax.vjp(jax.nn.gelu, hidden_pre)
    grad_out_experts = jnp.einsum(
        "erh,erd->ehd",
        activated.astype(jnp.bfloat16),
        grad_result,
        preferred_element_type=jnp.float32,
    )
    grad_activated = jnp.einsum(
        "erd,ehd->erh", grad_result, out_full, preferred_element_type=jnp.float32
    )
    grad_pre = gelu_pullback(grad_activated)[0].astype(jnp.bfloat16)
    grad_in_experts = jnp.einsum(
        "erd,erh->edh", arrived, grad_pre, preferred_element_type=jnp.float32
    )
    grad_arrived = jnp.einsum(
        "erh,edh->erd", grad_pre, in_full, preferred_element_type=jnp.float32
    ).astype(jnp.bfloat16)
    grad_returned = lax.all_to_all(grad_arrived, "expert", split_axis=1, concat_axis=0, tiled=True)
    grad_in_share, grad_out_share = (
        lax.psum_scatter(
            grad_in_experts.astype(jnp.bfloat16), "shard", scatter_dimension=1, tiled=True
        ).astype(jnp.float32),
        lax.psum_scatter(
            grad_out_experts.astype(jnp.bfloat16), "shard", scatter_dimension=1, tiled=True
        ).astype(jnp.float32),
    )
    grad_routes = grad_returned.reshape(experts_all * CAP, model_width)[slot_index]
    grad_normed = jnp.sum(
        grad_routes.reshape(row_count, TOP, model_width).astype(jnp.float32), axis=1
    )
    grad_chances = jnp.sum(jnp.where(matches, grad_gates[:, :, None], 0.0), axis=1)
    grad_logits = chances * (grad_chances - jnp.sum(grad_chances * chances, axis=-1, keepdims=True))
    grad_logits = grad_logits.astype(jnp.bfloat16)
    grad_router = jnp.einsum("rd,re->de", normed, grad_logits, preferred_element_type=jnp.float32)
    grad_normed = grad_normed + jnp.einsum(
        "re,de->rd", grad_logits, router_full, preferred_element_type=jnp.float32
    )
    _, norm_pullback = jax.vjp(layer_norm, current, gain_row, shift_row)
    grad_input, grad_gain, grad_shift = norm_pullback(grad_normed)
    return (
        grad_states + grad_input,
        grad_router,
        grad_gain,
        grad_shift,
        grad_in_share,
        grad_out_share,
    )


def shards(
    states,
    qkv_weight,
    out_weight,
    norm_gain,
    norm_bias,
    router_weight,
    expert_in,
    expert_out,
    chosen,
    image_count,
    teacher,
):
    qkv_full, out_full, gain_full, bias_full, router_full = (
        lax.all_gather(qkv_weight, "shard", axis=1, tiled=True),
        lax.all_gather(out_weight, "shard", axis=1, tiled=True),
        lax.all_gather(norm_gain, "shard", axis=1, tiled=True),
        lax.all_gather(norm_bias, "shard", axis=1, tiled=True),
        lax.all_gather(router_weight, "shard", axis=1, tiled=True),
    )
    gain_float = gain_full.astype(jnp.float32)
    bias_float = bias_full.astype(jnp.float32)
    layer_count = qkv_weight.shape[0]
    row_count, model_width = states.shape
    slot_image = jnp.arange(row_count, dtype=jnp.int32) // SEQ
    living = slot_image < image_count[0]
    counted = lax.psum(image_count[0].astype(jnp.float32) * SEQ, ("expert", "shard"))
    current = states.astype(jnp.float32)
    attention_kept = []
    mixture_kept = []
    for layer_index in range(layer_count):
        current, kept_attention = attention_forward(
            current,
            qkv_full[layer_index],
            out_full[layer_index],
            gain_float[layer_index, :, 0],
            bias_float[layer_index, :, 0],
        )
        current, kept_mixture = mixture_forward(
            current,
            gain_float[layer_index, :, 1],
            bias_float[layer_index, :, 1],
            router_full[layer_index],
            expert_in[layer_index],
            expert_out[layer_index],
            chosen[layer_index],
        )
        attention_kept.append(kept_attention)
        mixture_kept.append(kept_mixture)
    missed = current - teacher.astype(jnp.float32)
    grad_states = jnp.where(living[:, None], 2.0 * missed, 0.0) / counted
    qkv_list = [None] * layer_count
    out_list = [None] * layer_count
    gain_list = [None] * layer_count
    bias_list = [None] * layer_count
    router_list = [None] * layer_count
    in_list = [None] * layer_count
    experts_out_list = [None] * layer_count
    for layer_index in reversed(range(layer_count)):
        grad_states, grad_router, gain_second, shift_second, grad_in_share, grad_out_share = (
            mixture_backward(
                grad_states,
                mixture_kept[layer_index],
                gain_float[layer_index, :, 1],
                bias_float[layer_index, :, 1],
                router_full[layer_index],
                expert_in[layer_index],
                expert_out[layer_index],
            )
        )
        grad_states, grad_qkv, grad_out, gain_first, shift_first = attention_backward(
            grad_states,
            attention_kept[layer_index],
            qkv_full[layer_index],
            out_full[layer_index],
            gain_float[layer_index, :, 0],
            bias_float[layer_index, :, 0],
        )
        qkv_list[layer_index] = grad_qkv
        out_list[layer_index] = grad_out
        gain_list[layer_index] = jnp.stack([gain_first, gain_second], axis=-1)
        bias_list[layer_index] = jnp.stack([shift_first, shift_second], axis=-1)
        router_list[layer_index] = grad_router
        in_list[layer_index] = grad_in_share
        experts_out_list[layer_index] = grad_out_share
    mixer_grads = (
        jnp.stack(qkv_list),
        jnp.stack(out_list),
        jnp.stack(gain_list),
        jnp.stack(bias_list),
        jnp.stack(router_list),
    )
    summed = lax.psum(
        (mixer_grads[0], mixer_grads[1], mixer_grads[2], mixer_grads[3], mixer_grads[4]),
        ("expert", "shard"),
    )
    share_width = model_width // lax.axis_size("shard")
    start_index = lax.axis_index("shard") * share_width
    reduced = tuple(
        (lax.dynamic_slice_in_dim(member, start_index, share_width, 1) for member in summed)
    )
    return (
        current.astype(jnp.bfloat16),
        grad_states * counted,
        reduced[0],
        reduced[1],
        reduced[2],
        reduced[3],
        reduced[4],
        jnp.stack(in_list),
        jnp.stack(experts_out_list),
    )


def pad_rows(values, fill=0):
    width = values.shape[-1]
    images = values.reshape(SLOTS, SEQ, width)
    images = jnp.pad(images, ((0, 0), (0, SEQ_PAD - SEQ), (0, 0)), constant_values=fill)
    images = images.reshape(SLOTS * SEQ_PAD, width)
    return jnp.pad(images, ((0, ROWS - SLOTS * SEQ_PAD), (0, 0)), constant_values=fill)


def live_rows(values):
    images = values[: SLOTS * SEQ_PAD].reshape(SLOTS, SEQ_PAD, values.shape[-1])
    return images[:, :SEQ].reshape(SLOTS * SEQ, values.shape[-1])


def owners(
    states,
    qkv_weight,
    out_weight,
    norm_gain,
    norm_bias,
    router_weight,
    expert_in,
    expert_out,
    chosen,
    image_count,
    teacher,
):
    layers, share, _ = qkv_weight.shape
    model = states.shape[1]
    groups = lax.axis_size("expert")
    piece = share // groups
    spare = LANES - EXPERTS - 5
    marks = jnp.zeros((layers, share, 1 + spare), BF16)
    packed = jnp.concatenate([qkv_weight, out_weight, router_weight, norm_gain, norm_bias, marks], axis=2)
    packed = lax.dynamic_slice_in_dim(packed, lax.axis_index("expert") * piece, piece, 1)
    mark_at = 4 * model + EXPERTS + 4
    packed = packed.at[0, 0, mark_at].set(image_count[0].astype(BF16))
    picks = [pad_rows(chosen[layer], -1).T for layer in range(layers)]
    picks = jnp.concatenate(picks + [jnp.full((8 - TOP * layers, ROWS), -1, jnp.int32)])
    arrays = dict(states_ref=states, piece_ref=packed[0], picks_ref=picks)
    kept = []
    next_in = None
    for layer in range(layers):
        more = layer + 1 < layers
        if more:
            arrays.update(next_piece_ref=packed[layer + 1])
        made = run_layer(layer, arrays, next_in, expert_out, expert_in)
        state = types.SimpleNamespace(**arrays, **made)
        kept.append(state)
        if layer == 0:
            counted = state.marks_ref[0, EXPERTS + 4] * SEQ
            slot_image = jnp.arange(states.shape[0], dtype=jnp.int32) // SEQ
            living = slot_image < image_count[0]
            twice = pad_rows(jnp.where(living, 2.0, 0.0)[:, None])
        if more:
            next_in = state.next_hbm
            arrays = dict(
                below_ref=state.x1_ref,
                step_ref=state.delta_ref,
                w_ref=state.next_w_ref,
                picks_ref=picks,
                theirs_ref=kept[0].theirs_ref,
            )
        if layer + 2 == layers:
            arrays.update(teacher_ref=pad_rows(teacher), twice_ref=twice, marks_ref=kept[0].marks_ref)
    grad, sent = state.grad_ref, state.sent_ref
    smalls, ins, outs = [None] * layers, [None] * layers, [None] * layers
    carried = ()
    for layer in reversed(range(layers)):
        state = kept[layer]
        own_in = kept[layer - 1].next_hbm if layer else state.kept_in_hbm
        sums, grad_gates, grad_in, grad_out, *shared = run_unmix(grad, sent, state, own_in, carried)
        if shared:
            (outs[layer + 1],) = shared
        blocks = lambda part: part.reshape(SHARDS, part.shape[0] // SHARDS, part.shape[1])
        carried = (blocks(grad_out),)
        ins[layer] = lax.all_to_all(blocks(grad_in), "shard", split_axis=0, concat_axis=0, tiled=True)
        grad, sent, smalls[layer] = run_back(grad, sums, grad_gates, state)
    small, outs[0] = run_finish(smalls, *carried)
    final = kept[-1].final_ref
    in_grad, out_grad, qkv, mixed, side, first_grad = run_output(ins, outs, small, grad, counted.reshape(1))
    return (
        live_rows(final),
        first_grad,
        qkv,
        mixed,
        side[:, :, EXPERTS : EXPERTS + 2],
        side[:, :, EXPERTS + 2 : EXPERTS + 4],
        side[:, :, :EXPERTS],
        in_grad,
        out_grad,
    )


def plan_of(mesh):
    return owners if owns(mesh) else shards


def owns(mesh):
    groups, shards_all = mesh.shape["expert"], mesh.shape["shard"]
    return shards_all == SHARDS and groups * shards_all == EXPERTS


def solution(mesh):
    in_specs = (
        P(("expert", "shard"), None),
        P(None, "shard", None),
        P(None, "shard", None),
        P(None, "shard", None),
        P(None, "shard", None),
        P(None, "shard", None),
        P(None, "expert", "shard", None),
        P(None, "expert", "shard", None),
        P(None, ("expert", "shard"), None),
        P(("expert", "shard")),
        P(("expert", "shard"), None),
    )
    out_specs = (
        P(("expert", "shard"), None),
        P(("expert", "shard"), None),
        P(None, "shard", None),
        P(None, "shard", None),
        P(None, "shard", None),
        P(None, "shard", None),
        P(None, "shard", None),
        P(None, "expert", "shard", None),
        P(None, "expert", "shard", None),
    )
    return jax.shard_map(plan_of(mesh), mesh=mesh, in_specs=in_specs, out_specs=out_specs, check_vma=False)
```
